128 devices in a mesh: lon: 32 (over z, y_lo, x), ch: 4 (over y_hi, core).
Axes of the slice: x: 4, y: 4 (y_hi: 2, y_lo: 2; y = y_hi * 2 + y_lo), z: 4, core: 2. Of those that a mesh axis runs over, the one named last changes fastest.
Arguments:
- grid_inputs: bfloat16 [921600, 474], P('lon'), may hold values from -6 to 6
- embed_weight: bfloat16 [474, 512], replicated, may hold values from -0.25 to 0.25
- embed_bias: float32 [512], replicated, may hold values from -3 to 3
- mesh_latent: bfloat16 [20480, 512], P('lon', 'ch'), may hold values from -6 to 6
- edge_features: bfloat16 [4, 720896], P(None, 'lon'), may hold values from -6 to 6
- senders: int32 [720896], P('lon'), may hold values from 0 to 921599, as said below
- receivers: int32 [720896], P('lon'), may hold values from 0 to 20479, as said below
- sender_weight: bfloat16 [512, 512], P(None, 'ch'), may hold values from -0.25 to 0.25
- receiver_weight: bfloat16 [512, 512], P(None, 'ch'), may hold values from -0.25 to 0.25
- feature_weight: bfloat16 [4, 512], P(None, 'ch'), may hold values from -3 to 3
- hidden_bias: float32 [512], P('ch'), may hold values from -3 to 3
- message_weight: bfloat16 [512, 512], P('ch'), may hold values from -0.25 to 0.25
- message_bias: float32 [512], replicated, may hold values from -1.2 to 1.2
- norm_gain: float32 [512], P('ch'), may hold values from 0.5 to 1.5
- norm_shift: float32 [512], P('ch'), may hold values from -3 to 3
Outputs:
- mesh_out: bfloat16 [20480, 512], P('lon', 'ch')
The draws below stay inside these ranges and needn't reach their ends.
Inputs may be any that keep to these rules, and one draw needn't show every extreme that they name: Edge e belongs to block b = e // 22528. Its sender is c * 640 + t with latitude row t and a column c that lies, counted around the closed circle of 1440 columns, at most 4 columns before or after the block's own columns b * 45 to b * 45 + 44; some block reaches 4 columns on both sides. Within each aligned run of min(2048, 22528) edges of a block, the senders' columns, counted from the block's first widened column, lie within 7 consecutive columns. `receivers`: the receiver of edge e lies among the mesh nodes b * 640 to b * 640 + 639 of its block b = e // 22528; a mesh node may receive no edge.
All inputs are finite; a program needn't handle non-finite values.
Results may differ from the reference program's by a relative error of at most 0.0028.
Values may be sent and summed in bfloat16 or wider, within the bound.
No kernel may reach another device: no remote copies, remote signals or barrier semaphores. Data moves between devices by JAX's collectives and lax.ppermute only.
A program may use at most 128 MiB of HBM per device.

```python
import jax
import jax.numpy as jnp
from jax import lax

CIN = 474
L = 512
CE = 4
COLS_DEV = 45
LAT = 640
M_DEV = 640
E_DEV = 22528
HALO = 4
NCOL = 1440
NGRID = 921600
NMESH = 20480
NEDGE = 720896


def draw_senders(key, part):
    base_key = jax.random.fold_in(key, 11)
    reach_key, pick_key, col_key, lat_key = jax.random.split(base_key, 4)
    blocks = NEDGE // E_DEV
    reaches = jax.random.randint(reach_key, (blocks,), 1, HALO + 1)
    chosen = jax.random.randint(pick_key, (), 0, blocks)
    reaches = jnp.where(jnp.arange(blocks) == chosen, HALO, reaches)
    edge_ids = jnp.arange(NEDGE)
    owning = edge_ids // E_DEV
    within = edge_ids % E_DEV
    reach = reaches[owning]
    span = COLS_DEV + 2 * reach
    jitter = jax.random.randint(col_key, (NEDGE,), 0, 2)
    offset = jnp.minimum(within * span // E_DEV + jitter, span - 1)
    offset = jnp.where(within == 0, 0, offset)
    offset = jnp.where(within == E_DEV - 1, span - 1, offset)
    column = jnp.mod(owning * COLS_DEV + offset - reach, NCOL)
    latitude = jax.random.randint(lat_key, (NEDGE,), 0, LAT)
    return (column * LAT + latitude).astype(jnp.int32)


def draw_receivers(key, part):
    base_key = jax.random.fold_in(key, 23)
    edge_ids = jnp.arange(NEDGE)
    slots = jax.random.randint(base_key, (NEDGE,), 0, M_DEV)
    return (edge_ids // E_DEV * M_DEV + slots).astype(jnp.int32)


def shard_levels(key, extent, cuts, smallest, high):
    def one(axis_at, parts):
        steps = jax.random.uniform(jax.random.fold_in(jax.random.fold_in(key, 6), axis_at), (parts,), jnp.float32, smallest / len(cuts), high / len(cuts))
        return jnp.repeat(jnp.exp(steps), extent[axis_at] // parts).reshape((-1,) + (1,) * (len(extent) - axis_at - 1))

    level = one(*cuts[0])
    for cut in cuts[1:]:
        level = level * one(*cut)
    return level


def normal_values(own_key, shape, scale, bound, shards=(), held_as=jnp.bfloat16):
    result = scale * jax.random.normal(own_key, shape, jnp.float32)
    if shards:
        result = result * shard_levels(own_key, shape, shards, -0.22, 0.18)
    return jnp.clip(result, -bound, bound).astype(held_as)


def setup_inputs(seed: int = 0) -> dict:
    keys = jax.random.split(jax.random.key(seed), 16)
    grid_inputs = normal_values(keys[0], (NGRID, CIN), 1.0, 6.0, ((0, 32),))
    embed_weight = normal_values(keys[1], (CIN, L), CIN ** -0.5, 0.25)
    embed_bias = normal_values(keys[2], (L,), 0.5, 3.0, (), jnp.float32)
    mesh_latent = normal_values(keys[3], (NMESH, L), 1.0, 6.0, ((0, 32), (1, 4)))
    edge_features = normal_values(keys[4], (CE, NEDGE), 1.0, 6.0, ((1, 32),))
    senders = draw_senders(jax.random.fold_in(keys[15], 71), 0)
    receivers = draw_receivers(jax.random.fold_in(keys[15], 71), 0)
    sender_weight = normal_values(keys[7], (L, L), L ** -0.5, 0.25, ((1, 4),))
    receiver_weight = normal_values(keys[8], (L, L), L ** -0.5, 0.25, ((1, 4),))
    feature_weight = normal_values(keys[9], (CE, L), CE ** -0.5, 3.0, ((1, 4),))
    hidden_bias = normal_values(keys[10], (L,), 0.5, 3.0, ((0, 4),), jnp.float32)
    message_weight = normal_values(keys[11], (L, L), L ** -0.5, 0.25, ((0, 4),))
    message_bias = normal_values(keys[12], (L,), 0.2, 1.2, (), jnp.float32)
    norm_gain = jnp.clip(1.0 + 0.1 * jax.random.normal(keys[13], (L,), jnp.float32), 0.5, 1.5)
    norm_shift = normal_values(keys[14], (L,), 0.5, 3.0, ((0, 4),), jnp.float32)
    return {"grid_inputs": grid_inputs, "embed_weight": embed_weight, "embed_bias": embed_bias, "mesh_latent": mesh_latent, "edge_features": edge_features, "senders": senders, "receivers": receivers, "sender_weight": sender_weight, "receiver_weight": receiver_weight, "feature_weight": feature_weight, "hidden_bias": hidden_bias, "message_weight": message_weight, "message_bias": message_bias, "norm_gain": norm_gain, "norm_shift": norm_shift}


def reference(grid_inputs, embed_weight, embed_bias, mesh_latent, edge_features, senders, receivers, sender_weight, receiver_weight, feature_weight, hidden_bias, message_weight, message_bias, norm_gain, norm_shift):
    latent = jax.nn.silu(jnp.dot(grid_inputs, embed_weight, preferred_element_type=jnp.float32) + embed_bias).astype(jnp.bfloat16)
    sent_terms = jnp.dot(latent, sender_weight, preferred_element_type=jnp.float32)
    recv_terms = jnp.dot(mesh_latent, receiver_weight, preferred_element_type=jnp.float32)
    blocks = NEDGE // E_DEV
    feature_blocks = jnp.transpose(edge_features.reshape(CE, blocks, E_DEV), (1, 2, 0))
    send_blocks = senders.reshape(blocks, E_DEV)
    recv_blocks = receivers.reshape(blocks, E_DEV)

    def accumulate(carried, pieces):
        totals, tallies = carried
        send_ids, recv_ids, features = pieces
        before = sent_terms[send_ids] + recv_terms[recv_ids]
        before = before + jnp.dot(features, feature_weight, preferred_element_type=jnp.float32) + hidden_bias
        hidden = jax.nn.silu(before).astype(jnp.bfloat16)
        totals = totals + jax.ops.segment_sum(hidden.astype(jnp.float32), recv_ids, num_segments=NMESH)
        tallies = tallies + jax.ops.segment_sum(jnp.ones((E_DEV,), jnp.float32), recv_ids, num_segments=NMESH)
        return ((totals, tallies), None)
    start = (jnp.zeros((NMESH, L), jnp.float32), jnp.zeros((NMESH,), jnp.float32))
    (totals, tallies), ignored = lax.scan(accumulate, start, (send_blocks, recv_blocks, feature_blocks))
    aggregated = jnp.dot(totals, message_weight.astype(jnp.float32), precision=lax.Precision.HIGHEST)
    aggregated = aggregated + tallies[:, None] * message_bias
    centre = lax.optimization_barrier(jnp.mean(aggregated, axis=1, keepdims=True))
    spread = lax.optimization_barrier(jnp.mean(jnp.square(aggregated - centre), axis=1, keepdims=True))
    normed = (aggregated - centre) * lax.rsqrt(spread + 1.0)
    return (mesh_latent.astype(jnp.float32) + normed * norm_gain + norm_shift).astype(jnp.bfloat16)
```

```python
import functools

import jax
import jax.numpy as jnp
from jax import lax
from jax.experimental import pallas as pl
from jax.experimental.pallas import tpu as pltpu
from jax.sharding import PartitionSpec as P

LAT = 640
HALO = 4
CHUNK = 512
RUN_CHUNKS = 4
SLOTS = 4
WINDOW = 7
PITCH = CHUNK + 8
UNROLL = 32

f32 = jnp.float32
bf16 = jnp.bfloat16


def silu(value):
    half = 0.5 * value
    return half + half * jnp.tanh(half)


def dot(left, right):
    return jnp.dot(left, right, preferred_element_type=f32)


def wide_row(ref, index):
    return ref[pl.ds(pl.multiple_of(index * 4, 4), 4), :]


def chunk_of(tile):
    return jnp.concatenate([tile[j * PITCH : j * PITCH + CHUNK, :] for j in range(4)], axis=1)


def list_chunks(chunks, first_chunk, low_ref, high_ref, own_columns, outer, chunk_list):
    def step(i, count):
        low = low_ref[first_chunk + i]
        high = high_ref[first_chunk + i]
        halo = (low < HALO) | (high >= HALO + own_columns)
        mine = halo if outer else jnp.logical_not(halo)

        @pl.when(mine)
        def _():
            chunk_list[count] = i

        return count + jnp.where(mine, 1, 0)

    return lax.fori_loop(0, chunks, step, 0)


def list_columns(count, first_chunk, low_ref, high_ref, chunk_list, column_list, offset_list):
    slot0 = lax.shift_right_logical(first_chunk, 2)
    total = jnp.int32(0)
    seg_first = jnp.int32(1000)
    seg_last = jnp.int32(-1)
    seg_start = jnp.int32(0)
    for slot in range(SLOTS):

        def step(t, carry):
            low, high = carry
            g = first_chunk + chunk_list[t]
            here = lax.shift_right_logical(g, 2) == slot0 + slot
            return (
                jnp.where(here, jnp.minimum(low, low_ref[g]), low),
                jnp.where(here, jnp.maximum(high, high_ref[g]), high),
            )

        low, high = lax.fori_loop(0, count, step, (jnp.int32(1000), jnp.int32(-1)))
        has = high >= 0
        joins = has & (low >= seg_first) & (low <= seg_last + 1)
        begin = jnp.where(joins, seg_last + 1, low)
        fresh = jnp.where(has, jnp.maximum(high - begin + 1, 0), 0)
        base = total

        def put(j, carry):
            column_list[base + j] = begin + j
            return carry

        lax.fori_loop(0, fresh, put, 0)
        opens = has & jnp.logical_not(joins)
        seg_start = jnp.where(opens, total, seg_start)
        seg_first = jnp.where(opens, low, seg_first)
        seg_last = jnp.where(opens, high, jnp.maximum(seg_last, high))
        total = total + fresh
        offset_list[slot] = (seg_start - seg_first) * LAT
    return total


def embed_kernel(outer, chunks, own_columns, channels, *refs):
    if outer:
        (place, points, low_ref, high_ref, grid, low_own, low_swap, high_own, high_swap,
         weight, bias, _, out) = refs[:13]
        rest = refs[13:]
    else:
        place, points, low_ref, high_ref, grid, weight, bias, out = refs[:8]
        rest = refs[8:]
    table, columns, tile, result, chunk_list, column_list, offset_list, in_sems, out_sems = rest
    first_chunk = place[0] * chunks
    core = place[1]
    count = list_chunks(chunks, first_chunk, low_ref, high_ref, own_columns, outer, chunk_list)
    total = list_columns(
        count, first_chunk, low_ref, high_ref, chunk_list, column_list, offset_list
    )

    def fetch(source, column, slot):
        start = pl.multiple_of(column * LAT, 128)
        pltpu.make_async_copy(
            source.at[:, pl.ds(start, LAT)], columns.at[slot], in_sems.at[slot]
        ).start()

    def start_column(i):
        column = column_list[i]
        slot = lax.rem(i, 2)
        if not outer:
            fetch(grid, column - HALO, slot)
            return
        inside = (column >= HALO) & (column < HALO + own_columns)

        @pl.when(inside)
        def _():
            fetch(grid, column - HALO, slot)

        for is_side, shift, direct, swapped in (
            (column < HALO, 0, low_own, low_swap),
            (column >= HALO + own_columns, HALO + own_columns, high_own, high_swap),
        ):
            place_in = column - shift
            half = lax.shift_right_arithmetic(place_in, 1)
            within = lax.bitwise_and(place_in, 1)

            @pl.when(is_side & (half == core))
            def _():
                fetch(direct, within, slot)

            @pl.when(is_side & (half != core))
            def _():
                fetch(swapped, within, slot)

    @pl.when(total > 0)
    def _():
        start_column(0)

    def turn(i, carry):
        slot = lax.rem(i, 2)

        @pl.when(i + 1 < total)
        def _():
            start_column(i + 1)

        pltpu.make_async_copy(
            grid.at[:, pl.ds(0, LAT)], columns.at[slot], in_sems.at[slot]
        ).wait()
        source = columns.at[slot]
        for l in range(LAT // 128):
            lanes = pl.ds(l * 128, 128)
            for j in range(4):
                top = min(channels, (j + 1) * 128)
                block = source[j * 128 : top, lanes]
                if top < (j + 1) * 128:
                    block = jnp.pad(block, ((0, (j + 1) * 128 - top), (0, 0)))
                row = pl.multiple_of((i * LAT + l * 128) * 4, 8)
                table[pl.ds(row + j, 128, stride=4), :] = block.T.astype(f32)
        return carry

    lax.fori_loop(0, total, turn, 0)

    def work(t, carry):
        i = chunk_list[t]
        g = first_chunk + i
        offset = offset_list[
            lax.shift_right_logical(g, 2) - lax.shift_right_logical(first_chunk, 2)
        ]
        edge0 = g * CHUNK

        def gather(b, inner):
            for u in range(UNROLL):
                e = b * UNROLL + u
                tile[pl.ds(e, 4, stride=PITCH), :] = wide_row(table, points[edge0 + e] + offset)
            return inner

        lax.fori_loop(0, CHUNK // UNROLL, gather, 0)
        slot = lax.rem(t, 2)
        latent = silu(dot(chunk_of(tile).astype(bf16), weight[...]) + bias[...]).astype(bf16)

        @pl.when(t >= 2)
        def _():
            pltpu.make_async_copy(
                result.at[slot], out.at[pl.ds(0, CHUNK)], out_sems.at[slot]
            ).wait()

        result[slot] = latent
        pltpu.make_async_copy(
            result.at[slot],
            out.at[pl.ds(pl.multiple_of(i * CHUNK, CHUNK), CHUNK)],
            out_sems.at[slot],
        ).start()
        return carry

    lax.fori_loop(0, count, work, 0)
    for back in (2, 1):

        @pl.when(count >= back)
        def _():
            slot = lax.rem(count - back, 2)
            pltpu.make_async_copy(
                result.at[slot], out.at[pl.ds(0, CHUNK)], out_sems.at[slot]
            ).wait()


def edge_kernel(chunks, nodes, place, receivers, latent, ids, features, w0, w1, w2, w3,
                m0, m1, m2, m3, message_bias, keep, send,
                rows, tile, arrived, send_weight, recv_weight, message_weight, mesh, feature_weight,
                totals, tally, sems):
    k = place[0]
    first_chunk = k * chunks

    def start(t):
        slot = lax.rem(t, 2)
        pltpu.make_async_copy(
            latent.at[pl.ds(pl.multiple_of(t * CHUNK, CHUNK), CHUNK)], arrived.at[slot], sems.at[slot]
        ).start()

    start(0)
    biases = []
    for j, (w, m) in enumerate(((w0, m0), (w1, m1), (w2, m2), (w3, m3))):
        lanes = pl.ds(j * 128, 128)
        send_weight[:, lanes] = w[0:512, :]
        recv_weight[:, lanes] = w[512:1024, :]
        for q in range(4):
            message_weight[j * 128 : (j + 1) * 128, q * 128 : (q + 1) * 128] = w[
                1024 + q * 128 : 1024 + (q + 1) * 128, :
            ]
        extra = w[1536:1552, :].astype(f32)
        feature_weight[0:4, lanes] = extra[0:4, :]
        biases.append(extra[4:5, :] + extra[5:6, :] + extra[6:7, :])
        at = pl.multiple_of(jnp.bitwise_xor(k, j) * 128, 128)
        mesh[:, pl.ds(at, 128)] = m[...]
    bias = jnp.concatenate(biases, axis=1)
    terms = dot(mesh[...], recv_weight[...]) + bias
    for j in range(4):
        rows[pl.ds(j, nodes, stride=4), :] = terms[:, j * 128 : (j + 1) * 128]
    totals[...] = jnp.zeros_like(totals)
    tally[...] = jnp.zeros_like(tally)
    features_by = feature_weight[...].astype(bf16)

    def work(t, carry):
        slot = lax.rem(t, 2)
        g = first_chunk + t
        edge0 = g * CHUNK

        @pl.when(t + 1 < chunks)
        def _():
            start(t + 1)

        def gather(b, inner):
            for u in range(UNROLL):
                e = b * UNROLL + u
                tile[pl.ds(e, 4, stride=PITCH), :] = wide_row(rows, receivers[edge0 + e])
            return inner

        lax.fori_loop(0, CHUNK // UNROLL, gather, 0)
        pltpu.make_async_copy(
            latent.at[pl.ds(0, CHUNK)], arrived.at[slot], sems.at[slot]
        ).wait()
        before = (
            dot(arrived[slot], send_weight[...])
            + chunk_of(tile)
            + lax.dot_general(
                features[g], features_by, (((0,), (0,)), ((), ())), preferred_element_type=f32
            )
        )
        hidden = silu(before).astype(bf16)
        hot = jnp.where(
            lax.broadcasted_iota(jnp.int32, (nodes, CHUNK), 0) == ids[pl.ds(g, 1), :], 1.0, 0.0
        )
        totals[...] += dot(hot.astype(bf16), hidden)
        tally[...] += (hot[:, 0:128] + hot[:, 128:256]) + (hot[:, 256:384] + hot[:, 384:512])
        return carry

    lax.fori_loop(0, chunks, work, 0)
    counts = jnp.sum(tally[...], axis=1, keepdims=True)
    whole = totals[...]
    upper = whole.astype(bf16)
    lower = (whole - upper.astype(f32)).astype(bf16)
    totals[...] = (
        dot(upper, message_weight[...])
        + dot(lower, message_weight[...])
        + counts * message_bias[...]
    )
    for r in range(2):
        mine = pl.multiple_of(jnp.bitwise_xor(k, 2 * r) * 128, 128)
        theirs = pl.multiple_of(jnp.bitwise_xor(k, 2 * r + 1) * 128, 128)
        keep[r] = totals[:, pl.ds(mine, 128)]
        send[r] = totals[:, pl.ds(theirs, 128)]


VMEM = pl.BlockSpec(memory_space=pltpu.VMEM)
SMEM = pl.BlockSpec(memory_space=pltpu.SMEM)
ANY = pl.BlockSpec(memory_space=pl.ANY)


def embed_call(outer, chunks, own_columns, channels, operands):
    width = 512
    count = len(operands)
    specs = [SMEM] * 4 + [ANY] * (5 if outer else 1) + [VMEM] * 2
    if outer:
        specs = specs + [ANY]
    slots = SLOTS * WINDOW
    return pl.pallas_call(
        functools.partial(embed_kernel, outer, chunks, own_columns, channels),
        out_shape=jax.ShapeDtypeStruct((chunks * CHUNK, width), bf16),
        in_specs=specs,
        out_specs=ANY,
        input_output_aliases={count - 1: 0} if outer else {},
        scratch_shapes=[
            pltpu.VMEM((slots * LAT * 4, 128), f32),
            pltpu.VMEM((2, channels, LAT), bf16),
            pltpu.VMEM((4 * PITCH, 128), f32),
            pltpu.VMEM((2, CHUNK, width), bf16),
            pltpu.SMEM((16,), jnp.int32),
            pltpu.SMEM((32,), jnp.int32),
            pltpu.SMEM((8,), jnp.int32),
            pltpu.SemaphoreType.DMA((2,)),
            pltpu.SemaphoreType.DMA((2,)),
        ],
        compiler_params=pltpu.CompilerParams(vmem_limit_bytes=60 * 2**20),
        name="embed_outer" if outer else "embed_inner",
    )(*operands)


def edge_call(chunks, nodes, operands):
    width = 512
    part = jax.ShapeDtypeStruct((2, nodes, 128), f32)
    return pl.pallas_call(
        functools.partial(edge_kernel, chunks, nodes),
        out_shape=(part, part),
        in_specs=[SMEM] * 2 + [ANY] + [VMEM] * 11,
        out_specs=(VMEM, VMEM),
        scratch_shapes=[
            pltpu.VMEM((nodes * 4, 128), f32),
            pltpu.VMEM((4 * PITCH, 128), f32),
            pltpu.VMEM((2, CHUNK, width), bf16),
            pltpu.VMEM((width, width), bf16),
            pltpu.VMEM((width, width), bf16),
            pltpu.VMEM((width, width), bf16),
            pltpu.VMEM((nodes, width), bf16),
            pltpu.VMEM((4, width), f32),
            pltpu.VMEM((nodes, width), f32),
            pltpu.VMEM((nodes, 128), f32),
            pltpu.SemaphoreType.DMA((2,)),
        ],
        compiler_params=pltpu.CompilerParams(vmem_limit_bytes=56 * 2**20),
        name="edges",
    )(*operands)


def on_device(
    grid_inputs,
    embed_weight,
    embed_bias,
    mesh_latent,
    edge_features,
    senders,
    receivers,
    sender_weight,
    receiver_weight,
    feature_weight,
    hidden_bias,
    message_weight,
    message_bias,
    norm_gain,
    norm_shift,
):
    lon_count = lax.axis_size("lon")
    ch_count = lax.axis_size("ch")
    lon_place = lax.axis_index("lon")
    ch_place = lax.axis_index("ch")
    core = lax.bitwise_and(ch_place, 1)
    place = jnp.stack([ch_place, core]).astype(jnp.int32)
    points_own, channels = grid_inputs.shape
    own_columns = points_own // LAT
    mesh_nodes = mesh_latent.shape[0]
    full_width = message_weight.shape[1]
    edge_count = senders.shape[0]
    all_chunks = edge_count // CHUNK
    chunks = all_chunks // ch_count

    swap = [(i, i ^ 1) for i in range(ch_count)]
    across = [(i, i ^ 2) for i in range(ch_count)]
    facing = [
        (lon * ch_count + ch, (lon ^ 4) * ch_count + (ch ^ 2))
        for lon in range(lon_count)
        for ch in range(ch_count)
    ]
    forward = [(i, (i + 1) % lon_count) for i in range(lon_count)]
    backward = [(target, source) for source, target in forward]

    flat = grid_inputs.T
    half_points = HALO * LAT // 2
    low_half = lax.dynamic_slice_in_dim(
        flat, points_own - 2 * half_points + core * half_points, half_points, 1
    )
    high_half = lax.dynamic_slice_in_dim(flat, core * half_points, half_points, 1)
    low_own = lax.ppermute(low_half, "lon", forward)
    high_own = lax.ppermute(high_half, "lon", backward)
    low_swap = lax.ppermute(low_own, "ch", swap)
    high_swap = lax.ppermute(high_own, "ch", swap)

    part0 = lax.reduce_precision(hidden_bias, 8, 7)
    part1 = lax.reduce_precision(hidden_bias - part0, 8, 7)
    part2 = lax.reduce_precision(hidden_bias - part0 - part1, 8, 7)
    share = message_weight.shape[0]
    bundle = jnp.concatenate(
        [sender_weight, receiver_weight]
        + [message_weight[:, q * share : (q + 1) * share] for q in range(ch_count)]
        + [feature_weight, jnp.stack([part0, part1, part2]).astype(bf16)]
        + [jnp.zeros((9, share), bf16)],
        axis=0,
    )
    bundle_far = lax.ppermute(bundle, ("lon", "ch"), facing)
    bundle_near = lax.ppermute(bundle, "ch", swap)
    bundle_last = lax.ppermute(bundle_far, "ch", swap)
    mesh_far = lax.ppermute(mesh_latent, "ch", across)
    mesh_near = lax.ppermute(mesh_latent, "ch", swap)
    mesh_last = lax.ppermute(mesh_far, "ch", swap)

    points = jnp.mod(
        senders - lon_place * points_own + HALO * LAT, points_own * lon_count
    )
    by_chunk = points.reshape(all_chunks, CHUNK)
    low_column = jnp.min(by_chunk, axis=1) // LAT
    high_column = jnp.max(by_chunk, axis=1) // LAT
    local_recv = receivers - lon_place * mesh_nodes

    weight = jnp.pad(embed_weight, ((0, full_width - channels), (0, 0)))
    common = [place, points, low_column, high_column, flat]
    latent = embed_call(
        False, chunks, own_columns, channels, common + [weight, embed_bias[None, :]]
    )
    latent = embed_call(
        True, chunks, own_columns, channels,
        common + [low_own, low_swap, high_own, high_swap, weight, embed_bias[None, :], latent],
    )
    feature_blocks = jnp.transpose(
        edge_features.reshape(edge_features.shape[0], all_chunks, CHUNK), (1, 0, 2)
    )
    keep, send = edge_call(
        chunks, mesh_nodes,
        [place, local_recv, latent, local_recv.reshape(all_chunks, CHUNK), feature_blocks,
         bundle, bundle_near, bundle_far, bundle_last,
         mesh_latent, mesh_near, mesh_far, mesh_last, message_bias[None, :]],
    )
    halves = keep + lax.ppermute(send, "ch", swap)
    node_share = halves[0] + lax.ppermute(halves[1], "ch", across)
    first_sum, second = lax.psum(
        (
            jnp.sum(node_share, axis=1, keepdims=True),
            jnp.sum(jnp.square(node_share), axis=1, keepdims=True),
        ),
        "ch",
    )
    centre = first_sum / full_width
    spread = second / full_width - jnp.square(centre)
    normed = (node_share - centre) * lax.rsqrt(spread + 1.0)
    return (mesh_latent.astype(f32) + normed * norm_gain + norm_shift).astype(bf16)


def solution(mesh):
    return jax.shard_map(
        on_device,
        mesh=mesh,
        in_specs=(
            P("lon", None),
            P(),
            P(),
            P("lon", "ch"),
            P(None, "lon"),
            P("lon"),
            P("lon"),
            P(None, "ch"),
            P(None, "ch"),
            P(None, "ch"),
            P("ch"),
            P("ch", None),
            P(),
            P("ch"),
            P("ch"),
        ),
        out_specs=P("lon", "ch"),
        check_vma=False,
    )
```

```python
import functools

import jax
import jax.numpy as jnp
from jax import lax
from jax.experimental import pallas as pl
from jax.experimental.pallas import tpu as pltpu
from jax.sharding import PartitionSpec as P


LAT = 640
HALO = 4
CHUNK = 512
SLOTS = 4
WINDOW = 7
PITCH = CHUNK + 8
UNROLL = 32
BUFFERS = 4

f32 = jnp.float32
bf16 = jnp.bfloat16


def silu(value):
    half = 0.5 * value
    return half + half * jnp.tanh(half)


def dot(left, right):
    return jnp.dot(left, right, preferred_element_type=f32)


def wide_row(ref, index):
    return ref[pl.ds(pl.multiple_of(index, 4), 4), :]


def chunk_of(tile):
    return jnp.concatenate([tile[j * PITCH : j * PITCH + CHUNK, :] for j in range(4)], axis=1)


def list_chunks(chunks, low_ref, high_ref, own_columns, outer, chunk_list):
    def step(i, count):
        halo = (low_ref[i] < HALO) | (high_ref[i] >= HALO + own_columns)
        mine = halo if outer else jnp.logical_not(halo)

        @pl.when(mine)
        def _():
            chunk_list[count] = i

        return count + jnp.where(mine, 1, 0)

    return lax.fori_loop(0, chunks, step, 0)


def list_columns(count, first_chunk, low_ref, high_ref, chunk_list, column_list, offset_list):
    slot0 = lax.shift_right_logical(first_chunk, 2)
    total = jnp.int32(0)
    seg_first = jnp.int32(1000)
    seg_last = jnp.int32(-1)
    seg_start = jnp.int32(0)
    for slot in range(SLOTS):

        def step(t, carry):
            low, high = carry
            i = chunk_list[t]
            here = lax.shift_right_logical(first_chunk + i, 2) == slot0 + slot
            return (
                jnp.where(here, jnp.minimum(low, low_ref[i]), low),
                jnp.where(here, jnp.maximum(high, high_ref[i]), high),
            )

        low, high = lax.fori_loop(0, count, step, (jnp.int32(1000), jnp.int32(-1)))
        has = high >= 0
        joins = has & (low >= seg_first) & (low <= seg_last + 1)
        begin = jnp.where(joins, seg_last + 1, low)
        fresh = jnp.where(has, jnp.maximum(high - begin + 1, 0), 0)
        base = total

        def put(j, carry):
            column_list[base + j] = begin + j
            return carry

        lax.fori_loop(0, fresh, put, 0)
        opens = has & jnp.logical_not(joins)
        seg_start = jnp.where(opens, total, seg_start)
        seg_first = jnp.where(opens, low, seg_first)
        seg_last = jnp.where(opens, high, jnp.maximum(seg_last, high))
        total = total + fresh
        offset_list[slot] = (seg_start - seg_first) * (LAT * 4)
    return total


def block_kernel(outer, chunks, own_columns, channels, nodes, *refs):
    place, points, receivers, low_ref, high_ref, grid = refs[:6]
    refs = refs[6:]
    if outer:
        low_own, low_swap, high_own, high_swap = refs[:4]
        refs = refs[4:]
    embed_in, embed_bias, ids, features = refs[:4]
    bundles = refs[4:8]
    meshes = refs[8:12]
    refs = refs[12:]
    if outer:
        message_bias, first_totals, first_tally, *parts = refs[:7]
        totals, tally = refs[-2:]
        refs = refs[7:-2]
    else:
        totals, tally = refs[:2]
        refs = refs[2:]
    (table, columns, sent, got, inputs, rows, embed_weight, send_weight, recv_weight,
     message_weight, mesh, extras, chunk_list, column_list, offset_list, in_sems, sems) = refs
    k = place[0]
    core = place[1]
    first_chunk = k * chunks
    count = list_chunks(chunks, low_ref, high_ref, own_columns, outer, chunk_list)
    total = list_columns(
        count, first_chunk, low_ref, high_ref, chunk_list, column_list, offset_list
    )

    copies = []
    for j in range(4):
        lanes = pl.ds(j * 128, 128)
        copies.append((bundles[j].at[pl.ds(0, 512)], send_weight.at[:, lanes]))
        copies.append((bundles[j].at[pl.ds(512, 512)], recv_weight.at[:, lanes]))
        copies.append((bundles[j].at[pl.ds(1536, 16)], extras.at[j]))
        at = pl.multiple_of(jnp.bitwise_xor(k, j) * 128, 128)
        copies.append((meshes[j], mesh.at[:, pl.ds(at, 128)]))
    copies = [pltpu.make_async_copy(a, b, sems.at[n]) for n, (a, b) in enumerate(copies)]
    late = []
    if outer:
        for j in range(4):
            for q in range(4):
                late.append(
                    pltpu.make_async_copy(
                        bundles[j].at[pl.ds(1024 + q * 128, 128)],
                        message_weight.at[pl.ds(j * 128, 128), pl.ds(q * 128, 128)],
                        sems.at[16 + j * 4 + q],
                    )
                )
        for copy in late:
            copy.start()
        totals[...] = first_totals[...]
        tally[...] = first_tally[...]
    else:
        totals[...] = jnp.zeros_like(totals)
        tally[...] = jnp.zeros_like(tally)

    def fetch(source, column, slot):
        start = pl.multiple_of(column * LAT, 128)
        pltpu.make_async_copy(
            source.at[:, pl.ds(start, LAT)], columns.at[slot], in_sems.at[slot]
        ).start()

    def start_column(i):
        column = column_list[i]
        slot = lax.rem(i, BUFFERS)
        if not outer:
            fetch(grid, column - HALO, slot)
            return
        inside = (column >= HALO) & (column < HALO + own_columns)

        @pl.when(inside)
        def _():
            fetch(grid, column - HALO, slot)

        for is_side, shift, direct, swapped in (
            (column < HALO, 0, low_own, low_swap),
            (column >= HALO + own_columns, HALO + own_columns, high_own, high_swap),
        ):
            place_in = column - shift
            half = lax.shift_right_arithmetic(place_in, 1)
            within = lax.bitwise_and(place_in, 1)

            @pl.when(is_side & (half == core))
            def _():
                fetch(direct, within, slot)

            @pl.when(is_side & (half != core))
            def _():
                fetch(swapped, within, slot)

    def turn(i, carry):
        slot = lax.rem(i, BUFFERS)

        @pl.when(i + BUFFERS - 1 < total)
        def _():
            start_column(i + BUFFERS - 1)

        pltpu.make_async_copy(
            grid.at[:, pl.ds(0, LAT)], columns.at[slot], in_sems.at[slot]
        ).wait()
        source = columns.at[slot]
        for l in range(LAT // 128):
            lanes = pl.ds(l * 128, 128)
            for j in range(4):
                top = min(channels, (j + 1) * 128)
                block = source[j * 128 : top, lanes]
                if top < (j + 1) * 128:
                    block = jnp.pad(block, ((0, (j + 1) * 128 - top), (0, 0)))
                row = pl.multiple_of((i * LAT + l * 128) * 4, 8)
                table[pl.ds(row + j, 128, stride=4), :] = block.T.astype(f32)
        return carry

    def sender_place(t):
        i = chunk_list[t]
        slot = lax.shift_right_logical(first_chunk + i, 2) - lax.shift_right_logical(
            first_chunk, 2
        )
        return i * CHUNK, offset_list[slot]

    @pl.when(count > 0)
    def _():
        for b in range(BUFFERS - 1):

            @pl.when(b < total)
            def _():
                start_column(b)

        for copy in copies:
            copy.start()
        embed_weight[464:512, :] = jnp.zeros((48, 512), bf16)
        embed_weight[0:channels, :] = embed_in[...]
        lax.fori_loop(0, total, turn, 0)
        for copy in copies:
            copy.wait()
        bias = jnp.concatenate(
            [
                sum(extras[j, 4 + r : 5 + r, :].astype(f32) for r in range(3))
                for j in range(4)
            ],
            axis=1,
        )
        terms = dot(mesh[...], recv_weight[...]) + bias
        for j in range(4):
            rows[pl.ds(j, nodes, stride=4), :] = terms[:, j * 128 : (j + 1) * 128]
        edge0, offset = sender_place(0)

        def gather(b, inner):
            base = edge0 + b * UNROLL
            for u in range(UNROLL):
                sent[pl.ds(b * UNROLL + u, 4, stride=PITCH), :] = wide_row(
                    table, points[base + u] + offset
                )
            return inner

        lax.fori_loop(0, CHUNK // UNROLL, gather, 0)
        features_by = jnp.concatenate([extras[j, 0:4, :] for j in range(4)], axis=1)

        def work(t, carry):
            i = chunk_list[t]
            edge = i * CHUNK
            inputs[...] = chunk_of(sent).astype(bf16)
            for e in range(CHUNK):
                got[pl.ds(e, 4, stride=PITCH), :] = wide_row(rows, receivers[edge + e])
            latent = silu(dot(inputs[...], embed_weight[...]) + embed_bias[...]).astype(bf16)
            before = (
                dot(latent, send_weight[...])
                + chunk_of(got)
                + lax.dot_general(
                    features[first_chunk + i], features_by, (((0,), (0,)), ((), ())),
                    preferred_element_type=f32,
                )
            )
            hidden = silu(before).astype(bf16)
            hot = jnp.where(
                lax.broadcasted_iota(jnp.int32, (nodes, CHUNK), 0) * 4 == ids[pl.ds(i, 1), :],
                1.0,
                0.0,
            )
            next_edge, next_offset = sender_place(jnp.minimum(t + 1, count - 1))
            for e in range(CHUNK):
                sent[pl.ds(e, 4, stride=PITCH), :] = wide_row(
                    table, points[next_edge + e] + next_offset
                )
            totals[...] += dot(hot.astype(bf16), hidden)
            tally[...] += (hot[:, 0:128] + hot[:, 128:256]) + (hot[:, 256:384] + hot[:, 384:512])
            return carry

        lax.fori_loop(0, count, work, 0)

    if not outer:
        return
    counts = jnp.sum(tally[...], axis=1, keepdims=True)
    whole = totals[...]
    upper = whole.astype(bf16)
    lower = (whole - upper.astype(f32)).astype(bf16)
    for copy in late:
        copy.wait()
    totals[...] = (
        dot(upper, message_weight[...])
        + dot(lower, message_weight[...])
        + counts * message_bias[...]
    )
    for r in range(2):
        mine = pl.multiple_of(jnp.bitwise_xor(k, 2 * r) * 128, 128)
        theirs = pl.multiple_of(jnp.bitwise_xor(k, 2 * r + 1) * 128, 128)
        parts[r][...] = totals[:, pl.ds(mine, 128)]
        parts[2 + r][...] = totals[:, pl.ds(theirs, 128)]


VMEM = pl.BlockSpec(memory_space=pltpu.VMEM)
SMEM = pl.BlockSpec(memory_space=pltpu.SMEM)
ANY = pl.BlockSpec(memory_space=pl.ANY)


def block_call(outer, chunks, own_columns, channels, nodes, operands):
    width = 512
    part = jax.ShapeDtypeStruct((nodes, 128), f32)
    sums = (
        jax.ShapeDtypeStruct((nodes, width), f32),
        jax.ShapeDtypeStruct((nodes, 128), f32),
    )
    specs = [SMEM] * 5 + [ANY] * (5 if outer else 1) + [VMEM] * 4 + [ANY] * 8
    if outer:
        specs = specs + [VMEM] * 3
    slots = SLOTS * WINDOW
    edges = chunks * CHUNK
    square = pltpu.VMEM((width, width), bf16)
    return pl.pallas_call(
        functools.partial(block_kernel, outer, chunks, own_columns, channels, nodes),
        out_shape=(part,) * 4 if outer else sums,
        in_specs=specs,
        out_specs=(VMEM,) * (4 if outer else 2),
        scratch_shapes=[
            pltpu.VMEM((slots * LAT * 4, 128), f32),
            pltpu.VMEM((BUFFERS, channels, LAT), bf16),
            pltpu.VMEM((4 * PITCH, 128), f32),
            pltpu.VMEM((4 * PITCH, 128), f32),
            pltpu.VMEM((CHUNK, width), bf16),
            pltpu.VMEM((nodes * 4, 128), f32),
            square,
            square,
            square,
            square,
            pltpu.VMEM((nodes, width), bf16),
            pltpu.VMEM((4, 16, 128), bf16),
            pltpu.SMEM((16,), jnp.int32),
            pltpu.SMEM((32,), jnp.int32),
            pltpu.SMEM((8,), jnp.int32),
            pltpu.SemaphoreType.DMA((BUFFERS,)),
            pltpu.SemaphoreType.DMA((32,)),
        ]
        + ([pltpu.VMEM(value.shape, f32) for value in sums] if outer else []),
        compiler_params=pltpu.CompilerParams(vmem_limit_bytes=60 * 2**20),
        cost_estimate=pl.CostEstimate(
            flops=2 * edges * width * (2 * width + nodes),
            bytes_accessed=2 * edges * width,
            transcendentals=2 * edges * width,
        ),
        name="block_outer" if outer else "block_inner",
    )(*operands)


def encoder(
    grid_inputs,
    embed_weight,
    embed_bias,
    mesh_latent,
    edge_features,
    senders,
    receivers,
    sender_weight,
    receiver_weight,
    feature_weight,
    hidden_bias,
    message_weight,
    message_bias,
    norm_gain,
    norm_shift,
):
    lon_count = lax.axis_size("lon")
    ch_count = lax.axis_size("ch")
    lon_place = lax.axis_index("lon")
    ch_place = lax.axis_index("ch")
    core = lax.bitwise_and(ch_place, 1)
    place = jnp.stack([ch_place, core]).astype(jnp.int32)
    points_own, channels = grid_inputs.shape
    own_columns = points_own // LAT
    mesh_nodes = mesh_latent.shape[0]
    full_width = message_weight.shape[1]
    edge_count = senders.shape[0]
    all_chunks = edge_count // CHUNK
    chunks = all_chunks // ch_count

    swap = [(i, i ^ 1) for i in range(ch_count)]
    across = [(i, i ^ 2) for i in range(ch_count)]
    facing = [
        (lon * ch_count + ch, (lon ^ 4) * ch_count + (ch ^ 2))
        for lon in range(lon_count)
        for ch in range(ch_count)
    ]
    forward = [(i, (i + 1) % lon_count) for i in range(lon_count)]
    backward = [(target, source) for source, target in forward]

    flat = grid_inputs.T
    half_points = HALO * LAT // 2
    low_half = lax.dynamic_slice_in_dim(
        flat, points_own - 2 * half_points + core * half_points, half_points, 1
    )
    high_half = lax.dynamic_slice_in_dim(flat, core * half_points, half_points, 1)
    low_own = lax.ppermute(low_half, "lon", forward)
    high_own = lax.ppermute(high_half, "lon", backward)
    low_swap = lax.ppermute(low_own, "ch", swap)
    high_swap = lax.ppermute(high_own, "ch", swap)

    part0 = lax.reduce_precision(hidden_bias, 8, 7)
    part1 = lax.reduce_precision(hidden_bias - part0, 8, 7)
    part2 = lax.reduce_precision(hidden_bias - part0 - part1, 8, 7)
    share = message_weight.shape[0]
    bundle = jnp.concatenate(
        [sender_weight, receiver_weight]
        + [message_weight[:, q * share : (q + 1) * share] for q in range(ch_count)]
        + [feature_weight, jnp.stack([part0, part1, part2]).astype(bf16)]
        + [jnp.zeros((9, share), bf16)],
        axis=0,
    )
    bundle_far = lax.ppermute(bundle, ("lon", "ch"), facing)
    bundle_near = lax.ppermute(bundle, "ch", swap)
    bundle_last = lax.ppermute(bundle_far, "ch", swap)
    mesh_far = lax.ppermute(mesh_latent, "ch", across)
    mesh_near = lax.ppermute(mesh_latent, "ch", swap)
    mesh_last = lax.ppermute(mesh_far, "ch", swap)

    own_senders, own_receivers = (
        lax.dynamic_slice_in_dim(ends.reshape(all_chunks, CHUNK), ch_place * chunks, chunks, 0)
        for ends in (senders, receivers)
    )
    points = jnp.mod(
        own_senders - lon_place * points_own + HALO * LAT, points_own * lon_count
    )
    low_column = jnp.min(points, axis=1) // LAT
    high_column = jnp.max(points, axis=1) // LAT
    ids = (own_receivers - lon_place * mesh_nodes) * 4
    feature_blocks = jnp.transpose(
        edge_features.reshape(edge_features.shape[0], all_chunks, CHUNK), (1, 0, 2)
    )

    call = functools.partial(
        block_call, chunks=chunks, own_columns=own_columns, channels=channels, nodes=mesh_nodes
    )
    scalars = [place, (points * 4).reshape(-1), ids.reshape(-1), low_column, high_column, flat]
    arrays = [
        embed_weight, embed_bias[None, :], ids, feature_blocks,
        bundle, bundle_near, bundle_far, bundle_last,
        mesh_latent, mesh_near, mesh_far, mesh_last,
    ]
    totals, tally = call(False, operands=scalars + arrays)
    keep_here, keep_far, send_here, send_far = call(
        True,
        operands=scalars
        + [low_own, low_swap, high_own, high_swap]
        + arrays
        + [message_bias[None, :], totals, tally],
    )
    far = keep_far + lax.ppermute(send_far, "ch", swap)
    far = lax.ppermute(far.astype(bf16), "ch", across).astype(f32)
    node_share = keep_here + lax.ppermute(send_here, "ch", swap) + far
    first_sum, second = lax.psum(
        (
            jnp.sum(node_share, axis=1, keepdims=True),
            jnp.sum(jnp.square(node_share), axis=1, keepdims=True),
        ),
        "ch",
    )
    centre = first_sum / full_width
    spread = second / full_width - jnp.square(centre)
    normed = (node_share - centre) * lax.rsqrt(spread + 1.0)
    return (mesh_latent.astype(f32) + normed * norm_gain + norm_shift).astype(bf16)


def solution(mesh):
    return jax.shard_map(
        encoder,
        mesh=mesh,
        in_specs=(
            P("lon", None),
            P(),
            P(),
            P("lon", "ch"),
            P(None, "lon"),
            P("lon"),
            P("lon"),
            P(None, "ch"),
            P(None, "ch"),
            P(None, "ch"),
            P("ch"),
            P("ch", None),
            P(),
            P("ch"),
            P("ch"),
        ),
        out_specs=P("lon", "ch"),
        check_vma=False,
    )
```

```python
import functools

import jax
import jax.numpy as jnp
from jax import lax
from jax.experimental import pallas as pl
from jax.experimental.pallas import tpu as pltpu
from jax.sharding import PartitionSpec as P


LAT = 640
HALO = 4
CHUNK = 512
SLOTS = 4
WINDOW = 7
PITCH = CHUNK + 8
UNROLL = 32
BUFFERS = 4
LIMIT = 6

f32 = jnp.float32
bf16 = jnp.bfloat16


def silu(value):
    half = 0.5 * value
    return half + half * jnp.tanh(half)


def dot(left, right):
    return jnp.dot(left, right, preferred_element_type=f32)


def wide_row(ref, index):
    return ref[pl.ds(pl.multiple_of(index, 4), 4), :]


def chunk_of(tile):
    return jnp.concatenate([tile[j * PITCH : j * PITCH + CHUNK, :] for j in range(4)], axis=1)


def list_chunks(chunks, low_ref, high_ref, own_columns, outer, chunk_list):
    def step(i, counts):
        inner_count, outer_count = counts
        halo = (low_ref[i] < HALO) | (high_ref[i] >= HALO + own_columns)
        early = jnp.logical_not(halo) & (inner_count < LIMIT)
        count = outer_count if outer else inner_count

        @pl.when(jnp.logical_not(early) if outer else early)
        def _():
            chunk_list[count] = i

        return inner_count + jnp.where(early, 1, 0), outer_count + jnp.where(early, 0, 1)

    return lax.fori_loop(0, chunks, step, (jnp.int32(0), jnp.int32(0)))[1 if outer else 0]


def list_columns(count, first_chunk, low_ref, high_ref, chunk_list, column_list, offset_list):
    slot0 = lax.shift_right_logical(first_chunk, 2)
    total = jnp.int32(0)
    seg_first = jnp.int32(1000)
    seg_last = jnp.int32(-1)
    seg_start = jnp.int32(0)
    for slot in range(SLOTS):

        def step(t, carry):
            low, high = carry
            i = chunk_list[t]
            here = lax.shift_right_logical(first_chunk + i, 2) == slot0 + slot
            return (
                jnp.where(here, jnp.minimum(low, low_ref[i]), low),
                jnp.where(here, jnp.maximum(high, high_ref[i]), high),
            )

        low, high = lax.fori_loop(0, count, step, (jnp.int32(1000), jnp.int32(-1)))
        has = high >= 0
        joins = has & (low >= seg_first) & (low <= seg_last + 1)
        begin = jnp.where(joins, seg_last + 1, low)
        fresh = jnp.where(has, jnp.maximum(high - begin + 1, 0), 0)
        base = total

        def put(j, carry):
            column_list[base + j] = begin + j
            return carry

        lax.fori_loop(0, fresh, put, 0)
        opens = has & jnp.logical_not(joins)
        seg_start = jnp.where(opens, total, seg_start)
        seg_first = jnp.where(opens, low, seg_first)
        seg_last = jnp.where(opens, high, jnp.maximum(seg_last, high))
        total = total + fresh
        offset_list[slot] = (seg_start - seg_first) * (LAT * 4)
    return total


def block_kernel(outer, chunks, own_columns, channels, nodes, *refs):
    place, points, receivers, low_ref, high_ref, grid = refs[:6]
    refs = refs[6:]
    if outer:
        low_own, low_swap, high_own, high_swap = refs[:4]
        refs = refs[4:]
    embed_in, embed_bias, ids, features = refs[:4]
    bundles = refs[4:8]
    meshes = refs[8:12]
    refs = refs[12:]
    if outer:
        message_bias, first_totals, first_tally, *parts = refs[:7]
        totals, tally = refs[-2:]
        refs = refs[7:-2]
    else:
        totals, tally = refs[:2]
        refs = refs[2:]
    (table, columns, sent, got, inputs, rows, embed_weight, send_weight, recv_weight,
     message_weight, mesh, extras, chunk_list, column_list, offset_list, in_sems, sems) = refs
    k = place[0]
    core = lax.bitwise_and(k, 1)
    first_chunk = k * chunks
    count = list_chunks(chunks, low_ref, high_ref, own_columns, outer, chunk_list)
    total = list_columns(
        count, first_chunk, low_ref, high_ref, chunk_list, column_list, offset_list
    )

    copies = []
    for j in range(4):
        lanes = pl.ds(j * 128, 128)
        copies.append((bundles[j].at[pl.ds(0, 512)], send_weight.at[:, lanes]))
        copies.append((bundles[j].at[pl.ds(512, 512)], recv_weight.at[:, lanes]))
        copies.append((bundles[j].at[pl.ds(1536, 16)], extras.at[j]))
        at = pl.multiple_of(jnp.bitwise_xor(k, j) * 128, 128)
        copies.append((meshes[j], mesh.at[:, pl.ds(at, 128)]))
    copies = [pltpu.make_async_copy(a, b, sems.at[n]) for n, (a, b) in enumerate(copies)]
    late = []
    if outer:
        for j in range(4):
            for q in range(4):
                late.append(
                    pltpu.make_async_copy(
                        bundles[j].at[pl.ds(1024 + q * 128, 128)],
                        message_weight.at[pl.ds(j * 128, 128), pl.ds(q * 128, 128)],
                        sems.at[16 + j * 4 + q],
                    )
                )
        for copy in late:
            copy.start()
        totals[...] = first_totals[...]
        tally[...] = first_tally[...]
    else:
        totals[...] = jnp.zeros_like(totals)
        tally[...] = jnp.zeros_like(tally)

    def fetch(source, column, slot):
        start = pl.multiple_of(column * LAT, 128)
        pltpu.make_async_copy(
            source.at[:, pl.ds(start, LAT)], columns.at[slot], in_sems.at[slot]
        ).start()

    def start_column(i):
        column = column_list[i]
        slot = lax.rem(i, BUFFERS)
        if not outer:
            fetch(grid, column - HALO, slot)
            return
        inside = (column >= HALO) & (column < HALO + own_columns)

        @pl.when(inside)
        def _():
            fetch(grid, column - HALO, slot)

        for is_side, shift, direct, swapped in (
            (column < HALO, 0, low_own, low_swap),
            (column >= HALO + own_columns, HALO + own_columns, high_own, high_swap),
        ):
            place_in = column - shift
            half = lax.shift_right_arithmetic(place_in, 1)
            within = lax.bitwise_and(place_in, 1)

            @pl.when(is_side & (half == core))
            def _():
                fetch(direct, within, slot)

            @pl.when(is_side & (half != core))
            def _():
                fetch(swapped, within, slot)

    def turn(i, carry):
        slot = lax.rem(i, BUFFERS)

        @pl.when(i + BUFFERS - 1 < total)
        def _():
            start_column(i + BUFFERS - 1)

        pltpu.make_async_copy(
            grid.at[:, pl.ds(0, LAT)], columns.at[slot], in_sems.at[slot]
        ).wait()
        source = columns.at[slot]
        for l in range(LAT // 128):
            lanes = pl.ds(l * 128, 128)
            for j in range(4):
                top = min(channels, (j + 1) * 128)
                block = source[j * 128 : top, lanes]
                if top < (j + 1) * 128:
                    block = jnp.pad(block, ((0, (j + 1) * 128 - top), (0, 0)))
                row = pl.multiple_of((i * LAT + l * 128) * 4, 8)
                table[pl.ds(row + j, 128, stride=4), :] = block.T.astype(f32)
        return carry

    def sender_place(t):
        i = chunk_list[t]
        slot = lax.shift_right_logical(first_chunk + i, 2) - lax.shift_right_logical(
            first_chunk, 2
        )
        return i * CHUNK, offset_list[slot]

    @pl.when(count > 0)
    def _():
        for b in range(BUFFERS - 1):

            @pl.when(b < total)
            def _():
                start_column(b)

        for copy in copies:
            copy.start()
        embed_weight[464:512, :] = jnp.zeros((48, 512), bf16)
        embed_weight[0:channels, :] = embed_in[...]
        lax.fori_loop(0, total, turn, 0)
        for copy in copies:
            copy.wait()
        bias = jnp.concatenate(
            [
                sum(extras[j, 4 + r : 5 + r, :].astype(f32) for r in range(3))
                for j in range(4)
            ],
            axis=1,
        )
        terms = dot(mesh[...], recv_weight[...]) + bias
        for j in range(4):
            rows[pl.ds(j, nodes, stride=4), :] = terms[:, j * 128 : (j + 1) * 128]
        edge0, offset = sender_place(0)

        def gather(b, inner):
            base = edge0 + b * UNROLL
            for u in range(UNROLL):
                sent[pl.ds(b * UNROLL + u, 4, stride=PITCH), :] = wide_row(
                    table, points[base + u] + offset
                )
            return inner

        lax.fori_loop(0, CHUNK // UNROLL, gather, 0)
        features_by = jnp.concatenate([extras[j, 0:4, :] for j in range(4)], axis=1)

        def work(t, carry):
            i = chunk_list[t]
            edge = i * CHUNK
            inputs[...] = chunk_of(sent).astype(bf16)
            for e in range(CHUNK):
                got[pl.ds(e, 4, stride=PITCH), :] = wide_row(rows, receivers[edge + e])
            latent = silu(dot(inputs[...], embed_weight[...]) + embed_bias[...]).astype(bf16)
            before = (
                dot(latent, send_weight[...])
                + chunk_of(got)
                + lax.dot_general(
                    features[first_chunk + i], features_by, (((0,), (0,)), ((), ())),
                    preferred_element_type=f32,
                )
            )
            hidden = silu(before).astype(bf16)
            node = lax.broadcasted_iota(jnp.int32, (nodes, 128), 0) * 4
            hots = [
                jnp.where(node == ids[pl.ds(i * 4 + q, 1), :], 1.0, 0.0) for q in range(4)
            ]
            hot = jnp.concatenate([value.astype(bf16) for value in hots], axis=1)
            next_edge, next_offset = sender_place(jnp.minimum(t + 1, count - 1))
            for e in range(CHUNK):
                sent[pl.ds(e, 4, stride=PITCH), :] = wide_row(
                    table, points[next_edge + e] + next_offset
                )
            totals[...] += dot(hot, hidden)
            tally[...] += (hots[0] + hots[1]) + (hots[2] + hots[3])
            return carry

        lax.fori_loop(0, count, work, 0)

    if not outer:
        return
    counts = jnp.sum(tally[...], axis=1, keepdims=True)
    whole = totals[...]
    upper = whole.astype(bf16)
    lower = (whole - upper.astype(f32)).astype(bf16)
    for copy in late:
        copy.wait()
    totals[...] = (
        dot(upper, message_weight[...])
        + dot(lower, message_weight[...])
        + counts * message_bias[...]
    )
    for r in range(2):
        mine = pl.multiple_of(jnp.bitwise_xor(k, 2 * r) * 128, 128)
        theirs = pl.multiple_of(jnp.bitwise_xor(k, 2 * r + 1) * 128, 128)
        parts[r][...] = totals[:, pl.ds(mine, 128)]
        parts[2 + r][...] = totals[:, pl.ds(theirs, 128)]


def pack_kernel(chunks, points_own, all_points, nodes, share, place, senders, receivers,
                feature_weight, hidden_bias, grid, sender_weight, receiver_weight, message_weight,
                points, ids, low_ref, high_ref, bundle, low_half, high_half, extra, sems):
    lon = place[0]
    k = place[1]
    half = HALO * LAT // 2
    side = lax.bitwise_and(k, 1) * half
    low_at = pl.multiple_of(points_own - 2 * half + side, 128)
    copies = [
        (sender_weight, bundle.at[pl.ds(0, 512)]),
        (receiver_weight, bundle.at[pl.ds(512, 512)]),
        (grid.at[:, pl.ds(low_at, half)], low_half),
        (grid.at[:, pl.ds(pl.multiple_of(side, 128), half)], high_half),
    ]
    for q in range(4):
        copies.append(
            (
                message_weight.at[:, pl.ds(q * share, share)],
                bundle.at[pl.ds(1024 + q * share, share)],
            )
        )
    copies = [pltpu.make_async_copy(a, b, sems.at[n]) for n, (a, b) in enumerate(copies)]
    for copy in copies:
        copy.start()
    bias = hidden_bias[...]
    upper = bias.astype(bf16)
    middle = (bias - upper.astype(f32)).astype(bf16)
    lower = (bias - upper.astype(f32) - middle.astype(f32)).astype(bf16)
    extra[...] = jnp.concatenate(
        [feature_weight[...].astype(f32)]
        + [value.astype(f32) for value in (upper, middle, lower)]
        + [jnp.zeros((9, share), f32)],
        axis=0,
    ).astype(bf16)
    last = pltpu.make_async_copy(extra, bundle.at[pl.ds(1536, 16)], sems.at[len(copies)])
    last.start()
    for i in range(chunks):
        rows = pl.ds(pl.multiple_of((k * chunks + i) * 4, 4), 4)
        point = senders[rows, :] - lon * points_own + HALO * LAT
        point = jnp.where(point < 0, point + all_points, point)
        point = jnp.where(point >= all_points, point - all_points, point)
        points[i * 4 : i * 4 + 4, :] = point * 4
        ids[i * 4 : i * 4 + 4, :] = (receivers[rows, :] - lon * nodes) * 4
        for ref, end in ((low_ref, jnp.min(point)), (high_ref, jnp.max(point))):
            ref[i] = lax.shift_right_logical(lax.shift_right_logical(end, 7) * 13108, 16)
    for copy in copies:
        copy.wait()
    last.wait()


def pack_call(chunks, points_own, all_points, channels, nodes, share, operands):
    half = HALO * LAT // 2
    index = jax.ShapeDtypeStruct((chunks * 4, 128), jnp.int32)
    ends = jax.ShapeDtypeStruct((chunks,), jnp.int32)
    side = jax.ShapeDtypeStruct((channels, half), bf16)
    return pl.pallas_call(
        functools.partial(pack_kernel, chunks, points_own, all_points, nodes, share),
        out_shape=(
            index, index, ends, ends, jax.ShapeDtypeStruct((1552, share), bf16), side, side,
        ),
        in_specs=[SMEM] + [VMEM] * 4 + [ANY] * 4,
        out_specs=(VMEM, VMEM, SMEM, SMEM, ANY, ANY, ANY),
        scratch_shapes=[pltpu.VMEM((16, share), bf16), pltpu.SemaphoreType.DMA((9,))],
        name="pack",
    )(*operands)


VMEM = pl.BlockSpec(memory_space=pltpu.VMEM)
SMEM = pl.BlockSpec(memory_space=pltpu.SMEM)
ANY = pl.BlockSpec(memory_space=pl.ANY)


def block_call(outer, chunks, own_columns, channels, nodes, operands):
    width = 512
    part = jax.ShapeDtypeStruct((nodes, 128), f32)
    sums = (
        jax.ShapeDtypeStruct((nodes, width), f32),
        jax.ShapeDtypeStruct((nodes, 128), f32),
    )
    specs = [SMEM] * 5 + [ANY] * (5 if outer else 1) + [VMEM] * 4 + [ANY] * 8
    if outer:
        specs = specs + [VMEM] * 3
    slots = SLOTS * WINDOW
    edges = chunks * CHUNK
    square = pltpu.VMEM((width, width), bf16)
    return pl.pallas_call(
        functools.partial(block_kernel, outer, chunks, own_columns, channels, nodes),
        out_shape=(part,) * 4 if outer else sums,
        in_specs=specs,
        out_specs=(VMEM,) * (4 if outer else 2),
        scratch_shapes=[
            pltpu.VMEM((slots * LAT * 4, 128), f32),
            pltpu.VMEM((BUFFERS, channels, LAT), bf16),
            pltpu.VMEM((4 * PITCH, 128), f32),
            pltpu.VMEM((4 * PITCH, 128), f32),
            pltpu.VMEM((CHUNK, width), bf16),
            pltpu.VMEM((nodes * 4, 128), f32),
            square,
            square,
            square,
            square,
            pltpu.VMEM((nodes, width), bf16),
            pltpu.VMEM((4, 16, 128), bf16),
            pltpu.SMEM((16,), jnp.int32),
            pltpu.SMEM((32,), jnp.int32),
            pltpu.SMEM((8,), jnp.int32),
            pltpu.SemaphoreType.DMA((BUFFERS,)),
            pltpu.SemaphoreType.DMA((32,)),
        ]
        + ([pltpu.VMEM(value.shape, f32) for value in sums] if outer else []),
        compiler_params=pltpu.CompilerParams(vmem_limit_bytes=60 * 2**20),
        cost_estimate=pl.CostEstimate(
            flops=2 * edges * width * (2 * width + nodes),
            bytes_accessed=2 * edges * width,
            transcendentals=2 * edges * width,
        ),
        name="block_outer" if outer else "block_inner",
    )(*operands)


def encoder(
    grid_inputs,
    embed_weight,
    embed_bias,
    mesh_latent,
    edge_features,
    senders,
    receivers,
    sender_weight,
    receiver_weight,
    feature_weight,
    hidden_bias,
    message_weight,
    message_bias,
    norm_gain,
    norm_shift,
):
    lon_count = lax.axis_size("lon")
    ch_count = lax.axis_size("ch")
    lon_place = lax.axis_index("lon")
    ch_place = lax.axis_index("ch")
    place = ch_place[None].astype(jnp.int32)
    points_own, channels = grid_inputs.shape
    own_columns = points_own // LAT
    mesh_nodes = mesh_latent.shape[0]
    full_width = message_weight.shape[1]
    edge_count = senders.shape[0]
    all_chunks = edge_count // CHUNK
    chunks = all_chunks // ch_count

    swap = [(i, i ^ 1) for i in range(ch_count)]
    across = [(i, i ^ 2) for i in range(ch_count)]
    facing = [
        (lon * ch_count + ch, (lon ^ 4) * ch_count + (ch ^ 2))
        for lon in range(lon_count)
        for ch in range(ch_count)
    ]
    forward = [(i, (i + 1) % lon_count) for i in range(lon_count)]
    backward = [(target, source) for source, target in forward]

    flat = grid_inputs.T
    points, ids, low_column, high_column, bundle, low_half, high_half = pack_call(
        chunks, points_own, points_own * lon_count, channels, mesh_nodes,
        message_weight.shape[0],
        [
            jnp.stack([lon_place, ch_place]).astype(jnp.int32),
            senders.reshape(-1, 128),
            receivers.reshape(-1, 128),
            feature_weight,
            hidden_bias[None, :],
            flat,
            sender_weight,
            receiver_weight,
            message_weight,
        ],
    )
    mesh_far = lax.ppermute(mesh_latent, "ch", across)
    bundle_far = lax.ppermute(bundle, ("lon", "ch"), facing)
    low_own = lax.ppermute(low_half, "lon", forward)
    high_own = lax.ppermute(high_half, "lon", backward)
    low_swap = lax.ppermute(low_own, "ch", swap)
    high_swap = lax.ppermute(high_own, "ch", swap)
    bundle_near = lax.ppermute(bundle, "ch", swap)
    bundle_last = lax.ppermute(bundle_far, "ch", swap)
    mesh_near = lax.ppermute(mesh_latent, "ch", swap)
    mesh_last = lax.ppermute(mesh_far, "ch", swap)
    feature_blocks = jnp.transpose(
        edge_features.reshape(edge_features.shape[0], all_chunks, CHUNK), (1, 0, 2)
    )

    call = functools.partial(
        block_call, chunks=chunks, own_columns=own_columns, channels=channels, nodes=mesh_nodes
    )
    scalars = [place, points.reshape(-1), ids.reshape(-1), low_column, high_column, flat]
    arrays = [
        embed_weight, embed_bias[None, :], ids, feature_blocks,
        bundle, bundle_near, bundle_far, bundle_last,
        mesh_latent, mesh_near, mesh_far, mesh_last,
    ]
    totals, tally = call(False, operands=scalars + arrays)
    keep_here, keep_far, send_here, send_far = call(
        True,
        operands=scalars
        + [low_own, low_swap, high_own, high_swap]
        + arrays
        + [message_bias[None, :], totals, tally],
    )
    far = keep_far + lax.ppermute(send_far, "ch", swap)
    far = lax.ppermute(far.astype(bf16), "ch", across).astype(f32)
    node_share = keep_here + lax.ppermute(send_here, "ch", swap) + far
    first_sum, second = lax.psum(
        (
            jnp.sum(node_share, axis=1, keepdims=True),
            jnp.sum(jnp.square(node_share), axis=1, keepdims=True),
        ),
        "ch",
    )
    centre = first_sum / full_width
    spread = second / full_width - jnp.square(centre)
    normed = (node_share - centre) * lax.rsqrt(spread + 1.0)
    return (mesh_latent.astype(f32) + normed * norm_gain + norm_shift).astype(bf16)


def solution(mesh):
    return jax.shard_map(
        encoder,
        mesh=mesh,
        in_specs=(
            P("lon", None),
            P(),
            P(),
            P("lon", "ch"),
            P(None, "lon"),
            P("lon"),
            P("lon"),
            P(None, "ch"),
            P(None, "ch"),
            P(None, "ch"),
            P("ch"),
            P("ch", None),
            P(),
            P("ch"),
            P("ch"),
        ),
        out_specs=P("lon", "ch"),
        check_vma=False,
    )
```

```python
import functools

import jax
import jax.numpy as jnp
from jax import lax
from jax.experimental import pallas as pl
from jax.experimental.pallas import tpu as pltpu
from jax.sharding import PartitionSpec as P


LAT = 640
HALO = 4
CHUNK = 512
SLOTS = 4
WINDOW = 7
PITCH = CHUNK + 8
UNROLL = 32
BUFFERS = 4
LIMIT = 6

f32 = jnp.float32
bf16 = jnp.bfloat16


def silu(value):
    half = 0.5 * value
    return half + half * jnp.tanh(half)


def dot(left, right):
    return jnp.dot(left, right, preferred_element_type=f32)


def wide_row(ref, index):
    return ref[pl.ds(pl.multiple_of(index, 4), 4), :]


def chunk_of(tile):
    return jnp.concatenate([tile[j * PITCH : j * PITCH + CHUNK, :] for j in range(4)], axis=1)


def list_chunks(chunks, low_ref, high_ref, own_columns, outer, chunk_list):
    def step(i, counts):
        inner_count, outer_count = counts
        halo = (low_ref[i] < HALO) | (high_ref[i] >= HALO + own_columns)
        early = jnp.logical_not(halo) & (inner_count < LIMIT)
        count = outer_count if outer else inner_count

        @pl.when(jnp.logical_not(early) if outer else early)
        def _():
            chunk_list[count] = i

        return inner_count + jnp.where(early, 1, 0), outer_count + jnp.where(early, 0, 1)

    return lax.fori_loop(0, chunks, step, (jnp.int32(0), jnp.int32(0)))[1 if outer else 0]


def list_columns(count, first_chunk, low_ref, high_ref, chunk_list, column_list, offset_list):
    slot0 = lax.shift_right_logical(first_chunk, 2)
    total = jnp.int32(0)
    seg_first = jnp.int32(1000)
    seg_last = jnp.int32(-1)
    seg_start = jnp.int32(0)
    for slot in range(SLOTS):

        def step(t, carry):
            low, high = carry
            i = chunk_list[t]
            here = lax.shift_right_logical(first_chunk + i, 2) == slot0 + slot
            return (
                jnp.where(here, jnp.minimum(low, low_ref[i]), low),
                jnp.where(here, jnp.maximum(high, high_ref[i]), high),
            )

        low, high = lax.fori_loop(0, count, step, (jnp.int32(1000), jnp.int32(-1)))
        has = high >= 0
        joins = has & (low >= seg_first) & (low <= seg_last + 1)
        begin = jnp.where(joins, seg_last + 1, low)
        fresh = jnp.where(has, jnp.maximum(high - begin + 1, 0), 0)
        base = total

        def put(j, carry):
            column_list[base + j] = begin + j
            return carry

        lax.fori_loop(0, fresh, put, 0)
        opens = has & jnp.logical_not(joins)
        seg_start = jnp.where(opens, total, seg_start)
        seg_first = jnp.where(opens, low, seg_first)
        seg_last = jnp.where(opens, high, jnp.maximum(seg_last, high))
        total = total + fresh
        offset_list[slot] = (seg_start - seg_first) * (LAT * 4)
    return total


def block_kernel(outer, chunks, own_columns, channels, nodes, *refs):
    place, points, receivers, low_ref, high_ref, grid = refs[:6]
    refs = refs[6:]
    if outer:
        low_own, low_swap, high_own, high_swap = refs[:4]
        refs = refs[4:]
    embed_in, embed_bias, ids, features = refs[:4]
    bundles = refs[4:8]
    meshes = refs[8:12]
    refs = refs[12:]
    if outer:
        messages = refs[:4]
        refs = refs[4:]
        message_bias, first_totals, first_tally, *parts = refs[:7]
        totals, tally = refs[-2:]
        refs = refs[7:-2]
    else:
        totals, tally = refs[:2]
        refs = refs[2:]
    (table, columns, sent, got, inputs, rows, embed_weight, send_weight, recv_weight,
     message_weight, mesh, extras, chunk_list, column_list, offset_list, in_sems, sems) = refs
    k = place[0]
    core = lax.bitwise_and(k, 1)
    first_chunk = k * chunks
    count = list_chunks(chunks, low_ref, high_ref, own_columns, outer, chunk_list)
    total = list_columns(
        count, first_chunk, low_ref, high_ref, chunk_list, column_list, offset_list
    )

    copies = []
    for j in range(4):
        lanes = pl.ds(j * 128, 128)
        copies.append((bundles[j].at[pl.ds(0, 512)], send_weight.at[:, lanes]))
        copies.append((bundles[j].at[pl.ds(512, 512)], recv_weight.at[:, lanes]))
        copies.append((bundles[j].at[pl.ds(1024, 16)], extras.at[j]))
        at = pl.multiple_of(jnp.bitwise_xor(k, j) * 128, 128)
        copies.append((meshes[j], mesh.at[:, pl.ds(at, 128)]))
    copies = [pltpu.make_async_copy(a, b, sems.at[n]) for n, (a, b) in enumerate(copies)]
    late = []
    if outer:
        for j in range(4):
            late.append(
                pltpu.make_async_copy(
                    messages[j], message_weight.at[pl.ds(j * 128, 128)], sems.at[16 + j]
                )
            )
        for copy in late:
            copy.start()
        totals[...] = first_totals[...]
        tally[...] = first_tally[...]
    else:
        totals[...] = jnp.zeros_like(totals)
        tally[...] = jnp.zeros_like(tally)

    def fetch(source, column, slot):
        start = pl.multiple_of(column * LAT, 128)
        pltpu.make_async_copy(
            source.at[:, pl.ds(start, LAT)], columns.at[slot], in_sems.at[slot]
        ).start()

    def start_column(i):
        column = column_list[i]
        slot = lax.rem(i, BUFFERS)
        if not outer:
            fetch(grid, column - HALO, slot)
            return
        inside = (column >= HALO) & (column < HALO + own_columns)

        @pl.when(inside)
        def _():
            fetch(grid, column - HALO, slot)

        for is_side, shift, direct, swapped in (
            (column < HALO, 0, low_own, low_swap),
            (column >= HALO + own_columns, HALO + own_columns, high_own, high_swap),
        ):
            place_in = column - shift
            half = lax.shift_right_arithmetic(place_in, 1)
            within = lax.bitwise_and(place_in, 1)

            @pl.when(is_side & (half == core))
            def _():
                fetch(direct, within, slot)

            @pl.when(is_side & (half != core))
            def _():
                fetch(swapped, within, slot)

    def turn(i, carry):
        slot = lax.rem(i, BUFFERS)

        @pl.when(i + BUFFERS - 1 < total)
        def _():
            start_column(i + BUFFERS - 1)

        pltpu.make_async_copy(
            grid.at[:, pl.ds(0, LAT)], columns.at[slot], in_sems.at[slot]
        ).wait()
        source = columns.at[slot]
        for l in range(LAT // 128):
            lanes = pl.ds(l * 128, 128)
            for j in range(4):
                top = min(channels, (j + 1) * 128)
                block = source[j * 128 : top, lanes]
                if top < (j + 1) * 128:
                    block = jnp.pad(block, ((0, (j + 1) * 128 - top), (0, 0)))
                row = pl.multiple_of((i * LAT + l * 128) * 4, 8)
                table[pl.ds(row + j, 128, stride=4), :] = block.T.astype(f32)
        return carry

    def sender_place(t):
        i = chunk_list[t]
        slot = lax.shift_right_logical(first_chunk + i, 2) - lax.shift_right_logical(
            first_chunk, 2
        )
        return i * CHUNK, offset_list[slot]

    @pl.when(count > 0)
    def _():
        for b in range(BUFFERS - 1):

            @pl.when(b < total)
            def _():
                start_column(b)

        for copy in copies:
            copy.start()
        embed_weight[464:512, :] = jnp.zeros((48, 512), bf16)
        embed_weight[0:channels, :] = embed_in[...]
        lax.fori_loop(0, total, turn, 0)
        for copy in copies:
            copy.wait()
        bias = jnp.concatenate(
            [
                sum(extras[j, 4 + r : 5 + r, :].astype(f32) for r in range(3))
                for j in range(4)
            ],
            axis=1,
        )
        terms = dot(mesh[...], recv_weight[...]) + bias
        for j in range(4):
            rows[pl.ds(j, nodes, stride=4), :] = terms[:, j * 128 : (j + 1) * 128]
        edge0, offset = sender_place(0)

        def gather(b, inner):
            base = edge0 + b * UNROLL
            for u in range(UNROLL):
                sent[pl.ds(b * UNROLL + u, 4, stride=PITCH), :] = wide_row(
                    table, points[base + u] + offset
                )
            return inner

        lax.fori_loop(0, CHUNK // UNROLL, gather, 0)
        features_by = jnp.concatenate([extras[j, 0:4, :] for j in range(4)], axis=1)

        def work(t, carry):
            i = chunk_list[t]
            edge = i * CHUNK
            inputs[...] = chunk_of(sent).astype(bf16)
            for e in range(CHUNK):
                got[pl.ds(e, 4, stride=PITCH), :] = wide_row(rows, receivers[edge + e])
            latent = silu(dot(inputs[...], embed_weight[...]) + embed_bias[...]).astype(bf16)
            before = (
                dot(latent, send_weight[...])
                + chunk_of(got)
                + lax.dot_general(
                    features[first_chunk + i], features_by, (((0,), (0,)), ((), ())),
                    preferred_element_type=f32,
                )
            )
            hidden = silu(before).astype(bf16)
            node = lax.broadcasted_iota(jnp.int32, (nodes, 128), 0) * 4
            hots = [
                jnp.where(node == ids[pl.ds(i * 4 + q, 1), :], 1.0, 0.0) for q in range(4)
            ]
            hot = jnp.concatenate([value.astype(bf16) for value in hots], axis=1)
            next_edge, next_offset = sender_place(jnp.minimum(t + 1, count - 1))
            for e in range(CHUNK):
                sent[pl.ds(e, 4, stride=PITCH), :] = wide_row(
                    table, points[next_edge + e] + next_offset
                )
            totals[...] += dot(hot, hidden)
            tally[...] += (hots[0] + hots[1]) + (hots[2] + hots[3])
            return carry

        lax.fori_loop(0, count, work, 0)

    if not outer:
        return
    counts = jnp.sum(tally[...], axis=1, keepdims=True)
    whole = totals[...]
    upper = whole.astype(bf16)
    lower = (whole - upper.astype(f32)).astype(bf16)
    for copy in late:
        copy.wait()
    totals[...] = (
        dot(upper, message_weight[...])
        + dot(lower, message_weight[...])
        + counts * message_bias[...]
    )
    for r in range(2):
        mine = pl.multiple_of(jnp.bitwise_xor(k, 2 * r) * 128, 128)
        theirs = pl.multiple_of(jnp.bitwise_xor(k, 2 * r + 1) * 128, 128)
        parts[r][...] = totals[:, pl.ds(mine, 128)]
        parts[2 + r][...] = totals[:, pl.ds(theirs, 128)]


def weights_kernel(place, feature_weight, hidden_bias, sender_weight, receiver_weight, bundle):
    bundle[0:512, :] = sender_weight[...]
    bundle[512:1024, :] = receiver_weight[...]
    bias = hidden_bias[...]
    upper = bias.astype(bf16)
    middle = (bias - upper.astype(f32)).astype(bf16)
    lower = (bias - upper.astype(f32) - middle.astype(f32)).astype(bf16)
    bundle[1024:1040, :] = jnp.concatenate(
        [feature_weight[...].astype(f32)]
        + [value.astype(f32) for value in (upper, middle, lower)]
        + [jnp.zeros((9, bias.shape[1]), f32)],
        axis=0,
    ).astype(bf16)


def pack_kernel(chunks, points_own, all_points, nodes, place, senders, receivers, grid,
                points, ids, low_ref, high_ref, low_half, high_half, sems):
    lon = place[0]
    k = place[1]
    half = HALO * LAT // 2
    side = lax.bitwise_and(k, 1) * half
    low_at = pl.multiple_of(points_own - 2 * half + side, 128)
    copies = [
        pltpu.make_async_copy(grid.at[:, pl.ds(low_at, half)], low_half, sems.at[0]),
        pltpu.make_async_copy(
            grid.at[:, pl.ds(pl.multiple_of(side, 128), half)], high_half, sems.at[1]
        ),
    ]
    for copy in copies:
        copy.start()
    for i in range(chunks):
        rows = pl.ds(pl.multiple_of((k * chunks + i) * 4, 4), 4)
        point = senders[rows, :] - lon * points_own + HALO * LAT
        point = jnp.where(point < 0, point + all_points, point)
        point = jnp.where(point >= all_points, point - all_points, point)
        points[i * 4 : i * 4 + 4, :] = point * 4
        ids[i * 4 : i * 4 + 4, :] = (receivers[rows, :] - lon * nodes) * 4
        for ref, end in ((low_ref, jnp.min(point)), (high_ref, jnp.max(point))):
            ref[i] = lax.shift_right_logical(lax.shift_right_logical(end, 7) * 13108, 16)
    for copy in copies:
        copy.wait()


def weights_call(share, operands):
    return pl.pallas_call(
        weights_kernel,
        out_shape=jax.ShapeDtypeStruct((1040, share), bf16),
        in_specs=[SMEM] + [VMEM] * 4,
        out_specs=VMEM,
        name="weights",
    )(*operands)


def pack_call(chunks, points_own, all_points, channels, nodes, operands):
    half = HALO * LAT // 2
    index = jax.ShapeDtypeStruct((chunks * 4, 128), jnp.int32)
    ends = jax.ShapeDtypeStruct((chunks,), jnp.int32)
    side = jax.ShapeDtypeStruct((channels, half), bf16)
    return pl.pallas_call(
        functools.partial(pack_kernel, chunks, points_own, all_points, nodes),
        out_shape=(index, index, ends, ends, side, side),
        in_specs=[SMEM] + [VMEM] * 2 + [ANY],
        out_specs=(VMEM, VMEM, SMEM, SMEM, VMEM, VMEM),
        scratch_shapes=[pltpu.SemaphoreType.DMA((2,))],
        name="pack",
    )(*operands)


VMEM = pl.BlockSpec(memory_space=pltpu.VMEM)
SMEM = pl.BlockSpec(memory_space=pltpu.SMEM)
ANY = pl.BlockSpec(memory_space=pl.ANY)


def block_call(outer, chunks, own_columns, channels, nodes, operands):
    width = 512
    part = jax.ShapeDtypeStruct((nodes, 128), f32)
    sums = (
        jax.ShapeDtypeStruct((nodes, width), f32),
        jax.ShapeDtypeStruct((nodes, 128), f32),
    )
    specs = [SMEM] * 5 + [ANY] * (5 if outer else 1) + [VMEM] * 4 + [ANY] * 8
    if outer:
        specs = specs + [ANY] * 4 + [VMEM] * 3
    slots = SLOTS * WINDOW
    edges = chunks * CHUNK
    square = pltpu.VMEM((width, width), bf16)
    return pl.pallas_call(
        functools.partial(block_kernel, outer, chunks, own_columns, channels, nodes),
        out_shape=(part,) * 4 if outer else sums,
        in_specs=specs,
        out_specs=(VMEM,) * (4 if outer else 2),
        scratch_shapes=[
            pltpu.VMEM((slots * LAT * 4, 128), f32),
            pltpu.VMEM((BUFFERS, channels, LAT), bf16),
            pltpu.VMEM((4 * PITCH, 128), f32),
            pltpu.VMEM((4 * PITCH, 128), f32),
            pltpu.VMEM((CHUNK, width), bf16),
            pltpu.VMEM((nodes * 4, 128), f32),
            square,
            square,
            square,
            square,
            pltpu.VMEM((nodes, width), bf16),
            pltpu.VMEM((4, 16, 128), bf16),
            pltpu.SMEM((16,), jnp.int32),
            pltpu.SMEM((32,), jnp.int32),
            pltpu.SMEM((8,), jnp.int32),
            pltpu.SemaphoreType.DMA((BUFFERS,)),
            pltpu.SemaphoreType.DMA((32,)),
        ]
        + ([pltpu.VMEM(value.shape, f32) for value in sums] if outer else []),
        compiler_params=pltpu.CompilerParams(vmem_limit_bytes=60 * 2**20),
        cost_estimate=pl.CostEstimate(
            flops=2 * edges * width * (2 * width + nodes),
            bytes_accessed=2 * edges * width,
            transcendentals=2 * edges * width,
        ),
        name="block_outer" if outer else "block_inner",
    )(*operands)


def encoder(
    grid_inputs,
    embed_weight,
    embed_bias,
    mesh_latent,
    edge_features,
    senders,
    receivers,
    sender_weight,
    receiver_weight,
    feature_weight,
    hidden_bias,
    message_weight,
    message_bias,
    norm_gain,
    norm_shift,
):
    lon_count = lax.axis_size("lon")
    ch_count = lax.axis_size("ch")
    lon_place = lax.axis_index("lon")
    ch_place = lax.axis_index("ch")
    place = ch_place[None].astype(jnp.int32)
    points_own, channels = grid_inputs.shape
    own_columns = points_own // LAT
    mesh_nodes = mesh_latent.shape[0]
    full_width = message_weight.shape[1]
    edge_count = senders.shape[0]
    all_chunks = edge_count // CHUNK
    chunks = all_chunks // ch_count

    swap = [(i, i ^ 1) for i in range(ch_count)]
    across = [(i, i ^ 2) for i in range(ch_count)]
    facing = [
        (lon * ch_count + ch, (lon ^ 4) * ch_count + (ch ^ 2))
        for lon in range(lon_count)
        for ch in range(ch_count)
    ]
    forward = [(i, (i + 1) % lon_count) for i in range(lon_count)]
    backward = [(target, source) for source, target in forward]

    flat = grid_inputs.T
    place_all = jnp.stack([lon_place, ch_place]).astype(jnp.int32)
    bundle = weights_call(
        message_weight.shape[0],
        [place_all, feature_weight, hidden_bias[None, :], sender_weight, receiver_weight],
    )
    bundle_far = lax.ppermute(bundle, ("lon", "ch"), facing)
    mesh_far = lax.ppermute(mesh_latent, "ch", across)
    points, ids, low_column, high_column, low_half, high_half = pack_call(
        chunks, points_own, points_own * lon_count, channels, mesh_nodes,
        [place_all, senders.reshape(-1, 128), receivers.reshape(-1, 128), flat],
    )
    low_own = lax.ppermute(low_half, "lon", forward)
    high_own = lax.ppermute(high_half, "lon", backward)
    low_swap = lax.ppermute(low_own, "ch", swap)
    high_swap = lax.ppermute(high_own, "ch", swap)
    bundle_near = lax.ppermute(bundle, "ch", swap)
    bundle_last = lax.ppermute(bundle_far, "ch", swap)
    mesh_near = lax.ppermute(mesh_latent, "ch", swap)
    mesh_last = lax.ppermute(mesh_far, "ch", swap)
    message_far = lax.ppermute(message_weight, ("lon", "ch"), facing)
    message_near = lax.ppermute(message_weight, "ch", swap)
    message_last = lax.ppermute(message_far, "ch", swap)
    feature_blocks = jnp.transpose(
        edge_features.reshape(edge_features.shape[0], all_chunks, CHUNK), (1, 0, 2)
    )

    call = functools.partial(
        block_call, chunks=chunks, own_columns=own_columns, channels=channels, nodes=mesh_nodes
    )
    scalars = [place, points.reshape(-1), ids.reshape(-1), low_column, high_column, flat]
    arrays = [
        embed_weight, embed_bias[None, :], ids, feature_blocks,
        bundle, bundle_near, bundle_far, bundle_last,
        mesh_latent, mesh_near, mesh_far, mesh_last,
    ]
    totals, tally = call(False, operands=scalars + arrays)
    keep_here, keep_far, send_here, send_far = call(
        True,
        operands=scalars
        + [low_own, low_swap, high_own, high_swap]
        + arrays
        + [message_weight, message_near, message_far, message_last]
        + [message_bias[None, :], totals, tally],
    )
    far = keep_far + lax.ppermute(send_far, "ch", swap)
    far = lax.ppermute(far.astype(bf16), "ch", across).astype(f32)
    node_share = keep_here + lax.ppermute(send_here, "ch", swap) + far
    first_sum, second = lax.psum(
        (
            jnp.sum(node_share, axis=1, keepdims=True),
            jnp.sum(jnp.square(node_share), axis=1, keepdims=True),
        ),
        "ch",
    )
    centre = first_sum / full_width
    spread = second / full_width - jnp.square(centre)
    normed = (node_share - centre) * lax.rsqrt(spread + 1.0)
    return (mesh_latent.astype(f32) + normed * norm_gain + norm_shift).astype(bf16)


def solution(mesh):
    return jax.shard_map(
        encoder,
        mesh=mesh,
        in_specs=(
            P("lon", None),
            P(),
            P(),
            P("lon", "ch"),
            P(None, "lon"),
            P("lon"),
            P("lon"),
            P(None, "ch"),
            P(None, "ch"),
            P(None, "ch"),
            P("ch"),
            P("ch", None),
            P(),
            P("ch"),
            P("ch"),
        ),
        out_specs=P("lon", "ch"),
        check_vma=False,
    )
```

```python
import functools

import jax
import jax.numpy as jnp
from jax import lax
from jax.experimental import pallas as pl
from jax.experimental.pallas import tpu as pltpu
from jax.sharding import PartitionSpec as P


LAT = 640
HALO = 4
CHUNK = 512
SLOTS = 4
WINDOW = 7
INNER_ROWS = 8
OUTER_ROWS = 10
BUFFERS = 3
LIMIT = 6

f32 = jnp.float32
bf16 = jnp.bfloat16


def silu(value):
    half = 0.5 * value
    return half + half * jnp.tanh(half)


def dot(left, right):
    return jnp.dot(left, right, preferred_element_type=f32)


def wide_row(ref, index):
    return ref[pl.ds(pl.multiple_of(index, 4), 4), :]


def chunk_of(tile):
    pitch = tile.shape[0] // 4
    return jnp.concatenate(
        [tile[j * pitch : (j + 1) * pitch - 8, :] for j in range(4)], axis=1
    )


def list_chunks(chunks, low_ref, high_ref, own_columns, outer, chunk_list):
    def step(i, counts):
        inner_count, outer_count = counts
        halo = (low_ref[i] < HALO) | (high_ref[i] >= HALO + own_columns)
        early = jnp.logical_not(halo) & (inner_count < LIMIT)
        count = outer_count if outer else inner_count

        @pl.when(jnp.logical_not(early) if outer else early)
        def _():
            chunk_list[count] = i

        return inner_count + jnp.where(early, 1, 0), outer_count + jnp.where(early, 0, 1)

    return lax.fori_loop(0, chunks, step, (jnp.int32(0), jnp.int32(0)))[1 if outer else 0]


def list_columns(count, first_chunk, low_ref, high_ref, chunk_list, column_list, offset_list):
    slot0 = lax.shift_right_logical(first_chunk, 2)
    total = jnp.int32(0)
    seg_first = jnp.int32(1000)
    seg_last = jnp.int32(-1)
    seg_start = jnp.int32(0)
    for slot in range(SLOTS):

        def step(t, carry):
            low, high = carry
            i = chunk_list[t]
            here = lax.shift_right_logical(first_chunk + i, 2) == slot0 + slot
            return (
                jnp.where(here, jnp.minimum(low, low_ref[i]), low),
                jnp.where(here, jnp.maximum(high, high_ref[i]), high),
            )

        low, high = lax.fori_loop(0, count, step, (jnp.int32(1000), jnp.int32(-1)))
        has = high >= 0
        joins = has & (low >= seg_first) & (low <= seg_last + 1)
        begin = jnp.where(joins, seg_last + 1, low)
        fresh = jnp.where(has, jnp.maximum(high - begin + 1, 0), 0)
        base = total

        def put(j, carry):
            column_list[base + j] = begin + j
            return carry

        lax.fori_loop(0, fresh, put, 0)
        opens = has & jnp.logical_not(joins)
        seg_start = jnp.where(opens, total, seg_start)
        seg_first = jnp.where(opens, low, seg_first)
        seg_last = jnp.where(opens, high, jnp.maximum(seg_last, high))
        total = total + fresh
        offset_list[slot] = (seg_start - seg_first) * (LAT * 4)
    return total


def block_kernel(outer, chunks, own_columns, channels, nodes, *refs):
    place, low_ref, high_ref, grid = refs[:4]
    refs = refs[4:]
    if outer:
        low_own, low_swap, high_own, high_swap = refs[:4]
        refs = refs[4:]
    points, embed_in, embed_bias, ids, features = refs[:5]
    bundles = refs[5:9]
    meshes = refs[9:13]
    refs = refs[13:]
    if outer:
        messages = refs[:4]
        refs = refs[4:]
        message_bias, first_totals, first_tally, *parts = refs[:7]
        totals, tally = refs[-2:]
        refs = refs[7:-2]
    else:
        totals, tally = refs[:2]
        refs = refs[2:]
    (table, columns, sent, got, inputs, rows, embed_weight, send_weight, recv_weight,
     message_weight, mesh, extras, placed, placed_s, recv_s, chunk_list, column_list, offset_list,
     in_sems, sems) = refs
    k = place[0]
    core = lax.bitwise_and(k, 1)
    first_chunk = k * chunks
    count = list_chunks(chunks, low_ref, high_ref, own_columns, outer, chunk_list)
    total = list_columns(
        count, first_chunk, low_ref, high_ref, chunk_list, column_list, offset_list
    )

    copies = []
    for j in range(4):
        lanes = pl.ds(j * 128, 128)
        copies.append((bundles[j].at[pl.ds(0, 512)], send_weight.at[:, lanes]))
        copies.append((bundles[j].at[pl.ds(512, 512)], recv_weight.at[:, lanes]))
        copies.append((bundles[j].at[pl.ds(1024, 16)], extras.at[j]))
        at = pl.multiple_of(jnp.bitwise_xor(k, j) * 128, 128)
        copies.append((meshes[j], mesh.at[:, pl.ds(at, 128)]))
    copies = [pltpu.make_async_copy(a, b, sems.at[n]) for n, (a, b) in enumerate(copies)]
    late = []
    if outer:
        for j in range(4):
            late.append(
                pltpu.make_async_copy(
                    messages[j], message_weight.at[pl.ds(j * 128, 128)], sems.at[16 + j]
                )
            )
        for copy in late:
            copy.start()
        firsts = [
            pltpu.make_async_copy(first_totals, totals, sems.at[20]),
            pltpu.make_async_copy(first_tally, tally, sems.at[21]),
        ]
        for copy in firsts:
            copy.start()
    else:
        totals[...] = jnp.zeros_like(totals)
        tally[...] = jnp.zeros_like(tally)

    def fetch(source, column, slot):
        start = pl.multiple_of(column * LAT, 128)
        pltpu.make_async_copy(
            source.at[:, pl.ds(start, LAT)], columns.at[slot], in_sems.at[slot]
        ).start()

    def start_column(i):
        column = column_list[i]
        slot = lax.rem(i, BUFFERS)
        if not outer:
            fetch(grid, column - HALO, slot)
            return
        inside = (column >= HALO) & (column < HALO + own_columns)

        @pl.when(inside)
        def _():
            fetch(grid, column - HALO, slot)

        for is_side, shift, direct, swapped in (
            (column < HALO, 0, low_own, low_swap),
            (column >= HALO + own_columns, HALO + own_columns, high_own, high_swap),
        ):
            place_in = column - shift
            half = lax.shift_right_arithmetic(place_in, 1)
            within = lax.bitwise_and(place_in, 1)

            @pl.when(is_side & (half == core))
            def _():
                fetch(direct, within, slot)

            @pl.when(is_side & (half != core))
            def _():
                fetch(swapped, within, slot)

    def turn(i, carry):
        slot = lax.rem(i, BUFFERS)

        @pl.when(i + BUFFERS - 1 < total)
        def _():
            start_column(i + BUFFERS - 1)

        pltpu.make_async_copy(
            grid.at[:, pl.ds(0, LAT)], columns.at[slot], in_sems.at[slot]
        ).wait()
        source = columns.at[slot]
        for l in range(LAT // 128):
            lanes = pl.ds(l * 128, 128)
            for j in range(4):
                top = min(channels, (j + 1) * 128)
                block = source[j * 128 : top, lanes]
                if top < (j + 1) * 128:
                    block = jnp.pad(block, ((0, (j + 1) * 128 - top), (0, 0)))
                row = pl.multiple_of((i * LAT + l * 128) * 4, 8)
                table[pl.ds(row + j, 128, stride=4), :] = block.T.astype(f32)
        return carry

    rows_here = OUTER_ROWS if outer else INNER_ROWS
    groups = lax.div(count * 4 + (rows_here - 1), rows_here)

    def row_places(group):
        places = []
        for q in range(rows_here):
            t = group * rows_here + q
            valid = t < count * 4
            t = jnp.minimum(t, count * 4 - 1)
            row = chunk_list[lax.shift_right_logical(t, 2)] * 4 + lax.bitwise_and(t, 3)
            places.append((row, valid))
        return places

    def gather(source, picks, places, target):
        pitch = rows_here * 128 + 8
        for q, (row, _) in enumerate(places):
            line = picks.at[row]
            for e in range(128):
                target[pl.ds(q * 128 + e, 4, stride=pitch), :] = wide_row(source, line[e])

    index_copies = [
        pltpu.make_async_copy(placed, placed_s, sems.at[30]),
        pltpu.make_async_copy(ids, recv_s, sems.at[31]),
    ]

    @pl.when(count > 0)
    def _():
        for b in range(BUFFERS - 1):

            @pl.when(b < total)
            def _():
                start_column(b)

        for i in range(chunks):
            slot = lax.shift_right_logical(first_chunk + i, 2) - lax.shift_right_logical(
                first_chunk, 2
            )
            placed[i * 4 : i * 4 + 4, :] = points[i * 4 : i * 4 + 4, :] + offset_list[slot]
        for copy in index_copies:
            copy.start()
        for copy in copies:
            copy.start()
        embed_weight[464:512, :] = jnp.zeros((48, 512), bf16)
        embed_weight[0:channels, :] = embed_in[...]
        lax.fori_loop(0, total, turn, 0)
        for copy in copies + index_copies:
            copy.wait()
        bias = jnp.concatenate(
            [
                sum(extras[j, 4 + r : 5 + r, :].astype(f32) for r in range(3))
                for j in range(4)
            ],
            axis=1,
        )
        terms = dot(mesh[...], recv_weight[...]) + bias
        for j in range(4):
            rows[pl.ds(j, nodes, stride=4), :] = terms[:, j * 128 : (j + 1) * 128]
        gather(table, placed_s, row_places(0), sent)
        features_by = jnp.concatenate([extras[j, 0:4, :] for j in range(4)], axis=1)

        if outer:
            for copy in firsts:
                copy.wait()

        def work(group, carry):
            places = row_places(group)
            inputs[...] = chunk_of(sent).astype(bf16)
            gather(rows, recv_s, places, got)
            latent = silu(dot(inputs[...], embed_weight[...]) + embed_bias[...]).astype(bf16)
            edge_values = jnp.concatenate(
                [features[first_chunk * 4 + row] for row, _ in places], axis=1
            )
            before = (
                dot(latent, send_weight[...])
                + chunk_of(got)
                + lax.dot_general(
                    edge_values, features_by, (((0,), (0,)), ((), ())),
                    preferred_element_type=f32,
                )
            )
            hidden = silu(before).astype(bf16)
            node = lax.broadcasted_iota(jnp.int32, (nodes, 128), 0) * 4
            hots = []
            heard = tally[...]
            for row, valid in places:
                at = jnp.where(valid, ids[pl.ds(row, 1), :], -1)
                value = jnp.where(node == at, 1.0, 0.0)
                heard = heard + value
                hots.append(value.astype(bf16))
            tally[...] = heard
            gather(table, placed_s, row_places(jnp.minimum(group + 1, groups - 1)), sent)
            totals[...] += dot(jnp.concatenate(hots, axis=1), hidden)
            return carry

        lax.fori_loop(0, groups, work, 0)

    if not outer:
        return

    @pl.when(count == 0)
    def _():
        for copy in firsts:
            copy.wait()

    counts = jnp.sum(tally[...], axis=1, keepdims=True)
    whole = totals[...]
    upper = whole.astype(bf16)
    lower = (whole - upper.astype(f32)).astype(bf16)
    for copy in late:
        copy.wait()
    totals[...] = (
        dot(upper, message_weight[...])
        + dot(lower, message_weight[...])
        + counts * message_bias[...]
    )
    for r in range(2):
        mine = pl.multiple_of(jnp.bitwise_xor(k, 2 * r) * 128, 128)
        theirs = pl.multiple_of(jnp.bitwise_xor(k, 2 * r + 1) * 128, 128)
        parts[r][...] = totals[:, pl.ds(mine, 128)]
        parts[2 + r][...] = totals[:, pl.ds(theirs, 128)]


def weights_kernel(feature_weight, hidden_bias, sender_weight, receiver_weight, bundle):
    bundle[0:512, :] = sender_weight[...]
    bundle[512:1024, :] = receiver_weight[...]
    bias = hidden_bias[...]
    upper = bias.astype(bf16)
    middle = (bias - upper.astype(f32)).astype(bf16)
    lower = (bias - upper.astype(f32) - middle.astype(f32)).astype(bf16)
    bundle[1024:1040, :] = jnp.concatenate(
        [feature_weight[...].astype(f32)]
        + [value.astype(f32) for value in (upper, middle, lower)]
        + [jnp.zeros((9, bias.shape[1]), f32)],
        axis=0,
    ).astype(bf16)


def pack_kernel(chunks, points_own, all_points, nodes, lon_ref, place, senders, receivers, grid,
                points, ids, low_ref, high_ref, low_half, high_half, sems):
    lon = lon_ref[0]
    k = place[0]
    half = HALO * LAT // 2
    side = lax.bitwise_and(k, 1) * half
    low_at = pl.multiple_of(points_own - 2 * half + side, 128)
    copies = [
        pltpu.make_async_copy(grid.at[:, pl.ds(low_at, half)], low_half, sems.at[0]),
        pltpu.make_async_copy(
            grid.at[:, pl.ds(pl.multiple_of(side, 128), half)], high_half, sems.at[1]
        ),
    ]
    for copy in copies:
        copy.start()
    for i in range(chunks):
        rows = pl.ds(pl.multiple_of((k * chunks + i) * 4, 4), 4)
        point = senders[rows, :] - lon * points_own + HALO * LAT
        point = jnp.where(point < 0, point + all_points, point)
        point = jnp.where(point >= all_points, point - all_points, point)
        points[i * 4 : i * 4 + 4, :] = point * 4
        ids[i * 4 : i * 4 + 4, :] = (receivers[rows, :] - lon * nodes) * 4
        for ref, end in ((low_ref, jnp.min(point)), (high_ref, jnp.max(point))):
            ref[i] = lax.shift_right_logical(lax.shift_right_logical(end, 7) * 13108, 16)
    for copy in copies:
        copy.wait()


def weights_call(share, operands):
    return pl.pallas_call(
        weights_kernel,
        out_shape=jax.ShapeDtypeStruct((1040, share), bf16),
        in_specs=[VMEM] * 4,
        out_specs=VMEM,
        name="weights",
    )(*operands)


def pack_call(chunks, points_own, all_points, channels, nodes, operands):
    half = HALO * LAT // 2
    index = jax.ShapeDtypeStruct((chunks * 4, 128), jnp.int32)
    ends = jax.ShapeDtypeStruct((chunks,), jnp.int32)
    side = jax.ShapeDtypeStruct((channels, half), bf16)
    return pl.pallas_call(
        functools.partial(pack_kernel, chunks, points_own, all_points, nodes),
        out_shape=(index, index, ends, ends, side, side),
        in_specs=[SMEM] * 2 + [VMEM] * 2 + [ANY],
        out_specs=(VMEM, VMEM, SMEM, SMEM, VMEM, VMEM),
        scratch_shapes=[pltpu.SemaphoreType.DMA((2,))],
        name="pack",
    )(*operands)


VMEM = pl.BlockSpec(memory_space=pltpu.VMEM)
SMEM = pl.BlockSpec(memory_space=pltpu.SMEM)
ANY = pl.BlockSpec(memory_space=pl.ANY)


def block_call(outer, chunks, own_columns, channels, nodes, operands):
    width = 512
    part = jax.ShapeDtypeStruct((nodes, 128), f32)
    sums = (
        jax.ShapeDtypeStruct((nodes, width), f32),
        jax.ShapeDtypeStruct((nodes, 128), f32),
    )
    specs = [SMEM] * 3 + [ANY] * (5 if outer else 1) + [VMEM] * 5 + [ANY] * 8
    if outer:
        specs = specs + [ANY] * 4 + [VMEM] + [ANY] * 2
    slots = SLOTS * WINDOW
    edges = chunks * CHUNK
    square = pltpu.VMEM((width, width), bf16)
    group_edges = 128 * (OUTER_ROWS if outer else INNER_ROWS)
    tile = pltpu.VMEM((4 * (group_edges + 8), 128), f32)
    return pl.pallas_call(
        functools.partial(block_kernel, outer, chunks, own_columns, channels, nodes),
        out_shape=(part,) * 4 if outer else sums,
        in_specs=specs,
        out_specs=(VMEM,) * (4 if outer else 2),
        scratch_shapes=[
            pltpu.VMEM((slots * LAT * 4, 128), f32),
            pltpu.VMEM((BUFFERS, channels, LAT), bf16),
            tile,
            tile,
            pltpu.VMEM((group_edges, width), bf16),
            pltpu.VMEM((nodes * 4, 128), f32),
            square,
            square,
            square,
            square,
            pltpu.VMEM((nodes, width), bf16),
            pltpu.VMEM((4, 16, 128), bf16),
            pltpu.VMEM((chunks * 4, 128), jnp.int32),
            pltpu.SMEM((chunks * 4, 128), jnp.int32),
            pltpu.SMEM((chunks * 4, 128), jnp.int32),
            pltpu.SMEM((16,), jnp.int32),
            pltpu.SMEM((32,), jnp.int32),
            pltpu.SMEM((8,), jnp.int32),
            pltpu.SemaphoreType.DMA((BUFFERS,)),
            pltpu.SemaphoreType.DMA((32,)),
        ]
        + ([pltpu.VMEM(value.shape, f32) for value in sums] if outer else []),
        compiler_params=pltpu.CompilerParams(vmem_limit_bytes=60 * 2**20),
        cost_estimate=pl.CostEstimate(
            flops=2 * edges * width * (2 * width + nodes),
            bytes_accessed=2 * edges * width,
            transcendentals=2 * edges * width,
        ),
        name="block_outer" if outer else "block_inner",
    )(*operands)


def encoder(
    grid_inputs,
    embed_weight,
    embed_bias,
    mesh_latent,
    edge_features,
    senders,
    receivers,
    sender_weight,
    receiver_weight,
    feature_weight,
    hidden_bias,
    message_weight,
    message_bias,
    norm_gain,
    norm_shift,
):
    lon_count = lax.axis_size("lon")
    ch_count = lax.axis_size("ch")
    lon_place = lax.axis_index("lon")
    ch_place = lax.axis_index("ch")
    place = ch_place[None].astype(jnp.int32)
    points_own, channels = grid_inputs.shape
    own_columns = points_own // LAT
    mesh_nodes = mesh_latent.shape[0]
    full_width = message_weight.shape[1]
    edge_count = senders.shape[0]
    all_chunks = edge_count // CHUNK
    chunks = all_chunks // ch_count

    swap = [(i, i ^ 1) for i in range(ch_count)]
    across = [(i, i ^ 2) for i in range(ch_count)]
    facing = [
        (lon * ch_count + ch, (lon ^ 4) * ch_count + (ch ^ 2))
        for lon in range(lon_count)
        for ch in range(ch_count)
    ]
    forward = [(i, (i + 1) % lon_count) for i in range(lon_count)]
    backward = [(target, source) for source, target in forward]

    flat = grid_inputs.T
    lon_scalar = lon_place[None].astype(jnp.int32)
    bundle = weights_call(
        message_weight.shape[0],
        [feature_weight, hidden_bias[None, :], sender_weight, receiver_weight],
    )
    bundle_far = lax.ppermute(bundle, ("lon", "ch"), facing)
    mesh_far = lax.ppermute(mesh_latent, "ch", across)
    points, ids, low_column, high_column, low_half, high_half = pack_call(
        chunks, points_own, points_own * lon_count, channels, mesh_nodes,
        [lon_scalar, place, senders.reshape(-1, 128), receivers.reshape(-1, 128), flat],
    )
    low_own = lax.ppermute(low_half, "lon", forward)
    high_own = lax.ppermute(high_half, "lon", backward)
    low_swap = lax.ppermute(low_own, "ch", swap)
    high_swap = lax.ppermute(high_own, "ch", swap)
    bundle_near = lax.ppermute(bundle, "ch", swap)
    bundle_last = lax.ppermute(bundle_far, "ch", swap)
    mesh_near = lax.ppermute(mesh_latent, "ch", swap)
    mesh_last = lax.ppermute(mesh_far, "ch", swap)
    message_far = lax.ppermute(message_weight, ("lon", "ch"), facing)
    message_near = lax.ppermute(message_weight, "ch", swap)
    message_last = lax.ppermute(message_far, "ch", swap)
    feature_blocks = jnp.transpose(
        edge_features.reshape(edge_features.shape[0], -1, 128), (1, 0, 2)
    )

    call = functools.partial(
        block_call, chunks=chunks, own_columns=own_columns, channels=channels, nodes=mesh_nodes
    )
    scalars = [place, low_column, high_column, flat]
    arrays = [
        points, embed_weight, embed_bias[None, :], ids, feature_blocks,
        bundle, bundle_near, bundle_far, bundle_last,
        mesh_latent, mesh_near, mesh_far, mesh_last,
    ]
    totals, tally = call(False, operands=scalars + arrays)
    keep_here, keep_far, send_here, send_far = call(
        True,
        operands=scalars
        + [low_own, low_swap, high_own, high_swap]
        + arrays
        + [message_weight, message_near, message_far, message_last]
        + [message_bias[None, :], totals, tally],
    )
    far = keep_far + lax.ppermute(send_far, "ch", swap)
    far = lax.ppermute(far.astype(bf16), "ch", across).astype(f32)
    node_share = keep_here + lax.ppermute(send_here, "ch", swap) + far
    first_sum, second = lax.psum(
        (
            jnp.sum(node_share, axis=1, keepdims=True),
            jnp.sum(jnp.square(node_share), axis=1, keepdims=True),
        ),
        "ch",
    )
    centre = first_sum / full_width
    spread = second / full_width - jnp.square(centre)
    normed = (node_share - centre) * lax.rsqrt(spread + 1.0)
    return (mesh_latent.astype(f32) + normed * norm_gain + norm_shift).astype(bf16)


def solution(mesh):
    return jax.shard_map(
        encoder,
        mesh=mesh,
        in_specs=(
            P("lon", None),
            P(),
            P(),
            P("lon", "ch"),
            P(None, "lon"),
            P("lon"),
            P("lon"),
            P(None, "ch"),
            P(None, "ch"),
            P(None, "ch"),
            P("ch"),
            P("ch", None),
            P(),
            P("ch"),
            P("ch"),
        ),
        out_specs=P("lon", "ch"),
        check_vma=False,
    )
```

```python
import functools

import jax
import jax.numpy as jnp
from jax import lax
from jax.experimental import pallas as pl
from jax.experimental.pallas import tpu as pltpu
from jax.sharding import PartitionSpec as P


LAT = 640
HALO = 4
CHUNK = 512
SLOTS = 4
WINDOW = 7
PITCH = CHUNK + 8
BUFFERS = 8
LIMIT = 6

f32 = jnp.float32
bf16 = jnp.bfloat16


def silu(value):
    half = 0.5 * value
    return half + half * jnp.tanh(half)


def dot(left, right):
    return jnp.dot(left, right, preferred_element_type=f32)


def wide_row(ref, index):
    return ref[pl.ds(pl.multiple_of(index, 4), 4), :]


def chunk_of(tile):
    return jnp.concatenate([tile[j * PITCH : j * PITCH + CHUNK, :] for j in range(4)], axis=1)


def list_chunks(chunks, low_ref, high_ref, own_columns, outer, chunk_list):
    def step(i, counts):
        inner_count, outer_count = counts
        halo = (low_ref[i] < HALO) | (high_ref[i] >= HALO + own_columns)
        early = jnp.logical_not(halo) & (inner_count < LIMIT)
        count = outer_count if outer else inner_count

        @pl.when(jnp.logical_not(early) if outer else early)
        def _():
            chunk_list[count] = i

        return inner_count + jnp.where(early, 1, 0), outer_count + jnp.where(early, 0, 1)

    return lax.fori_loop(0, chunks, step, (jnp.int32(0), jnp.int32(0)))[1 if outer else 0]


def list_columns(count, first_chunk, low_ref, high_ref, chunk_list, column_list, offset_list):
    slot0 = lax.shift_right_logical(first_chunk, 2)
    total = jnp.int32(0)
    seg_first = jnp.int32(1000)
    seg_last = jnp.int32(-1)
    seg_start = jnp.int32(0)
    for slot in range(SLOTS):

        def step(t, carry):
            low, high = carry
            i = chunk_list[t]
            here = lax.shift_right_logical(first_chunk + i, 2) == slot0 + slot
            return (
                jnp.where(here, jnp.minimum(low, low_ref[i]), low),
                jnp.where(here, jnp.maximum(high, high_ref[i]), high),
            )

        low, high = lax.fori_loop(0, count, step, (jnp.int32(1000), jnp.int32(-1)))
        has = high >= 0
        joins = has & (low >= seg_first) & (low <= seg_last + 1)
        begin = jnp.where(joins, seg_last + 1, low)
        fresh = jnp.where(has, jnp.maximum(high - begin + 1, 0), 0)
        base = total

        def put(j, carry):
            column_list[base + j] = begin + j
            return carry

        lax.fori_loop(0, fresh, put, 0)
        opens = has & jnp.logical_not(joins)
        seg_start = jnp.where(opens, total, seg_start)
        seg_first = jnp.where(opens, low, seg_first)
        seg_last = jnp.where(opens, high, jnp.maximum(seg_last, high))
        total = total + fresh
        offset_list[slot] = (seg_start - seg_first) * (LAT * 4)
    return total


def block_kernel(outer, chunks, own_columns, channels, nodes, *refs):
    place, low_ref, high_ref, grid = refs[:4]
    refs = refs[4:]
    if outer:
        low_own, low_swap, high_own, high_swap = refs[:4]
        refs = refs[4:]
    points, embed_in, embed_bias, ids, features = refs[:5]
    bundles = refs[5:9]
    meshes = refs[9:13]
    refs = refs[13:]
    if outer:
        messages = refs[:4]
        refs = refs[4:]
        message_bias, first_totals, first_tally, *parts = refs[:7]
        totals, tally = refs[-2:]
        refs = refs[7:-2]
    else:
        totals, tally = refs[:2]
        refs = refs[2:]
    (table, columns, sent, got, inputs, rows, embed_weight, send_weight, recv_weight,
     message_weight, mesh, extras, placed, placed_s, recv_s, chunk_list, column_list, offset_list,
     in_sems, sems) = refs
    k = place[0]
    core = lax.bitwise_and(k, 1)
    first_chunk = k * chunks
    count = list_chunks(chunks, low_ref, high_ref, own_columns, outer, chunk_list)
    total = list_columns(
        count, first_chunk, low_ref, high_ref, chunk_list, column_list, offset_list
    )

    copies = []
    for j in range(4):
        lanes = pl.ds(j * 128, 128)
        copies.append((bundles[j].at[pl.ds(0, 512)], send_weight.at[:, lanes]))
        copies.append((bundles[j].at[pl.ds(512, 512)], recv_weight.at[:, lanes]))
        copies.append((bundles[j].at[pl.ds(1024, 16)], extras.at[j]))
        at = pl.multiple_of(jnp.bitwise_xor(k, j) * 128, 128)
        copies.append((meshes[j], mesh.at[:, pl.ds(at, 128)]))
    copies = [pltpu.make_async_copy(a, b, sems.at[n]) for n, (a, b) in enumerate(copies)]
    late = []
    if outer:
        for j in range(4):
            late.append(
                pltpu.make_async_copy(
                    messages[j], message_weight.at[pl.ds(j * 128, 128)], sems.at[16 + j]
                )
            )
        for copy in late:
            copy.start()
        totals[...] = first_totals[...]
        tally[...] = first_tally[...]
    else:
        totals[...] = jnp.zeros_like(totals)
        tally[...] = jnp.zeros_like(tally)

    def fetch(source, column, slot):
        start = pl.multiple_of(column * LAT, 128)
        pltpu.make_async_copy(
            source.at[:, pl.ds(start, LAT)], columns.at[slot], in_sems.at[slot]
        ).start()

    def start_column(i):
        column = column_list[i]
        slot = lax.rem(i, BUFFERS)
        if not outer:
            fetch(grid, column - HALO, slot)
            return
        inside = (column >= HALO) & (column < HALO + own_columns)

        @pl.when(inside)
        def _():
            fetch(grid, column - HALO, slot)

        for is_side, shift, direct, swapped in (
            (column < HALO, 0, low_own, low_swap),
            (column >= HALO + own_columns, HALO + own_columns, high_own, high_swap),
        ):
            place_in = column - shift
            half = lax.shift_right_arithmetic(place_in, 1)
            within = lax.bitwise_and(place_in, 1)

            @pl.when(is_side & (half == core))
            def _():
                fetch(direct, within, slot)

            @pl.when(is_side & (half != core))
            def _():
                fetch(swapped, within, slot)

    def turn(i, carry):
        slot = lax.rem(i, BUFFERS)

        @pl.when(i + BUFFERS - 1 < total)
        def _():
            start_column(i + BUFFERS - 1)

        pltpu.make_async_copy(
            grid.at[:, pl.ds(0, LAT)], columns.at[slot], in_sems.at[slot]
        ).wait()
        source = columns.at[slot]
        for l in range(LAT // 128):
            lanes = pl.ds(l * 128, 128)
            for j in range(4):
                top = min(channels, (j + 1) * 128)
                block = source[j * 128 : top, lanes]
                if top < (j + 1) * 128:
                    block = jnp.pad(block, ((0, (j + 1) * 128 - top), (0, 0)))
                row = pl.multiple_of((i * LAT + l * 128) * 4, 8)
                table[pl.ds(row + j, 128, stride=4), :] = block.T.astype(f32)
        return carry

    def indices(ref, t):
        return ref.at[pl.ds(pl.multiple_of(chunk_list[t] * 4, 4), 4)]

    def gather(source, picks, target):
        for e in range(CHUNK):
            target[pl.ds(e, 4, stride=PITCH), :] = wide_row(source, picks[e // 128, e % 128])

    index_copies = [
        pltpu.make_async_copy(placed, placed_s, sems.at[30]),
        pltpu.make_async_copy(ids, recv_s, sems.at[31]),
    ]

    @pl.when(count > 0)
    def _():
        for b in range(BUFFERS - 1):

            @pl.when(b < total)
            def _():
                start_column(b)

        for i in range(chunks):
            slot = lax.shift_right_logical(first_chunk + i, 2) - lax.shift_right_logical(
                first_chunk, 2
            )
            placed[i * 4 : i * 4 + 4, :] = points[i * 4 : i * 4 + 4, :] + offset_list[slot]
        for copy in index_copies:
            copy.start()
        for copy in copies:
            copy.start()
        embed_weight[464:512, :] = jnp.zeros((48, 512), bf16)
        embed_weight[0:channels, :] = embed_in[...]
        lax.fori_loop(0, total, turn, 0)
        for copy in copies + index_copies:
            copy.wait()
        bias = jnp.concatenate(
            [
                sum(extras[j, 4 + r : 5 + r, :].astype(f32) for r in range(3))
                for j in range(4)
            ],
            axis=1,
        )
        terms = dot(mesh[...], recv_weight[...]) + bias
        for j in range(4):
            rows[pl.ds(j, nodes, stride=4), :] = terms[:, j * 128 : (j + 1) * 128]
        gather(table, indices(placed_s, 0), sent)
        features_by = jnp.concatenate([extras[j, 0:4, :] for j in range(4)], axis=1)

        def work(t, carry):
            i = chunk_list[t]
            inputs[...] = chunk_of(sent).astype(bf16)
            gather(rows, indices(recv_s, t), got)
            latent = silu(dot(inputs[...], embed_weight[...]) + embed_bias[...]).astype(bf16)
            before = (
                dot(latent, send_weight[...])
                + chunk_of(got)
                + lax.dot_general(
                    features[first_chunk + i], features_by, (((0,), (0,)), ((), ())),
                    preferred_element_type=f32,
                )
            )
            hidden = silu(before).astype(bf16)
            node = lax.broadcasted_iota(jnp.int32, (nodes, 128), 0) * 4
            hots = [
                jnp.where(node == ids[pl.ds(i * 4 + q, 1), :], 1.0, 0.0) for q in range(4)
            ]
            hot = jnp.concatenate([value.astype(bf16) for value in hots], axis=1)
            gather(table, indices(placed_s, jnp.minimum(t + 1, count - 1)), sent)
            totals[...] += dot(hot, hidden)
            tally[...] += (hots[0] + hots[1]) + (hots[2] + hots[3])
            return carry

        lax.fori_loop(0, count, work, 0)

    if not outer:
        return
    counts = jnp.sum(tally[...], axis=1, keepdims=True)
    whole = totals[...]
    upper = whole.astype(bf16)
    lower = (whole - upper.astype(f32)).astype(bf16)
    for copy in late:
        copy.wait()
    totals[...] = (
        dot(upper, message_weight[...])
        + dot(lower, message_weight[...])
        + counts * message_bias[...]
    )
    for r in range(2):
        mine = pl.multiple_of(jnp.bitwise_xor(k, 2 * r) * 128, 128)
        theirs = pl.multiple_of(jnp.bitwise_xor(k, 2 * r + 1) * 128, 128)
        parts[r][...] = totals[:, pl.ds(mine, 128)]
        parts[2 + r][...] = totals[:, pl.ds(theirs, 128)]


def share_kernel(keep, got, far, share, sums):
    value = keep[...] + got[...] + far[...].astype(f32)
    share[...] = value
    turned = value.T
    sums[0:1, :] = jnp.sum(turned, axis=0, keepdims=True)
    sums[1:2, :] = jnp.sum(turned * turned, axis=0, keepdims=True)


def norm_kernel(width, share, own, near, across, last, mesh_latent, gain, shift, out):
    total = (own[...] + near[...]) + (across[...] + last[...])
    centre = total[0:1, :] / width
    spread = total[1:2, :] / width - centre * centre
    scale = lax.rsqrt(spread + 1.0)
    nodes = centre.shape[1]
    turned = jnp.concatenate([centre, scale, jnp.zeros((6, nodes), f32)], axis=0).T
    normed = (share[...] - turned[:, 0:1]) * turned[:, 1:2]
    out[...] = (mesh_latent[...].astype(f32) + normed * gain[...] + shift[...]).astype(bf16)


def weights_kernel(feature_weight, hidden_bias, sender_weight, receiver_weight, bundle):
    bundle[0:512, :] = sender_weight[...]
    bundle[512:1024, :] = receiver_weight[...]
    bias = hidden_bias[...]
    upper = bias.astype(bf16)
    middle = (bias - upper.astype(f32)).astype(bf16)
    lower = (bias - upper.astype(f32) - middle.astype(f32)).astype(bf16)
    bundle[1024:1040, :] = jnp.concatenate(
        [feature_weight[...].astype(f32)]
        + [value.astype(f32) for value in (upper, middle, lower)]
        + [jnp.zeros((9, bias.shape[1]), f32)],
        axis=0,
    ).astype(bf16)


def pack_kernel(chunks, points_own, all_points, nodes, lon_ref, place, senders, receivers, grid,
                points, ids, low_ref, high_ref, low_half, high_half, sems):
    lon = lon_ref[0]
    k = place[0]
    half = HALO * LAT // 2
    side = lax.bitwise_and(k, 1) * half
    low_at = pl.multiple_of(points_own - 2 * half + side, 128)
    copies = [
        pltpu.make_async_copy(grid.at[:, pl.ds(low_at, half)], low_half, sems.at[0]),
        pltpu.make_async_copy(
            grid.at[:, pl.ds(pl.multiple_of(side, 128), half)], high_half, sems.at[1]
        ),
    ]
    for copy in copies:
        copy.start()
    for i in range(chunks):
        rows = pl.ds(pl.multiple_of((k * chunks + i) * 4, 4), 4)
        point = senders[rows, :] - lon * points_own + HALO * LAT
        point = jnp.where(point < 0, point + all_points, point)
        point = jnp.where(point >= all_points, point - all_points, point)
        points[i * 4 : i * 4 + 4, :] = point * 4
        ids[i * 4 : i * 4 + 4, :] = (receivers[rows, :] - lon * nodes) * 4
        for ref, end in ((low_ref, jnp.min(point)), (high_ref, jnp.max(point))):
            ref[i] = lax.shift_right_logical(lax.shift_right_logical(end, 7) * 13108, 16)
    for copy in copies:
        copy.wait()


def weights_call(share, operands):
    return pl.pallas_call(
        weights_kernel,
        out_shape=jax.ShapeDtypeStruct((1040, share), bf16),
        in_specs=[VMEM] * 4,
        out_specs=VMEM,
        name="weights",
    )(*operands)


def pack_call(chunks, points_own, all_points, channels, nodes, operands):
    half = HALO * LAT // 2
    index = jax.ShapeDtypeStruct((chunks * 4, 128), jnp.int32)
    ends = jax.ShapeDtypeStruct((chunks,), jnp.int32)
    side = jax.ShapeDtypeStruct((channels, half), bf16)
    return pl.pallas_call(
        functools.partial(pack_kernel, chunks, points_own, all_points, nodes),
        out_shape=(index, index, ends, ends, side, side),
        in_specs=[SMEM] * 2 + [VMEM] * 2 + [ANY],
        out_specs=(VMEM, VMEM, SMEM, SMEM, VMEM, VMEM),
        scratch_shapes=[pltpu.SemaphoreType.DMA((2,))],
        name="pack",
    )(*operands)


VMEM = pl.BlockSpec(memory_space=pltpu.VMEM)
SMEM = pl.BlockSpec(memory_space=pltpu.SMEM)
ANY = pl.BlockSpec(memory_space=pl.ANY)


def block_call(outer, chunks, own_columns, channels, nodes, operands):
    width = 512
    part = jax.ShapeDtypeStruct((nodes, 128), f32)
    sums = (
        jax.ShapeDtypeStruct((nodes, width), f32),
        jax.ShapeDtypeStruct((nodes, 128), f32),
    )
    specs = [SMEM] * 3 + [ANY] * (5 if outer else 1) + [VMEM] * 5 + [ANY] * 8
    if outer:
        specs = specs + [ANY] * 4 + [VMEM] * 3
    slots = SLOTS * WINDOW
    edges = chunks * CHUNK
    square = pltpu.VMEM((width, width), bf16)
    return pl.pallas_call(
        functools.partial(block_kernel, outer, chunks, own_columns, channels, nodes),
        out_shape=(part,) * 4 if outer else sums,
        in_specs=specs,
        out_specs=(VMEM,) * (4 if outer else 2),
        scratch_shapes=[
            pltpu.VMEM((slots * LAT * 4, 128), f32),
            pltpu.VMEM((BUFFERS, channels, LAT), bf16),
            pltpu.VMEM((4 * PITCH, 128), f32),
            pltpu.VMEM((4 * PITCH, 128), f32),
            pltpu.VMEM((CHUNK, width), bf16),
            pltpu.VMEM((nodes * 4, 128), f32),
            square,
            square,
            square,
            square,
            pltpu.VMEM((nodes, width), bf16),
            pltpu.VMEM((4, 16, 128), bf16),
            pltpu.VMEM((chunks * 4, 128), jnp.int32),
            pltpu.SMEM((chunks * 4, 128), jnp.int32),
            pltpu.SMEM((chunks * 4, 128), jnp.int32),
            pltpu.SMEM((16,), jnp.int32),
            pltpu.SMEM((32,), jnp.int32),
            pltpu.SMEM((8,), jnp.int32),
            pltpu.SemaphoreType.DMA((BUFFERS,)),
            pltpu.SemaphoreType.DMA((32,)),
        ]
        + ([pltpu.VMEM(value.shape, f32) for value in sums] if outer else []),
        compiler_params=pltpu.CompilerParams(vmem_limit_bytes=60 * 2**20),
        cost_estimate=pl.CostEstimate(
            flops=2 * edges * width * (2 * width + nodes),
            bytes_accessed=2 * edges * width,
            transcendentals=2 * edges * width,
        ),
        name="block_outer" if outer else "block_inner",
    )(*operands)


def encoder(
    grid_inputs,
    embed_weight,
    embed_bias,
    mesh_latent,
    edge_features,
    senders,
    receivers,
    sender_weight,
    receiver_weight,
    feature_weight,
    hidden_bias,
    message_weight,
    message_bias,
    norm_gain,
    norm_shift,
):
    lon_count = lax.axis_size("lon")
    ch_count = lax.axis_size("ch")
    lon_place = lax.axis_index("lon")
    ch_place = lax.axis_index("ch")
    place = ch_place[None].astype(jnp.int32)
    points_own, channels = grid_inputs.shape
    own_columns = points_own // LAT
    mesh_nodes = mesh_latent.shape[0]
    full_width = message_weight.shape[1]
    edge_count = senders.shape[0]
    all_chunks = edge_count // CHUNK
    chunks = all_chunks // ch_count

    swap = [(i, i ^ 1) for i in range(ch_count)]
    across = [(i, i ^ 2) for i in range(ch_count)]
    facing = [
        (lon * ch_count + ch, (lon ^ 4) * ch_count + (ch ^ 2))
        for lon in range(lon_count)
        for ch in range(ch_count)
    ]
    forward = [(i, (i + 1) % lon_count) for i in range(lon_count)]
    backward = [(target, source) for source, target in forward]

    flat = grid_inputs.T
    lon_scalar = lon_place[None].astype(jnp.int32)
    bundle = weights_call(
        message_weight.shape[0],
        [feature_weight, hidden_bias[None, :], sender_weight, receiver_weight],
    )
    bundle_far = lax.ppermute(bundle, ("lon", "ch"), facing)
    mesh_far = lax.ppermute(mesh_latent, "ch", across)
    points, ids, low_column, high_column, low_half, high_half = pack_call(
        chunks, points_own, points_own * lon_count, channels, mesh_nodes,
        [lon_scalar, place, senders.reshape(-1, 128), receivers.reshape(-1, 128), flat],
    )
    low_own = lax.ppermute(low_half, "lon", forward)
    high_own = lax.ppermute(high_half, "lon", backward)
    low_swap = lax.ppermute(low_own, "ch", swap)
    high_swap = lax.ppermute(high_own, "ch", swap)
    bundle_near = lax.ppermute(bundle, "ch", swap)
    bundle_last = lax.ppermute(bundle_far, "ch", swap)
    mesh_near = lax.ppermute(mesh_latent, "ch", swap)
    mesh_last = lax.ppermute(mesh_far, "ch", swap)
    message_far = lax.ppermute(message_weight, ("lon", "ch"), facing)
    message_near = lax.ppermute(message_weight, "ch", swap)
    message_last = lax.ppermute(message_far, "ch", swap)
    feature_blocks = jnp.transpose(
        edge_features.reshape(edge_features.shape[0], all_chunks, CHUNK), (1, 0, 2)
    )

    call = functools.partial(
        block_call, chunks=chunks, own_columns=own_columns, channels=channels, nodes=mesh_nodes
    )
    scalars = [place, low_column, high_column, flat]
    arrays = [
        points, embed_weight, embed_bias[None, :], ids, feature_blocks,
        bundle, bundle_near, bundle_far, bundle_last,
        mesh_latent, mesh_near, mesh_far, mesh_last,
    ]
    totals, tally = call(False, operands=scalars + arrays)
    keep_here, keep_far, send_here, send_far = call(
        True,
        operands=scalars
        + [low_own, low_swap, high_own, high_swap]
        + arrays
        + [message_weight, message_near, message_far, message_last]
        + [message_bias[None, :], totals, tally],
    )
    far = keep_far + lax.ppermute(send_far, "ch", swap)
    far = lax.ppermute(far.astype(bf16), "ch", across)
    got = lax.ppermute(send_here, "ch", swap)
    share_shape = keep_here.shape
    node_share, sums = pl.pallas_call(
        share_kernel,
        out_shape=(
            jax.ShapeDtypeStruct(share_shape, f32),
            jax.ShapeDtypeStruct((2, mesh_nodes), f32),
        ),
        name="share",
    )(keep_here, got, far)
    others = [
        lax.ppermute(sums, "ch", [(i, i ^ j) for i in range(ch_count)]) for j in (2, 3, 1)
    ]
    return pl.pallas_call(
        functools.partial(norm_kernel, float(full_width)),
        out_shape=jax.ShapeDtypeStruct(share_shape, bf16),
        name="norm",
    )(node_share, sums, *others, mesh_latent, norm_gain[None, :], norm_shift[None, :])


def solution(mesh):
    return jax.shard_map(
        encoder,
        mesh=mesh,
        in_specs=(
            P("lon", None),
            P(),
            P(),
            P("lon", "ch"),
            P(None, "lon"),
            P("lon"),
            P("lon"),
            P(None, "ch"),
            P(None, "ch"),
            P(None, "ch"),
            P("ch"),
            P("ch", None),
            P(),
            P("ch"),
            P("ch"),
        ),
        out_specs=P("lon", "ch"),
        check_vma=False,
    )
```

```python
import functools

import jax
import jax.numpy as jnp
from jax import lax
from jax.experimental import pallas as pl
from jax.experimental.pallas import tpu as pltpu
from jax.sharding import PartitionSpec as P


LAT = 640
HALO = 4
CHUNK = 512
SLOTS = 4
WINDOW = 7
PITCH = CHUNK + 8
BUFFERS = 8
LIMIT = 7

f32 = jnp.float32
bf16 = jnp.bfloat16


def silu(value):
    half = 0.5 * value
    return half + half * jnp.tanh(half)


def dot(left, right):
    return jnp.dot(left, right, preferred_element_type=f32)


def wide_row(ref, index):
    return ref[pl.ds(pl.multiple_of(index, 4), 4), :]


def chunk_of(tile):
    return jnp.concatenate([tile[j * PITCH : j * PITCH + CHUNK, :] for j in range(4)], axis=1)


def list_chunks(chunks, low_ref, high_ref, own_columns, outer, chunk_list):
    def step(i, counts):
        inner_count, outer_count = counts
        halo = (low_ref[i] < HALO) | (high_ref[i] >= HALO + own_columns)
        early = jnp.logical_not(halo) & (inner_count < LIMIT)
        count = outer_count if outer else inner_count

        @pl.when(jnp.logical_not(early) if outer else early)
        def _():
            chunk_list[count] = i

        return inner_count + jnp.where(early, 1, 0), outer_count + jnp.where(early, 0, 1)

    return lax.fori_loop(0, chunks, step, (jnp.int32(0), jnp.int32(0)))[1 if outer else 0]


def list_columns(count, first_chunk, low_ref, high_ref, chunk_list, column_list, offset_list):
    slot0 = lax.shift_right_logical(first_chunk, 2)
    total = jnp.int32(0)
    seg_first = jnp.int32(1000)
    seg_last = jnp.int32(-1)
    seg_start = jnp.int32(0)
    for slot in range(SLOTS):

        def step(t, carry):
            low, high = carry
            i = chunk_list[t]
            here = lax.shift_right_logical(first_chunk + i, 2) == slot0 + slot
            return (
                jnp.where(here, jnp.minimum(low, low_ref[i]), low),
                jnp.where(here, jnp.maximum(high, high_ref[i]), high),
            )

        low, high = lax.fori_loop(0, count, step, (jnp.int32(1000), jnp.int32(-1)))
        has = high >= 0
        joins = has & (low >= seg_first) & (low <= seg_last + 1)
        begin = jnp.where(joins, seg_last + 1, low)
        fresh = jnp.where(has, jnp.maximum(high - begin + 1, 0), 0)
        base = total

        def put(j, carry):
            column_list[base + j] = begin + j
            return carry

        lax.fori_loop(0, fresh, put, 0)
        opens = has & jnp.logical_not(joins)
        seg_start = jnp.where(opens, total, seg_start)
        seg_first = jnp.where(opens, low, seg_first)
        seg_last = jnp.where(opens, high, jnp.maximum(seg_last, high))
        total = total + fresh
        offset_list[slot] = (seg_start - seg_first) * (LAT * 4)
    return total


def block_kernel(outer, chunks, own_columns, channels, nodes, *refs):
    place, low_ref, high_ref, grid = refs[:4]
    refs = refs[4:]
    if outer:
        low_own, low_swap, high_own, high_swap = refs[:4]
        refs = refs[4:]
    points, embed_in, embed_bias, ids, features = refs[:5]
    bundles = refs[5:9]
    meshes = refs[9:13]
    refs = refs[13:]
    if outer:
        messages = refs[:4]
        refs = refs[4:]
        message_bias, first_totals, first_tally, *parts = refs[:7]
        totals, tally = refs[-2:]
        refs = refs[7:-2]
    else:
        totals, tally = refs[:2]
        refs = refs[2:]
    (table, columns, sent, got, inputs, rows, embed_weight, send_weight, recv_weight,
     message_weight, mesh, extras, placed, placed_s, recv_s, chunk_list, column_list, offset_list,
     in_sems, sems) = refs
    k = place[0]
    core = lax.bitwise_and(k, 1)
    first_chunk = k * chunks
    count = list_chunks(chunks, low_ref, high_ref, own_columns, outer, chunk_list)
    total = list_columns(
        count, first_chunk, low_ref, high_ref, chunk_list, column_list, offset_list
    )

    copies = []
    for j in range(4):
        lanes = pl.ds(j * 128, 128)
        copies.append((bundles[j].at[pl.ds(0, 512)], send_weight.at[:, lanes]))
        copies.append((bundles[j].at[pl.ds(512, 512)], recv_weight.at[:, lanes]))
        copies.append((bundles[j].at[pl.ds(1024, 16)], extras.at[j]))
        at = pl.multiple_of(jnp.bitwise_xor(k, j) * 128, 128)
        copies.append((meshes[j], mesh.at[:, pl.ds(at, 128)]))
    copies = [pltpu.make_async_copy(a, b, sems.at[n]) for n, (a, b) in enumerate(copies)]
    late = []
    if outer:
        for j in range(4):
            late.append(
                pltpu.make_async_copy(
                    messages[j], message_weight.at[pl.ds(j * 128, 128)], sems.at[16 + j]
                )
            )
        for copy in late:
            copy.start()
        totals[...] = first_totals[...]
        tally[...] = first_tally[...]
    else:
        totals[...] = jnp.zeros_like(totals)
        tally[...] = jnp.zeros_like(tally)

    def fetch(source, column, slot):
        start = pl.multiple_of(column * LAT, 128)
        pltpu.make_async_copy(
            source.at[:, pl.ds(start, LAT)], columns.at[slot], in_sems.at[slot]
        ).start()

    def start_column(i):
        column = column_list[i]
        slot = lax.rem(i, BUFFERS)
        if not outer:
            fetch(grid, column - HALO, slot)
            return
        inside = (column >= HALO) & (column < HALO + own_columns)

        @pl.when(inside)
        def _():
            fetch(grid, column - HALO, slot)

        for is_side, shift, direct, swapped in (
            (column < HALO, 0, low_own, low_swap),
            (column >= HALO + own_columns, HALO + own_columns, high_own, high_swap),
        ):
            place_in = column - shift
            half = lax.shift_right_arithmetic(place_in, 1)
            within = lax.bitwise_and(place_in, 1)

            @pl.when(is_side & (half == core))
            def _():
                fetch(direct, within, slot)

            @pl.when(is_side & (half != core))
            def _():
                fetch(swapped, within, slot)

    def turn(i, carry):
        slot = lax.rem(i, BUFFERS)

        @pl.when(i + BUFFERS - 1 < total)
        def _():
            start_column(i + BUFFERS - 1)

        pltpu.make_async_copy(
            grid.at[:, pl.ds(0, LAT)], columns.at[slot], in_sems.at[slot]
        ).wait()
        source = columns.at[slot]
        for l in range(LAT // 128):
            lanes = pl.ds(l * 128, 128)
            for j in range(4):
                top = min(channels, (j + 1) * 128)
                block = source[j * 128 : top, lanes]
                if top < (j + 1) * 128:
                    block = jnp.pad(block, ((0, (j + 1) * 128 - top), (0, 0)))
                row = pl.multiple_of((i * LAT + l * 128) * 4, 8)
                table[pl.ds(row + j, 128, stride=4), :] = block.T.astype(f32)
        return carry

    def indices(ref, t):
        return ref.at[pl.ds(pl.multiple_of(chunk_list[t] * 4, 4), 4)]

    def gather(source, picks, target):
        for e in range(CHUNK):
            target[pl.ds(e, 4, stride=PITCH), :] = wide_row(source, picks[e // 128, e % 128])

    index_copies = [
        pltpu.make_async_copy(placed, placed_s, sems.at[30]),
        pltpu.make_async_copy(ids, recv_s, sems.at[31]),
    ]

    @pl.when(count > 0)
    def _():
        for b in range(BUFFERS - 1):

            @pl.when(b < total)
            def _():
                start_column(b)

        for i in range(chunks):
            slot = lax.shift_right_logical(first_chunk + i, 2) - lax.shift_right_logical(
                first_chunk, 2
            )
            placed[i * 4 : i * 4 + 4, :] = points[i * 4 : i * 4 + 4, :] + offset_list[slot]
        for copy in index_copies:
            copy.start()
        for copy in copies:
            copy.start()
        embed_weight[464:512, :] = jnp.zeros((48, 512), bf16)
        embed_weight[0:channels, :] = embed_in[...]
        lax.fori_loop(0, total, turn, 0)
        for copy in copies + index_copies:
            copy.wait()
        bias = jnp.concatenate(
            [
                sum(extras[j, 4 + r : 5 + r, :].astype(f32) for r in range(3))
                for j in range(4)
            ],
            axis=1,
        )
        terms = dot(mesh[...], recv_weight[...]) + bias
        for j in range(4):
            rows[pl.ds(j, nodes, stride=4), :] = terms[:, j * 128 : (j + 1) * 128]
        gather(table, indices(placed_s, 0), sent)
        features_by = jnp.concatenate([extras[j, 0:4, :] for j in range(4)], axis=1)

        def work(t, carry):
            i = chunk_list[t]
            inputs[...] = chunk_of(sent).astype(bf16)
            gather(rows, indices(recv_s, t), got)
            latent = silu(dot(inputs[...], embed_weight[...]) + embed_bias[...]).astype(bf16)
            before = (
                dot(latent, send_weight[...])
                + chunk_of(got)
                + lax.dot_general(
                    features[first_chunk + i], features_by, (((0,), (0,)), ((), ())),
                    preferred_element_type=f32,
                )
            )
            hidden = silu(before).astype(bf16)
            node = lax.broadcasted_iota(jnp.int32, (nodes, 128), 0) * 4
            hots = [
                jnp.where(node == ids[pl.ds(i * 4 + q, 1), :], 1.0, 0.0) for q in range(4)
            ]
            hot = jnp.concatenate([value.astype(bf16) for value in hots], axis=1)
            gather(table, indices(placed_s, jnp.minimum(t + 1, count - 1)), sent)
            totals[...] += dot(hot, hidden)
            tally[...] += (hots[0] + hots[1]) + (hots[2] + hots[3])
            return carry

        lax.fori_loop(0, count, work, 0)

    if not outer:
        return
    counts = jnp.sum(tally[...], axis=1, keepdims=True)
    whole = totals[...]
    upper = whole.astype(bf16)
    lower = (whole - upper.astype(f32)).astype(bf16)
    for copy in late:
        copy.wait()
    totals[...] = (
        dot(upper, message_weight[...])
        + dot(lower, message_weight[...])
        + counts * message_bias[...]
    )
    for r in range(2):
        mine = pl.multiple_of(jnp.bitwise_xor(k, 2 * r) * 128, 128)
        theirs = pl.multiple_of(jnp.bitwise_xor(k, 2 * r + 1) * 128, 128)
        parts[r][...] = totals[:, pl.ds(mine, 128)]
        parts[2 + r][...] = totals[:, pl.ds(theirs, 128)]


def weights_kernel(feature_weight, hidden_bias, sender_weight, receiver_weight, bundle):
    bundle[0:512, :] = sender_weight[...]
    bundle[512:1024, :] = receiver_weight[...]
    bias = hidden_bias[...]
    upper = bias.astype(bf16)
    middle = (bias - upper.astype(f32)).astype(bf16)
    lower = (bias - upper.astype(f32) - middle.astype(f32)).astype(bf16)
    bundle[1024:1040, :] = jnp.concatenate(
        [feature_weight[...].astype(f32)]
        + [value.astype(f32) for value in (upper, middle, lower)]
        + [jnp.zeros((9, bias.shape[1]), f32)],
        axis=0,
    ).astype(bf16)


def pack_kernel(chunks, points_own, all_points, nodes, lon_ref, place, senders, receivers, grid,
                points, ids, low_ref, high_ref, low_half, high_half, sems):
    lon = lon_ref[0]
    k = place[0]
    half = HALO * LAT // 2
    side = lax.bitwise_and(k, 1) * half
    low_at = pl.multiple_of(points_own - 2 * half + side, 128)
    copies = [
        pltpu.make_async_copy(grid.at[:, pl.ds(low_at, half)], low_half, sems.at[0]),
        pltpu.make_async_copy(
            grid.at[:, pl.ds(pl.multiple_of(side, 128), half)], high_half, sems.at[1]
        ),
    ]
    for copy in copies:
        copy.start()
    for i in range(chunks):
        rows = pl.ds(pl.multiple_of((k * chunks + i) * 4, 4), 4)
        point = senders[rows, :] - lon * points_own + HALO * LAT
        point = jnp.where(point < 0, point + all_points, point)
        point = jnp.where(point >= all_points, point - all_points, point)
        points[i * 4 : i * 4 + 4, :] = point * 4
        ids[i * 4 : i * 4 + 4, :] = (receivers[rows, :] - lon * nodes) * 4
        for ref, end in ((low_ref, jnp.min(point)), (high_ref, jnp.max(point))):
            ref[i] = lax.shift_right_logical(lax.shift_right_logical(end, 7) * 13108, 16)
    for copy in copies:
        copy.wait()


def weights_call(share, operands):
    return pl.pallas_call(
        weights_kernel,
        out_shape=jax.ShapeDtypeStruct((1040, share), bf16),
        in_specs=[VMEM] * 4,
        out_specs=VMEM,
        name="weights",
    )(*operands)


def pack_call(chunks, points_own, all_points, channels, nodes, operands):
    half = HALO * LAT // 2
    index = jax.ShapeDtypeStruct((chunks * 4, 128), jnp.int32)
    ends = jax.ShapeDtypeStruct((chunks,), jnp.int32)
    side = jax.ShapeDtypeStruct((channels, half), bf16)
    return pl.pallas_call(
        functools.partial(pack_kernel, chunks, points_own, all_points, nodes),
        out_shape=(index, index, ends, ends, side, side),
        in_specs=[SMEM] * 2 + [VMEM] * 2 + [ANY],
        out_specs=(VMEM, VMEM, SMEM, SMEM, VMEM, VMEM),
        scratch_shapes=[pltpu.SemaphoreType.DMA((2,))],
        name="pack",
    )(*operands)


VMEM = pl.BlockSpec(memory_space=pltpu.VMEM)
SMEM = pl.BlockSpec(memory_space=pltpu.SMEM)
ANY = pl.BlockSpec(memory_space=pl.ANY)


def block_call(outer, chunks, own_columns, channels, nodes, operands):
    width = 512
    part = jax.ShapeDtypeStruct((nodes, 128), f32)
    sums = (
        jax.ShapeDtypeStruct((nodes, width), f32),
        jax.ShapeDtypeStruct((nodes, 128), f32),
    )
    specs = [SMEM] * 3 + [ANY] * (5 if outer else 1) + [VMEM] * 5 + [ANY] * 8
    if outer:
        specs = specs + [ANY] * 4 + [VMEM] * 3
    slots = SLOTS * WINDOW
    edges = chunks * CHUNK
    square = pltpu.VMEM((width, width), bf16)
    return pl.pallas_call(
        functools.partial(block_kernel, outer, chunks, own_columns, channels, nodes),
        out_shape=(part,) * 4 if outer else sums,
        in_specs=specs,
        out_specs=(VMEM,) * (4 if outer else 2),
        scratch_shapes=[
            pltpu.VMEM((slots * LAT * 4, 128), f32),
            pltpu.VMEM((BUFFERS, channels, LAT), bf16),
            pltpu.VMEM((4 * PITCH, 128), f32),
            pltpu.VMEM((4 * PITCH, 128), f32),
            pltpu.VMEM((CHUNK, width), bf16),
            pltpu.VMEM((nodes * 4, 128), f32),
            square,
            square,
            square,
            square,
            pltpu.VMEM((nodes, width), bf16),
            pltpu.VMEM((4, 16, 128), bf16),
            pltpu.VMEM((chunks * 4, 128), jnp.int32),
            pltpu.SMEM((chunks * 4, 128), jnp.int32),
            pltpu.SMEM((chunks * 4, 128), jnp.int32),
            pltpu.SMEM((16,), jnp.int32),
            pltpu.SMEM((32,), jnp.int32),
            pltpu.SMEM((8,), jnp.int32),
            pltpu.SemaphoreType.DMA((BUFFERS,)),
            pltpu.SemaphoreType.DMA((32,)),
        ]
        + ([pltpu.VMEM(value.shape, f32) for value in sums] if outer else []),
        compiler_params=pltpu.CompilerParams(vmem_limit_bytes=60 * 2**20),
        cost_estimate=pl.CostEstimate(
            flops=2 * edges * width * (2 * width + nodes),
            bytes_accessed=2 * edges * width,
            transcendentals=2 * edges * width,
        ),
        name="block_outer" if outer else "block_inner",
    )(*operands)


def encoder(
    grid_inputs,
    embed_weight,
    embed_bias,
    mesh_latent,
    edge_features,
    senders,
    receivers,
    sender_weight,
    receiver_weight,
    feature_weight,
    hidden_bias,
    message_weight,
    message_bias,
    norm_gain,
    norm_shift,
):
    lon_count = lax.axis_size("lon")
    ch_count = lax.axis_size("ch")
    lon_place = lax.axis_index("lon")
    ch_place = lax.axis_index("ch")
    place = ch_place[None].astype(jnp.int32)
    points_own, channels = grid_inputs.shape
    own_columns = points_own // LAT
    mesh_nodes = mesh_latent.shape[0]
    full_width = message_weight.shape[1]
    edge_count = senders.shape[0]
    all_chunks = edge_count // CHUNK
    chunks = all_chunks // ch_count

    swap = [(i, i ^ 1) for i in range(ch_count)]
    across = [(i, i ^ 2) for i in range(ch_count)]
    facing = [
        (lon * ch_count + ch, (lon ^ 4) * ch_count + (ch ^ 2))
        for lon in range(lon_count)
        for ch in range(ch_count)
    ]
    forward = [(i, (i + 1) % lon_count) for i in range(lon_count)]
    backward = [(target, source) for source, target in forward]

    flat = grid_inputs.T
    lon_scalar = lon_place[None].astype(jnp.int32)
    bundle = weights_call(
        message_weight.shape[0],
        [feature_weight, hidden_bias[None, :], sender_weight, receiver_weight],
    )
    bundle_far = lax.ppermute(bundle, ("lon", "ch"), facing)
    mesh_far = lax.ppermute(mesh_latent, "ch", across)
    points, ids, low_column, high_column, low_half, high_half = pack_call(
        chunks, points_own, points_own * lon_count, channels, mesh_nodes,
        [lon_scalar, place, senders.reshape(-1, 128), receivers.reshape(-1, 128), flat],
    )
    low_own = lax.ppermute(low_half, "lon", forward)
    high_own = lax.ppermute(high_half, "lon", backward)
    low_swap = lax.ppermute(low_own, "ch", swap)
    high_swap = lax.ppermute(high_own, "ch", swap)
    bundle_near = lax.ppermute(bundle, "ch", swap)
    bundle_last = lax.ppermute(bundle_far, "ch", swap)
    mesh_near = lax.ppermute(mesh_latent, "ch", swap)
    mesh_last = lax.ppermute(mesh_far, "ch", swap)
    message_far = lax.ppermute(message_weight, ("lon", "ch"), facing)
    message_near = lax.ppermute(message_weight, "ch", swap)
    message_last = lax.ppermute(message_far, "ch", swap)
    feature_blocks = jnp.transpose(
        edge_features.reshape(edge_features.shape[0], all_chunks, CHUNK), (1, 0, 2)
    )

    call = functools.partial(
        block_call, chunks=chunks, own_columns=own_columns, channels=channels, nodes=mesh_nodes
    )
    scalars = [place, low_column, high_column, flat]
    arrays = [
        points, embed_weight, embed_bias[None, :], ids, feature_blocks,
        bundle, bundle_near, bundle_far, bundle_last,
        mesh_latent, mesh_near, mesh_far, mesh_last,
    ]
    totals, tally = call(False, operands=scalars + arrays)
    keep_here, keep_far, send_here, send_far = call(
        True,
        operands=scalars
        + [low_own, low_swap, high_own, high_swap]
        + arrays
        + [message_weight, message_near, message_far, message_last]
        + [message_bias[None, :], totals, tally],
    )
    far = keep_far + lax.ppermute(send_far, "ch", swap)
    far = lax.ppermute(far.astype(bf16), "ch", across).astype(f32)
    node_share = keep_here + lax.ppermute(send_here, "ch", swap) + far
    first_sum, second = lax.psum(
        (
            jnp.sum(node_share, axis=1, keepdims=True),
            jnp.sum(jnp.square(node_share), axis=1, keepdims=True),
        ),
        "ch",
    )
    centre = first_sum / full_width
    spread = second / full_width - jnp.square(centre)
    normed = (node_share - centre) * lax.rsqrt(spread + 1.0)
    return (mesh_latent.astype(f32) + normed * norm_gain + norm_shift).astype(bf16)


def solution(mesh):
    return jax.shard_map(
        encoder,
        mesh=mesh,
        in_specs=(
            P("lon", None),
            P(),
            P(),
            P("lon", "ch"),
            P(None, "lon"),
            P("lon"),
            P("lon"),
            P(None, "ch"),
            P(None, "ch"),
            P(None, "ch"),
            P("ch"),
            P("ch", None),
            P(),
            P("ch"),
            P("ch"),
        ),
        out_specs=P("lon", "ch"),
        check_vma=False,
    )
```

```python
import functools

import jax
import jax.numpy as jnp
from jax import lax
from jax.experimental import pallas as pl
from jax.experimental.pallas import tpu as pltpu
from jax.sharding import PartitionSpec as P


LAT = 640
HALO = 4
CHUNK = 512
SLOTS = 4
WINDOW = 7
PITCH = CHUNK + 8
BUFFERS = 8
LIMIT = 7

f32 = jnp.float32
bf16 = jnp.bfloat16


def silu(value):
    half = 0.5 * value
    return half + half * jnp.tanh(half)


def dot(left, right):
    return jnp.dot(left, right, preferred_element_type=f32)


def wide_row(ref, index):
    return ref[pl.ds(pl.multiple_of(index, 4), 4), :]


def chunk_of(tile):
    return jnp.concatenate([tile[j * PITCH : j * PITCH + CHUNK, :] for j in range(4)], axis=1)


def list_chunks(chunks, low_ref, high_ref, own_columns, outer, chunk_list):
    def step(i, counts):
        inner_count, outer_count = counts
        halo = (low_ref[i] < HALO) | (high_ref[i] >= HALO + own_columns)
        early = jnp.logical_not(halo) & (inner_count < LIMIT)
        count = outer_count if outer else inner_count

        @pl.when(jnp.logical_not(early) if outer else early)
        def _():
            chunk_list[count] = i

        return inner_count + jnp.where(early, 1, 0), outer_count + jnp.where(early, 0, 1)

    return lax.fori_loop(0, chunks, step, (jnp.int32(0), jnp.int32(0)))[1 if outer else 0]


def list_columns(count, first_chunk, low_ref, high_ref, chunk_list, column_list, offset_list):
    slot0 = lax.shift_right_logical(first_chunk, 2)
    total = jnp.int32(0)
    seg_first = jnp.int32(1000)
    seg_last = jnp.int32(-1)
    seg_start = jnp.int32(0)
    for slot in range(SLOTS):

        def step(t, carry):
            low, high = carry
            i = chunk_list[t]
            here = lax.shift_right_logical(first_chunk + i, 2) == slot0 + slot
            return (
                jnp.where(here, jnp.minimum(low, low_ref[i]), low),
                jnp.where(here, jnp.maximum(high, high_ref[i]), high),
            )

        low, high = lax.fori_loop(0, count, step, (jnp.int32(1000), jnp.int32(-1)))
        has = high >= 0
        joins = has & (low >= seg_first) & (low <= seg_last + 1)
        begin = jnp.where(joins, seg_last + 1, low)
        fresh = jnp.where(has, jnp.maximum(high - begin + 1, 0), 0)
        base = total

        def put(j, carry):
            column_list[base + j] = begin + j
            return carry

        lax.fori_loop(0, fresh, put, 0)
        opens = has & jnp.logical_not(joins)
        seg_start = jnp.where(opens, total, seg_start)
        seg_first = jnp.where(opens, low, seg_first)
        seg_last = jnp.where(opens, high, jnp.maximum(seg_last, high))
        total = total + fresh
        offset_list[slot] = (seg_start - seg_first) * (LAT * 4)
    return total


def block_kernel(outer, chunks, own_columns, channels, nodes, *refs):
    place, low_ref, high_ref, grid = refs[:4]
    refs = refs[4:]
    if outer:
        low_own, low_swap, high_own, high_swap = refs[:4]
        refs = refs[4:]
    points, embed_in, embed_bias, ids, features = refs[:5]
    bundles = refs[5:9]
    meshes = refs[9:13]
    refs = refs[13:]
    if outer:
        messages = refs[:4]
        refs = refs[4:]
        message_bias, first_totals, first_tally, *parts = refs[:7]
        totals, tally = refs[-2:]
        refs = refs[7:-2]
    else:
        totals, tally = refs[:2]
        refs = refs[2:]
    (table, columns, sent, got, inputs, rows, embed_weight, send_weight, recv_weight,
     message_weight, mesh, extras, placed, placed_s, recv_s, chunk_list, column_list, offset_list,
     in_sems, sems) = refs
    k = place[0]
    core = lax.bitwise_and(k, 1)
    first_chunk = k * chunks
    count = list_chunks(chunks, low_ref, high_ref, own_columns, outer, chunk_list)
    total = list_columns(
        count, first_chunk, low_ref, high_ref, chunk_list, column_list, offset_list
    )

    copies = []
    for j in range(4):
        lanes = pl.ds(j * 128, 128)
        copies.append((bundles[j].at[pl.ds(0, 512)], send_weight.at[:, lanes]))
        copies.append((bundles[j].at[pl.ds(512, 512)], recv_weight.at[:, lanes]))
        copies.append((bundles[j].at[pl.ds(1024, 16)], extras.at[j]))
        at = pl.multiple_of(jnp.bitwise_xor(k, j) * 128, 128)
        copies.append((meshes[j], mesh.at[:, pl.ds(at, 128)]))
    copies = [pltpu.make_async_copy(a, b, sems.at[n]) for n, (a, b) in enumerate(copies)]
    late = []
    if outer:
        for j in range(4):
            late.append(
                pltpu.make_async_copy(
                    messages[j], message_weight.at[pl.ds(j * 128, 128)], sems.at[16 + j]
                )
            )
        for copy in late:
            copy.start()
        totals[...] = first_totals[...]
        tally[...] = first_tally[...]
    else:
        totals[...] = jnp.zeros_like(totals)
        tally[...] = jnp.zeros_like(tally)

    def fetch(source, column, slot):
        start = pl.multiple_of(column * LAT, 128)
        pltpu.make_async_copy(
            source.at[:, pl.ds(start, LAT)], columns.at[slot], in_sems.at[slot]
        ).start()

    def start_column(i):
        column = column_list[i]
        slot = lax.rem(i, BUFFERS)
        if not outer:
            fetch(grid, column - HALO, slot)
            return
        inside = (column >= HALO) & (column < HALO + own_columns)

        @pl.when(inside)
        def _():
            fetch(grid, column - HALO, slot)

        for is_side, shift, direct, swapped in (
            (column < HALO, 0, low_own, low_swap),
            (column >= HALO + own_columns, HALO + own_columns, high_own, high_swap),
        ):
            place_in = column - shift
            half = lax.shift_right_arithmetic(place_in, 1)
            within = lax.bitwise_and(place_in, 1)

            @pl.when(is_side & (half == core))
            def _():
                fetch(direct, within, slot)

            @pl.when(is_side & (half != core))
            def _():
                fetch(swapped, within, slot)

    def turn(i, carry):
        slot = lax.rem(i, BUFFERS)

        @pl.when(i + BUFFERS - 1 < total)
        def _():
            start_column(i + BUFFERS - 1)

        pltpu.make_async_copy(
            grid.at[:, pl.ds(0, LAT)], columns.at[slot], in_sems.at[slot]
        ).wait()
        source = columns.at[slot]
        for l in range(LAT // 128):
            lanes = pl.ds(l * 128, 128)
            for j in range(4):
                top = min(channels, (j + 1) * 128)
                block = source[j * 128 : top, lanes]
                if top < (j + 1) * 128:
                    block = jnp.pad(block, ((0, (j + 1) * 128 - top), (0, 0)))
                row = pl.multiple_of((i * LAT + l * 128) * 4, 8)
                table[pl.ds(row + j, 128, stride=4), :] = block.T.astype(f32)
        return carry

    def indices(ref, t):
        return ref.at[pl.ds(pl.multiple_of(chunk_list[t] * 4, 4), 4)]

    def gather(source, picks, target):
        for e in range(CHUNK):
            target[pl.ds(e, 4, stride=PITCH), :] = wide_row(source, picks[e // 128, e % 128])

    index_copies = [
        pltpu.make_async_copy(placed, placed_s, sems.at[30]),
        pltpu.make_async_copy(ids, recv_s, sems.at[31]),
    ]

    @pl.when(count > 0)
    def _():
        for b in range(BUFFERS - 1):

            @pl.when(b < total)
            def _():
                start_column(b)

        for i in range(chunks):
            slot = lax.shift_right_logical(first_chunk + i, 2) - lax.shift_right_logical(
                first_chunk, 2
            )
            placed[i * 4 : i * 4 + 4, :] = points[i * 4 : i * 4 + 4, :] + offset_list[slot]
        for copy in index_copies:
            copy.start()
        for copy in copies:
            copy.start()
        embed_weight[464:512, :] = jnp.zeros((48, 512), bf16)
        embed_weight[0:channels, :] = embed_in[...]
        lax.fori_loop(0, total, turn, 0)
        for copy in copies + index_copies:
            copy.wait()
        bias = jnp.concatenate(
            [
                sum(extras[j, 4 + r : 5 + r, :].astype(f32) for r in range(3))
                for j in range(4)
            ],
            axis=1,
        )
        terms = dot(mesh[...], recv_weight[...]) + bias
        for j in range(4):
            rows[pl.ds(j, nodes, stride=4), :] = terms[:, j * 128 : (j + 1) * 128]
        gather(table, indices(placed_s, 0), sent)
        features_by = jnp.concatenate([extras[j, 0:4, :] for j in range(4)], axis=1)

        def work(t, carry):
            i = chunk_list[t]
            inputs[...] = chunk_of(sent).astype(bf16)
            gather(rows, indices(recv_s, t), got)
            latent = silu(dot(inputs[...], embed_weight[...]) + embed_bias[...]).astype(bf16)
            before = (
                dot(latent, send_weight[...])
                + chunk_of(got)
                + lax.dot_general(
                    features[first_chunk + i], features_by, (((0,), (0,)), ((), ())),
                    preferred_element_type=f32,
                )
            )
            hidden = silu(before).astype(bf16)
            node = lax.broadcasted_iota(jnp.int32, (nodes, 128), 0) * 4
            hots = [
                jnp.where(node == ids[pl.ds(i * 4 + q, 1), :], 1.0, 0.0) for q in range(4)
            ]
            hot = jnp.concatenate([value.astype(bf16) for value in hots], axis=1)
            gather(table, indices(placed_s, jnp.minimum(t + 1, count - 1)), sent)
            totals[...] += dot(hot, hidden)
            tally[...] += (hots[0] + hots[1]) + (hots[2] + hots[3])
            return carry

        lax.fori_loop(0, count, work, 0)

    if not outer:
        return
    counts = jnp.sum(tally[...], axis=1, keepdims=True)
    whole = totals[...]
    upper = whole.astype(bf16)
    lower = (whole - upper.astype(f32)).astype(bf16)
    for copy in late:
        copy.wait()
    totals[...] = (
        dot(upper, message_weight[...])
        + dot(lower, message_weight[...])
        + counts * message_bias[...]
    )
    for r in range(2):
        mine = pl.multiple_of(jnp.bitwise_xor(k, 2 * r) * 128, 128)
        theirs = pl.multiple_of(jnp.bitwise_xor(k, 2 * r + 1) * 128, 128)
        parts[r][...] = totals[:, pl.ds(mine, 128)]
        parts[2 + r][...] = totals[:, pl.ds(theirs, 128)]


def weights_kernel(feature_weight, hidden_bias, sender_weight, receiver_weight, bundle):
    bundle[0:512, :] = sender_weight[...]
    bundle[512:1024, :] = receiver_weight[...]
    bias = hidden_bias[...]
    upper = bias.astype(bf16)
    middle = (bias - upper.astype(f32)).astype(bf16)
    lower = (bias - upper.astype(f32) - middle.astype(f32)).astype(bf16)
    bundle[1024:1040, :] = jnp.concatenate(
        [feature_weight[...].astype(f32)]
        + [value.astype(f32) for value in (upper, middle, lower)]
        + [jnp.zeros((9, bias.shape[1]), f32)],
        axis=0,
    ).astype(bf16)


def pack_kernel(chunks, points_own, all_points, nodes, lon_ref, place, senders, receivers, grid,
                points, ids, low_ref, high_ref, low_half, high_half, pieces, sems):
    lon = lon_ref[0]
    k = place[0]
    half = HALO * LAT // 2
    side = lax.bitwise_and(k, 1) * half
    low_at = pl.multiple_of(points_own - 2 * half + side, 128)
    copies = []
    for n, (source_at, target, target_at) in enumerate(
        (begin + step, target, step)
        for begin, target in ((low_at, low_half), (side, high_half))
        for step in (0, LAT)
    ):
        copies.append(
            (
                pltpu.make_async_copy(
                    grid.at[:, pl.ds(pl.multiple_of(source_at, 128), LAT)],
                    pieces.at[n],
                    sems.at[n],
                ),
                pltpu.make_async_copy(
                    pieces.at[n], target.at[:, pl.ds(target_at, LAT)], sems.at[4 + n]
                ),
            )
        )
    for first, _ in copies:
        first.start()
    for i in range(chunks):
        rows = pl.ds(pl.multiple_of((k * chunks + i) * 4, 4), 4)
        point = senders[rows, :] - lon * points_own + HALO * LAT
        point = jnp.where(point < 0, point + all_points, point)
        point = jnp.where(point >= all_points, point - all_points, point)
        points[i * 4 : i * 4 + 4, :] = point * 4
        ids[i * 4 : i * 4 + 4, :] = (receivers[rows, :] - lon * nodes) * 4
        for ref, end in ((low_ref, jnp.min(point)), (high_ref, jnp.max(point))):
            ref[i] = lax.shift_right_logical(lax.shift_right_logical(end, 7) * 13108, 16)
    for first, then in copies:
        first.wait()
        then.start()
    for _, then in copies:
        then.wait()


def weights_call(share, operands):
    return pl.pallas_call(
        weights_kernel,
        out_shape=jax.ShapeDtypeStruct((1040, share), bf16),
        in_specs=[VMEM] * 4,
        out_specs=VMEM,
        name="weights",
    )(*operands)


def pack_call(chunks, points_own, all_points, channels, nodes, operands):
    half = HALO * LAT // 2
    index = jax.ShapeDtypeStruct((chunks * 4, 128), jnp.int32)
    ends = jax.ShapeDtypeStruct((chunks,), jnp.int32)
    side = jax.ShapeDtypeStruct((channels, half), bf16)
    return pl.pallas_call(
        functools.partial(pack_kernel, chunks, points_own, all_points, nodes),
        out_shape=(index, index, ends, ends, side, side),
        in_specs=[SMEM] * 2 + [VMEM] * 2 + [ANY],
        out_specs=(VMEM, VMEM, SMEM, SMEM, ANY, ANY),
        scratch_shapes=[
            pltpu.VMEM((4, channels, LAT), bf16),
            pltpu.SemaphoreType.DMA((8,)),
        ],
        name="pack",
    )(*operands)


VMEM = pl.BlockSpec(memory_space=pltpu.VMEM)
SMEM = pl.BlockSpec(memory_space=pltpu.SMEM)
ANY = pl.BlockSpec(memory_space=pl.ANY)


def block_call(outer, chunks, own_columns, channels, nodes, operands):
    width = 512
    part = jax.ShapeDtypeStruct((nodes, 128), f32)
    sums = (
        jax.ShapeDtypeStruct((nodes, width), f32),
        jax.ShapeDtypeStruct((nodes, 128), f32),
    )
    specs = [SMEM] * 3 + [ANY] * (5 if outer else 1) + [VMEM] * 5 + [ANY] * 8
    if outer:
        specs = specs + [ANY] * 4 + [VMEM] * 3
    slots = SLOTS * WINDOW
    edges = chunks * CHUNK
    square = pltpu.VMEM((width, width), bf16)
    return pl.pallas_call(
        functools.partial(block_kernel, outer, chunks, own_columns, channels, nodes),
        out_shape=(part,) * 4 if outer else sums,
        in_specs=specs,
        out_specs=(VMEM,) * (4 if outer else 2),
        scratch_shapes=[
            pltpu.VMEM((slots * LAT * 4, 128), f32),
            pltpu.VMEM((BUFFERS, channels, LAT), bf16),
            pltpu.VMEM((4 * PITCH, 128), f32),
            pltpu.VMEM((4 * PITCH, 128), f32),
            pltpu.VMEM((CHUNK, width), bf16),
            pltpu.VMEM((nodes * 4, 128), f32),
            square,
            square,
            square,
            square,
            pltpu.VMEM((nodes, width), bf16),
            pltpu.VMEM((4, 16, 128), bf16),
            pltpu.VMEM((chunks * 4, 128), jnp.int32),
            pltpu.SMEM((chunks * 4, 128), jnp.int32),
            pltpu.SMEM((chunks * 4, 128), jnp.int32),
            pltpu.SMEM((16,), jnp.int32),
            pltpu.SMEM((32,), jnp.int32),
            pltpu.SMEM((8,), jnp.int32),
            pltpu.SemaphoreType.DMA((BUFFERS,)),
            pltpu.SemaphoreType.DMA((32,)),
        ]
        + ([pltpu.VMEM(value.shape, f32) for value in sums] if outer else []),
        compiler_params=pltpu.CompilerParams(vmem_limit_bytes=60 * 2**20),
        cost_estimate=pl.CostEstimate(
            flops=2 * edges * width * (2 * width + nodes),
            bytes_accessed=2 * edges * width,
            transcendentals=2 * edges * width,
        ),
        name="block_outer" if outer else "block_inner",
    )(*operands)


def encoder(
    grid_inputs,
    embed_weight,
    embed_bias,
    mesh_latent,
    edge_features,
    senders,
    receivers,
    sender_weight,
    receiver_weight,
    feature_weight,
    hidden_bias,
    message_weight,
    message_bias,
    norm_gain,
    norm_shift,
):
    lon_count = lax.axis_size("lon")
    ch_count = lax.axis_size("ch")
    lon_place = lax.axis_index("lon")
    ch_place = lax.axis_index("ch")
    place = ch_place[None].astype(jnp.int32)
    points_own, channels = grid_inputs.shape
    own_columns = points_own // LAT
    mesh_nodes = mesh_latent.shape[0]
    full_width = message_weight.shape[1]
    edge_count = senders.shape[0]
    all_chunks = edge_count // CHUNK
    chunks = all_chunks // ch_count

    swap = [(i, i ^ 1) for i in range(ch_count)]
    across = [(i, i ^ 2) for i in range(ch_count)]
    facing = [
        (lon * ch_count + ch, (lon ^ 4) * ch_count + (ch ^ 2))
        for lon in range(lon_count)
        for ch in range(ch_count)
    ]
    forward = [(i, (i + 1) % lon_count) for i in range(lon_count)]
    backward = [(target, source) for source, target in forward]

    flat = grid_inputs.T
    lon_scalar = lon_place[None].astype(jnp.int32)
    bundle = weights_call(
        message_weight.shape[0],
        [feature_weight, hidden_bias[None, :], sender_weight, receiver_weight],
    )
    bundle_far = lax.ppermute(bundle, ("lon", "ch"), facing)
    mesh_far = lax.ppermute(mesh_latent, "ch", across)
    points, ids, low_column, high_column, low_half, high_half = pack_call(
        chunks, points_own, points_own * lon_count, channels, mesh_nodes,
        [lon_scalar, place, senders.reshape(-1, 128), receivers.reshape(-1, 128), flat],
    )
    low_own = lax.ppermute(low_half, "lon", forward)
    high_own = lax.ppermute(high_half, "lon", backward)
    low_swap = lax.ppermute(low_own, "ch", swap)
    high_swap = lax.ppermute(high_own, "ch", swap)
    bundle_near = lax.ppermute(bundle, "ch", swap)
    bundle_last = lax.ppermute(bundle_far, "ch", swap)
    mesh_near = lax.ppermute(mesh_latent, "ch", swap)
    mesh_last = lax.ppermute(mesh_far, "ch", swap)
    message_far = lax.ppermute(message_weight, ("lon", "ch"), facing)
    message_near = lax.ppermute(message_weight, "ch", swap)
    message_last = lax.ppermute(message_far, "ch", swap)
    feature_blocks = jnp.transpose(
        edge_features.reshape(edge_features.shape[0], all_chunks, CHUNK), (1, 0, 2)
    )

    call = functools.partial(
        block_call, chunks=chunks, own_columns=own_columns, channels=channels, nodes=mesh_nodes
    )
    scalars = [place, low_column, high_column, flat]
    arrays = [
        points, embed_weight, embed_bias[None, :], ids, feature_blocks,
        bundle, bundle_near, bundle_far, bundle_last,
        mesh_latent, mesh_near, mesh_far, mesh_last,
    ]
    totals, tally = call(False, operands=scalars + arrays)
    keep_here, keep_far, send_here, send_far = call(
        True,
        operands=scalars
        + [low_own, low_swap, high_own, high_swap]
        + arrays
        + [message_weight, message_near, message_far, message_last]
        + [message_bias[None, :], totals, tally],
    )
    far = keep_far + lax.ppermute(send_far, "ch", swap)
    far = lax.ppermute(far.astype(bf16), "ch", across).astype(f32)
    node_share = keep_here + lax.ppermute(send_here, "ch", swap) + far
    sums = jnp.stack([jnp.sum(node_share, axis=1), jnp.sum(jnp.square(node_share), axis=1)])
    first_sum, second = jnp.sum(lax.all_gather(sums, "ch"), axis=0)[:, :, None]
    centre = first_sum / full_width
    spread = second / full_width - jnp.square(centre)
    normed = (node_share - centre) * lax.rsqrt(spread + 1.0)
    return (mesh_latent.astype(f32) + normed * norm_gain + norm_shift).astype(bf16)


def solution(mesh):
    return jax.shard_map(
        encoder,
        mesh=mesh,
        in_specs=(
            P("lon", None),
            P(),
            P(),
            P("lon", "ch"),
            P(None, "lon"),
            P("lon"),
            P("lon"),
            P(None, "ch"),
            P(None, "ch"),
            P(None, "ch"),
            P("ch"),
            P("ch", None),
            P(),
            P("ch"),
            P("ch"),
        ),
        out_specs=P("lon", "ch"),
        check_vma=False,
    )
```

```python
import functools

import jax
import jax.numpy as jnp
from jax import lax
from jax.experimental import pallas as pl
from jax.experimental.pallas import tpu as pltpu
from jax.sharding import PartitionSpec as P


LAT = 640
HALO = 4
CHUNK = 512
SLOTS = 4
WINDOW = 7
PITCH = CHUNK + 8
BUFFERS = 8
LIMIT = 7

f32 = jnp.float32
bf16 = jnp.bfloat16


def silu(value):
    half = 0.5 * value
    return half + half * jnp.tanh(half)


def dot(left, right):
    return jnp.dot(left, right, preferred_element_type=f32)


def wide_row(ref, index):
    return ref[pl.ds(pl.multiple_of(index, 4), 4), :]


def chunk_of(tile):
    return jnp.concatenate([tile[j * PITCH : j * PITCH + CHUNK, :] for j in range(4)], axis=1)


def list_chunks(chunks, low_ref, high_ref, own_columns, outer, chunk_list):
    def step(i, counts):
        inner_count, outer_count = counts
        halo = (low_ref[i, 0] < HALO) | (high_ref[i, 0] >= HALO + own_columns)
        early = jnp.logical_not(halo) & (inner_count < LIMIT)
        count = outer_count if outer else inner_count

        @pl.when(jnp.logical_not(early) if outer else early)
        def _():
            chunk_list[count] = i

        return inner_count + jnp.where(early, 1, 0), outer_count + jnp.where(early, 0, 1)

    return lax.fori_loop(0, chunks, step, (jnp.int32(0), jnp.int32(0)))[1 if outer else 0]


def list_columns(count, first_chunk, low_ref, high_ref, chunk_list, column_list, offset_list):
    slot0 = lax.shift_right_logical(first_chunk, 2)
    total = jnp.int32(0)
    seg_first = jnp.int32(1000)
    seg_last = jnp.int32(-1)
    seg_start = jnp.int32(0)
    for slot in range(SLOTS):

        def step(t, carry):
            low, high = carry
            i = chunk_list[t]
            here = lax.shift_right_logical(first_chunk + i, 2) == slot0 + slot
            return (
                jnp.where(here, jnp.minimum(low, low_ref[i, 0]), low),
                jnp.where(here, jnp.maximum(high, high_ref[i, 0]), high),
            )

        low, high = lax.fori_loop(0, count, step, (jnp.int32(1000), jnp.int32(-1)))
        has = high >= 0
        joins = has & (low >= seg_first) & (low <= seg_last + 1)
        begin = jnp.where(joins, seg_last + 1, low)
        fresh = jnp.where(has, jnp.maximum(high - begin + 1, 0), 0)
        base = total

        def put(j, carry):
            column_list[base + j] = begin + j
            return carry

        lax.fori_loop(0, fresh, put, 0)
        opens = has & jnp.logical_not(joins)
        seg_start = jnp.where(opens, total, seg_start)
        seg_first = jnp.where(opens, low, seg_first)
        seg_last = jnp.where(opens, high, jnp.maximum(seg_last, high))
        total = total + fresh
        offset_list[slot] = (seg_start - seg_first) * (LAT * 4)
    return total


def block_kernel(outer, chunks, own_columns, channels, nodes, *refs):
    place, low_ref, high_ref, grid = refs[:4]
    refs = refs[4:]
    if outer:
        low_own, low_swap, high_own, high_swap = refs[:4]
        refs = refs[4:]
    points, embed_in, embed_bias, ids, features = refs[:5]
    bundles = refs[5:9]
    meshes = refs[9:13]
    refs = refs[13:]
    if outer:
        messages = refs[:4]
        refs = refs[4:]
        message_bias, first_totals, first_tally, *parts = refs[:7]
        totals, tally = refs[-2:]
        refs = refs[7:-2]
    else:
        totals, tally = refs[:2]
        refs = refs[2:]
    (table, columns, sent, got, inputs, rows, embed_weight, send_weight, recv_weight,
     message_weight, mesh, extras, placed, placed_s, recv_s, chunk_list, column_list, offset_list,
     in_sems, sems) = refs
    k = place[0]
    core = lax.bitwise_and(k, 1)
    first_chunk = k * chunks
    count = list_chunks(chunks, low_ref, high_ref, own_columns, outer, chunk_list)
    total = list_columns(
        count, first_chunk, low_ref, high_ref, chunk_list, column_list, offset_list
    )

    copies = []
    for j in range(4):
        lanes = pl.ds(j * 128, 128)
        copies.append((bundles[j].at[pl.ds(0, 512)], send_weight.at[:, lanes]))
        copies.append((bundles[j].at[pl.ds(512, 512)], recv_weight.at[:, lanes]))
        copies.append((bundles[j].at[pl.ds(1024, 16)], extras.at[j]))
        at = pl.multiple_of(jnp.bitwise_xor(k, j) * 128, 128)
        copies.append((meshes[j], mesh.at[:, pl.ds(at, 128)]))
    copies = [pltpu.make_async_copy(a, b, sems.at[n]) for n, (a, b) in enumerate(copies)]
    late = []
    if outer:
        for j in range(4):
            late.append(
                pltpu.make_async_copy(
                    messages[j], message_weight.at[pl.ds(j * 128, 128)], sems.at[16 + j]
                )
            )
        for copy in late:
            copy.start()
        totals[...] = first_totals[...]
        tally[...] = first_tally[...]
    else:
        totals[...] = jnp.zeros_like(totals)
        tally[...] = jnp.zeros_like(tally)

    def fetch(source, column, slot):
        start = pl.multiple_of(column * LAT, 128)
        pltpu.make_async_copy(
            source.at[:, pl.ds(start, LAT)], columns.at[slot], in_sems.at[slot]
        ).start()

    def start_column(i):
        column = column_list[i]
        slot = lax.rem(i, BUFFERS)
        if not outer:
            fetch(grid, column - HALO, slot)
            return
        inside = (column >= HALO) & (column < HALO + own_columns)

        @pl.when(inside)
        def _():
            fetch(grid, column - HALO, slot)

        for is_side, shift, direct, swapped in (
            (column < HALO, 0, low_own, low_swap),
            (column >= HALO + own_columns, HALO + own_columns, high_own, high_swap),
        ):
            place_in = column - shift
            half = lax.shift_right_arithmetic(place_in, 1)
            within = lax.bitwise_and(place_in, 1)

            @pl.when(is_side & (half == core))
            def _():
                fetch(direct, within, slot)

            @pl.when(is_side & (half != core))
            def _():
                fetch(swapped, within, slot)

    def turn(i, carry):
        slot = lax.rem(i, BUFFERS)

        @pl.when(i + BUFFERS - 1 < total)
        def _():
            start_column(i + BUFFERS - 1)

        pltpu.make_async_copy(
            grid.at[:, pl.ds(0, LAT)], columns.at[slot], in_sems.at[slot]
        ).wait()
        source = columns.at[slot]
        for l in range(LAT // 128):
            lanes = pl.ds(l * 128, 128)
            for j in range(4):
                top = min(channels, (j + 1) * 128)
                block = source[j * 128 : top, lanes]
                if top < (j + 1) * 128:
                    block = jnp.pad(block, ((0, (j + 1) * 128 - top), (0, 0)))
                row = pl.multiple_of((i * LAT + l * 128) * 4, 8)
                table[pl.ds(row + j, 128, stride=4), :] = block.T.astype(f32)
        return carry

    def indices(ref, t):
        return ref.at[pl.ds(pl.multiple_of(chunk_list[t] * 4, 4), 4)]

    def gather(source, picks, target):
        for e in range(CHUNK):
            target[pl.ds(e, 4, stride=PITCH), :] = wide_row(source, picks[e // 128, e % 128])

    index_copies = [
        pltpu.make_async_copy(placed, placed_s, sems.at[30]),
        pltpu.make_async_copy(ids, recv_s, sems.at[31]),
    ]

    @pl.when(count > 0)
    def _():
        for b in range(BUFFERS - 1):

            @pl.when(b < total)
            def _():
                start_column(b)

        for i in range(chunks):
            slot = lax.shift_right_logical(first_chunk + i, 2) - lax.shift_right_logical(
                first_chunk, 2
            )
            placed[i * 4 : i * 4 + 4, :] = points[i * 4 : i * 4 + 4, :] + offset_list[slot]
        for copy in index_copies:
            copy.start()
        for copy in copies:
            copy.start()
        embed_weight[464:512, :] = jnp.zeros((48, 512), bf16)
        embed_weight[0:channels, :] = embed_in[...]
        lax.fori_loop(0, total, turn, 0)
        for copy in copies + index_copies:
            copy.wait()
        bias = jnp.concatenate(
            [
                sum(extras[j, 4 + r : 5 + r, :].astype(f32) for r in range(3))
                for j in range(4)
            ],
            axis=1,
        )
        terms = dot(mesh[...], recv_weight[...]) + bias
        for j in range(4):
            rows[pl.ds(j, nodes, stride=4), :] = terms[:, j * 128 : (j + 1) * 128]
        gather(table, indices(placed_s, 0), sent)
        features_by = jnp.concatenate([extras[j, 0:4, :] for j in range(4)], axis=1)

        def work(t, carry):
            i = chunk_list[t]
            inputs[...] = chunk_of(sent).astype(bf16)
            gather(rows, indices(recv_s, t), got)
            latent = silu(dot(inputs[...], embed_weight[...]) + embed_bias[...]).astype(bf16)
            before = (
                dot(latent, send_weight[...])
                + chunk_of(got)
                + lax.dot_general(
                    features[first_chunk + i], features_by, (((0,), (0,)), ((), ())),
                    preferred_element_type=f32,
                )
            )
            hidden = silu(before).astype(bf16)
            node = lax.broadcasted_iota(jnp.int32, (nodes, 128), 0) * 4
            hots = [
                jnp.where(node == ids[pl.ds(i * 4 + q, 1), :], 1.0, 0.0) for q in range(4)
            ]
            hot = jnp.concatenate([value.astype(bf16) for value in hots], axis=1)
            gather(table, indices(placed_s, jnp.minimum(t + 1, count - 1)), sent)
            totals[...] += dot(hot, hidden)
            tally[...] += (hots[0] + hots[1]) + (hots[2] + hots[3])
            return carry

        lax.fori_loop(0, count, work, 0)

    if not outer:
        return
    counts = jnp.sum(tally[...], axis=1, keepdims=True)
    whole = totals[...]
    upper = whole.astype(bf16)
    lower = (whole - upper.astype(f32)).astype(bf16)
    for copy in late:
        copy.wait()
    totals[...] = (
        dot(upper, message_weight[...])
        + dot(lower, message_weight[...])
        + counts * message_bias[...]
    )
    for r in range(2):
        mine = pl.multiple_of(jnp.bitwise_xor(k, 2 * r) * 128, 128)
        theirs = pl.multiple_of(jnp.bitwise_xor(k, 2 * r + 1) * 128, 128)
        parts[r][...] = totals[:, pl.ds(mine, 128)]
        parts[2 + r][...] = totals[:, pl.ds(theirs, 128)]


def weights_kernel(feature_weight, hidden_bias, sender_weight, receiver_weight, bundle):
    bundle[0:512, :] = sender_weight[...]
    bundle[512:1024, :] = receiver_weight[...]
    bias = hidden_bias[...]
    upper = bias.astype(bf16)
    middle = (bias - upper.astype(f32)).astype(bf16)
    lower = (bias - upper.astype(f32) - middle.astype(f32)).astype(bf16)
    bundle[1024:1040, :] = jnp.concatenate(
        [feature_weight[...].astype(f32)]
        + [value.astype(f32) for value in (upper, middle, lower)]
        + [jnp.zeros((9, bias.shape[1]), f32)],
        axis=0,
    ).astype(bf16)


def pack_kernel(chunks, points_own, all_points, nodes, lon_ref, place, senders, receivers, grid,
                points, ids, low_ref, high_ref, low_half, high_half, sems):
    lon = lon_ref[0]
    k = place[0]
    half = HALO * LAT // 2
    side = lax.bitwise_and(k, 1) * half
    low_at = pl.multiple_of(points_own - 2 * half + side, 128)
    copies = [
        pltpu.make_async_copy(grid.at[:, pl.ds(low_at, half)], low_half, sems.at[0]),
        pltpu.make_async_copy(
            grid.at[:, pl.ds(pl.multiple_of(side, 128), half)], high_half, sems.at[1]
        ),
    ]
    for copy in copies:
        copy.start()
    lows = []
    highs = []
    for i in range(chunks):
        rows = pl.ds(pl.multiple_of((k * chunks + i) * 4, 4), 4)
        point = senders[rows, :] - lon * points_own + HALO * LAT
        point = jnp.where(point < 0, point + all_points, point)
        point = jnp.where(point >= all_points, point - all_points, point)
        points[i * 4 : i * 4 + 4, :] = point * 4
        ids[i * 4 : i * 4 + 4, :] = (receivers[rows, :] - lon * nodes) * 4
        lows.append(jnp.min(point, axis=0, keepdims=True))
        highs.append(jnp.max(point, axis=0, keepdims=True))
    for ref, ends, reduce in ((low_ref, lows, jnp.min), (high_ref, highs, jnp.max)):
        ends = jnp.concatenate(ends + [ends[0]] * (16 - chunks), axis=0)
        ends = jnp.broadcast_to(reduce(ends, axis=1, keepdims=True), (16, 128))
        ref[...] = lax.shift_right_logical(lax.shift_right_logical(ends, 7) * 13108, 16)
    for copy in copies:
        copy.wait()


def weights_call(share, operands):
    return pl.pallas_call(
        weights_kernel,
        out_shape=jax.ShapeDtypeStruct((1040, share), bf16),
        in_specs=[VMEM] * 4,
        out_specs=VMEM,
        name="weights",
    )(*operands)


def pack_call(chunks, points_own, all_points, channels, nodes, operands):
    half = HALO * LAT // 2
    index = jax.ShapeDtypeStruct((chunks * 4, 128), jnp.int32)
    ends = jax.ShapeDtypeStruct((16, 128), jnp.int32)
    side = jax.ShapeDtypeStruct((channels, half), bf16)
    return pl.pallas_call(
        functools.partial(pack_kernel, chunks, points_own, all_points, nodes),
        out_shape=(index, index, ends, ends, side, side),
        in_specs=[SMEM] * 2 + [VMEM] * 2 + [ANY],
        out_specs=(VMEM,) * 6,
        scratch_shapes=[pltpu.SemaphoreType.DMA((2,))],
        name="pack",
    )(*operands)


VMEM = pl.BlockSpec(memory_space=pltpu.VMEM)
SMEM = pl.BlockSpec(memory_space=pltpu.SMEM)
ANY = pl.BlockSpec(memory_space=pl.ANY)


def block_call(outer, chunks, own_columns, channels, nodes, operands):
    width = 512
    part = jax.ShapeDtypeStruct((nodes, 128), f32)
    sums = (
        jax.ShapeDtypeStruct((nodes, width), f32),
        jax.ShapeDtypeStruct((nodes, 128), f32),
    )
    specs = [SMEM] * 3 + [ANY] * (5 if outer else 1) + [VMEM] * 5 + [ANY] * 8
    if outer:
        specs = specs + [ANY] * 4 + [VMEM] * 3
    slots = SLOTS * WINDOW
    edges = chunks * CHUNK
    square = pltpu.VMEM((width, width), bf16)
    return pl.pallas_call(
        functools.partial(block_kernel, outer, chunks, own_columns, channels, nodes),
        out_shape=(part,) * 4 if outer else sums,
        in_specs=specs,
        out_specs=(VMEM,) * (4 if outer else 2),
        scratch_shapes=[
            pltpu.VMEM((slots * LAT * 4, 128), f32),
            pltpu.VMEM((BUFFERS, channels, LAT), bf16),
            pltpu.VMEM((4 * PITCH, 128), f32),
            pltpu.VMEM((4 * PITCH, 128), f32),
            pltpu.VMEM((CHUNK, width), bf16),
            pltpu.VMEM((nodes * 4, 128), f32),
            square,
            square,
            square,
            square,
            pltpu.VMEM((nodes, width), bf16),
            pltpu.VMEM((4, 16, 128), bf16),
            pltpu.VMEM((chunks * 4, 128), jnp.int32),
            pltpu.SMEM((chunks * 4, 128), jnp.int32),
            pltpu.SMEM((chunks * 4, 128), jnp.int32),
            pltpu.SMEM((16,), jnp.int32),
            pltpu.SMEM((32,), jnp.int32),
            pltpu.SMEM((8,), jnp.int32),
            pltpu.SemaphoreType.DMA((BUFFERS,)),
            pltpu.SemaphoreType.DMA((32,)),
        ]
        + ([pltpu.VMEM(value.shape, f32) for value in sums] if outer else []),
        compiler_params=pltpu.CompilerParams(vmem_limit_bytes=60 * 2**20),
        cost_estimate=pl.CostEstimate(
            flops=2 * edges * width * (2 * width + nodes),
            bytes_accessed=2 * edges * width,
            transcendentals=2 * edges * width,
        ),
        name="block_outer" if outer else "block_inner",
    )(*operands)


def encoder(
    grid_inputs,
    embed_weight,
    embed_bias,
    mesh_latent,
    edge_features,
    senders,
    receivers,
    sender_weight,
    receiver_weight,
    feature_weight,
    hidden_bias,
    message_weight,
    message_bias,
    norm_gain,
    norm_shift,
):
    lon_count = lax.axis_size("lon")
    ch_count = lax.axis_size("ch")
    lon_place = lax.axis_index("lon")
    ch_place = lax.axis_index("ch")
    place = ch_place[None].astype(jnp.int32)
    points_own, channels = grid_inputs.shape
    own_columns = points_own // LAT
    mesh_nodes = mesh_latent.shape[0]
    full_width = message_weight.shape[1]
    edge_count = senders.shape[0]
    all_chunks = edge_count // CHUNK
    chunks = all_chunks // ch_count

    swap = [(i, i ^ 1) for i in range(ch_count)]
    across = [(i, i ^ 2) for i in range(ch_count)]
    facing = [
        (lon * ch_count + ch, (lon ^ 4) * ch_count + (ch ^ 2))
        for lon in range(lon_count)
        for ch in range(ch_count)
    ]
    forward = [(i, (i + 1) % lon_count) for i in range(lon_count)]
    backward = [(target, source) for source, target in forward]

    flat = grid_inputs.T
    lon_scalar = lon_place[None].astype(jnp.int32)
    bundle = weights_call(
        message_weight.shape[0],
        [feature_weight, hidden_bias[None, :], sender_weight, receiver_weight],
    )
    bundle_far = lax.ppermute(bundle, ("lon", "ch"), facing)
    mesh_far = lax.ppermute(mesh_latent, "ch", across)
    points, ids, low_column, high_column, low_half, high_half = pack_call(
        chunks, points_own, points_own * lon_count, channels, mesh_nodes,
        [lon_scalar, place, senders.reshape(-1, 128), receivers.reshape(-1, 128), flat],
    )
    low_own = lax.ppermute(low_half, "lon", forward)
    high_own = lax.ppermute(high_half, "lon", backward)
    low_swap = lax.ppermute(low_own, "ch", swap)
    high_swap = lax.ppermute(high_own, "ch", swap)
    bundle_near = lax.ppermute(bundle, "ch", swap)
    bundle_last = lax.ppermute(bundle_far, "ch", swap)
    mesh_near = lax.ppermute(mesh_latent, "ch", swap)
    mesh_last = lax.ppermute(mesh_far, "ch", swap)
    message_far = lax.ppermute(message_weight, ("lon", "ch"), facing)
    message_near = lax.ppermute(message_weight, "ch", swap)
    message_last = lax.ppermute(message_far, "ch", swap)
    feature_blocks = jnp.transpose(
        edge_features.reshape(edge_features.shape[0], all_chunks, CHUNK), (1, 0, 2)
    )

    call = functools.partial(
        block_call, chunks=chunks, own_columns=own_columns, channels=channels, nodes=mesh_nodes
    )
    scalars = [place, low_column, high_column, flat]
    arrays = [
        points, embed_weight, embed_bias[None, :], ids, feature_blocks,
        bundle, bundle_near, bundle_far, bundle_last,
        mesh_latent, mesh_near, mesh_far, mesh_last,
    ]
    totals, tally = call(False, operands=scalars + arrays)
    keep_here, keep_far, send_here, send_far = call(
        True,
        operands=scalars
        + [low_own, low_swap, high_own, high_swap]
        + arrays
        + [message_weight, message_near, message_far, message_last]
        + [message_bias[None, :], totals, tally],
    )
    far = keep_far + lax.ppermute(send_far, "ch", swap)
    far = lax.ppermute(far.astype(bf16), "ch", across).astype(f32)
    node_share = keep_here + lax.ppermute(send_here, "ch", swap) + far
    first_sum, second = lax.psum(
        (
            jnp.sum(node_share, axis=1, keepdims=True),
            jnp.sum(jnp.square(node_share), axis=1, keepdims=True),
        ),
        "ch",
    )
    centre = first_sum / full_width
    spread = second / full_width - jnp.square(centre)
    normed = (node_share - centre) * lax.rsqrt(spread + 1.0)
    return (mesh_latent.astype(f32) + normed * norm_gain + norm_shift).astype(bf16)


def solution(mesh):
    return jax.shard_map(
        encoder,
        mesh=mesh,
        in_specs=(
            P("lon", None),
            P(),
            P(),
            P("lon", "ch"),
            P(None, "lon"),
            P("lon"),
            P("lon"),
            P(None, "ch"),
            P(None, "ch"),
            P(None, "ch"),
            P("ch"),
            P("ch", None),
            P(),
            P("ch"),
            P("ch"),
        ),
        out_specs=P("lon", "ch"),
        check_vma=False,
    )
```

```python
import functools

import jax
import jax.numpy as jnp
from jax import lax
from jax.experimental import pallas as pl
from jax.experimental.pallas import tpu as pltpu
from jax.sharding import PartitionSpec as P


LAT = 640
HALO = 4
CHUNK = 512
SLOTS = 4
WINDOW = 7
PITCH = CHUNK + 8
BUFFERS = 8
LIMIT = 7

f32 = jnp.float32
bf16 = jnp.bfloat16


def silu(value):
    half = 0.5 * value
    return half + half * jnp.tanh(half)


def dot(left, right):
    return jnp.dot(left, right, preferred_element_type=f32)


def wide_row(ref, index):
    return ref[pl.ds(pl.multiple_of(index, 4), 4), :]


def chunk_of(tile):
    return jnp.concatenate([tile[j * PITCH : j * PITCH + CHUNK, :] for j in range(4)], axis=1)


def list_chunks(chunks, low_ref, high_ref, own_columns, outer, chunk_list):
    def step(i, counts):
        inner_count, outer_count = counts
        halo = (low_ref[i] < HALO) | (high_ref[i] >= HALO + own_columns)
        early = jnp.logical_not(halo) & (inner_count < LIMIT)
        count = outer_count if outer else inner_count

        @pl.when(jnp.logical_not(early) if outer else early)
        def _():
            chunk_list[count] = i

        return inner_count + jnp.where(early, 1, 0), outer_count + jnp.where(early, 0, 1)

    return lax.fori_loop(0, chunks, step, (jnp.int32(0), jnp.int32(0)))[1 if outer else 0]


def list_columns(count, first_chunk, low_ref, high_ref, chunk_list, column_list, offset_list):
    slot0 = lax.shift_right_logical(first_chunk, 2)
    total = jnp.int32(0)
    seg_first = jnp.int32(1000)
    seg_last = jnp.int32(-1)
    seg_start = jnp.int32(0)
    for slot in range(SLOTS):

        def step(t, carry):
            low, high = carry
            i = chunk_list[t]
            here = lax.shift_right_logical(first_chunk + i, 2) == slot0 + slot
            return (
                jnp.where(here, jnp.minimum(low, low_ref[i]), low),
                jnp.where(here, jnp.maximum(high, high_ref[i]), high),
            )

        low, high = lax.fori_loop(0, count, step, (jnp.int32(1000), jnp.int32(-1)))
        has = high >= 0
        joins = has & (low >= seg_first) & (low <= seg_last + 1)
        begin = jnp.where(joins, seg_last + 1, low)
        fresh = jnp.where(has, jnp.maximum(high - begin + 1, 0), 0)
        base = total

        def put(j, carry):
            column_list[base + j] = begin + j
            return carry

        lax.fori_loop(0, fresh, put, 0)
        opens = has & jnp.logical_not(joins)
        seg_start = jnp.where(opens, total, seg_start)
        seg_first = jnp.where(opens, low, seg_first)
        seg_last = jnp.where(opens, high, jnp.maximum(seg_last, high))
        total = total + fresh
        offset_list[slot] = (seg_start - seg_first) * (LAT * 4)
    return total


def block_kernel(outer, chunks, own_columns, channels, nodes, *refs):
    place, low_ref, high_ref, grid = refs[:4]
    refs = refs[4:]
    if outer:
        low_own, low_swap, high_own, high_swap = refs[:4]
        refs = refs[4:]
    points, embed_in, embed_bias, ids, features = refs[:5]
    bundles = refs[5:9]
    meshes = refs[9:13]
    refs = refs[13:]
    if outer:
        message_bias, first_totals, first_tally, *parts = refs[:7]
        totals, tally = refs[-2:]
        refs = refs[7:-2]
    else:
        totals, tally = refs[:2]
        refs = refs[2:]
    (table, columns, sent, got, inputs, rows, embed_weight, send_weight, recv_weight,
     message_weight, mesh, extras, placed, placed_s, recv_s, chunk_list, column_list, offset_list,
     in_sems, sems) = refs
    k = place[0]
    core = lax.bitwise_and(k, 1)
    first_chunk = k * chunks
    count = list_chunks(chunks, low_ref, high_ref, own_columns, outer, chunk_list)
    total = list_columns(
        count, first_chunk, low_ref, high_ref, chunk_list, column_list, offset_list
    )

    copies = []
    for j in range(4):
        lanes = pl.ds(j * 128, 128)
        copies.append((bundles[j].at[pl.ds(0, 512)], send_weight.at[:, lanes]))
        copies.append((bundles[j].at[pl.ds(512, 512)], recv_weight.at[:, lanes]))
        copies.append((bundles[j].at[pl.ds(1024, 16)], extras.at[j]))
        at = pl.multiple_of(jnp.bitwise_xor(k, j) * 128, 128)
        copies.append((meshes[j], mesh.at[:, pl.ds(at, 128)]))
    copies = [pltpu.make_async_copy(a, b, sems.at[n]) for n, (a, b) in enumerate(copies)]
    late = []
    if outer:
        for j in range(4):
            for q in range(4):
                late.append(
                    pltpu.make_async_copy(
                        bundles[j].at[pl.ds(1040 + q * 128, 128)],
                        message_weight.at[pl.ds(j * 128, 128), pl.ds(q * 128, 128)],
                        sems.at[32 + j * 4 + q],
                    )
                )
        for copy in late:
            copy.start()
        totals[...] = first_totals[...]
        tally[...] = first_tally[...]
    else:
        totals[...] = jnp.zeros_like(totals)
        tally[...] = jnp.zeros_like(tally)

    def fetch(source, column, slot):
        start = pl.multiple_of(column * LAT, 128)
        pltpu.make_async_copy(
            source.at[:, pl.ds(start, LAT)], columns.at[slot], in_sems.at[slot]
        ).start()

    def start_column(i):
        column = column_list[i]
        slot = lax.rem(i, BUFFERS)
        if not outer:
            fetch(grid, column - HALO, slot)
            return
        inside = (column >= HALO) & (column < HALO + own_columns)

        @pl.when(inside)
        def _():
            fetch(grid, column - HALO, slot)

        for is_side, shift, direct, swapped in (
            (column < HALO, 0, low_own, low_swap),
            (column >= HALO + own_columns, HALO + own_columns, high_own, high_swap),
        ):
            place_in = column - shift
            half = lax.shift_right_arithmetic(place_in, 1)
            within = lax.bitwise_and(place_in, 1)

            @pl.when(is_side & (half == core))
            def _():
                fetch(direct, within, slot)

            @pl.when(is_side & (half != core))
            def _():
                fetch(swapped, within, slot)

    def turn(i, carry):
        slot = lax.rem(i, BUFFERS)

        @pl.when(i + BUFFERS - 1 < total)
        def _():
            start_column(i + BUFFERS - 1)

        pltpu.make_async_copy(
            grid.at[:, pl.ds(0, LAT)], columns.at[slot], in_sems.at[slot]
        ).wait()
        source = columns.at[slot]
        for l in range(LAT // 128):
            lanes = pl.ds(l * 128, 128)
            for j in range(4):
                top = min(channels, (j + 1) * 128)
                block = source[j * 128 : top, lanes]
                if top < (j + 1) * 128:
                    block = jnp.pad(block, ((0, (j + 1) * 128 - top), (0, 0)))
                row = pl.multiple_of((i * LAT + l * 128) * 4, 8)
                table[pl.ds(row + j, 128, stride=4), :] = block.T.astype(f32)
        return carry

    def indices(ref, t):
        return ref.at[pl.ds(pl.multiple_of(chunk_list[t] * 4, 4), 4)]

    def gather(source, picks, target):
        for e in range(CHUNK):
            target[pl.ds(e, 4, stride=PITCH), :] = wide_row(source, picks[e // 128, e % 128])

    index_copies = [
        pltpu.make_async_copy(placed, placed_s, sems.at[30]),
        pltpu.make_async_copy(ids, recv_s, sems.at[31]),
    ]

    @pl.when(count > 0)
    def _():
        for b in range(BUFFERS - 1):

            @pl.when(b < total)
            def _():
                start_column(b)

        for i in range(chunks):
            slot = lax.shift_right_logical(first_chunk + i, 2) - lax.shift_right_logical(
                first_chunk, 2
            )
            placed[i * 4 : i * 4 + 4, :] = points[i * 4 : i * 4 + 4, :] + offset_list[slot]
        for copy in index_copies:
            copy.start()
        for copy in copies:
            copy.start()
        embed_weight[464:512, :] = jnp.zeros((48, 512), bf16)
        embed_weight[0:channels, :] = embed_in[...]
        lax.fori_loop(0, total, turn, 0)
        for copy in copies + index_copies:
            copy.wait()
        bias = jnp.concatenate(
            [
                sum(extras[j, 4 + r : 5 + r, :].astype(f32) for r in range(3))
                for j in range(4)
            ],
            axis=1,
        )
        terms = dot(mesh[...], recv_weight[...]) + bias
        for j in range(4):
            rows[pl.ds(j, nodes, stride=4), :] = terms[:, j * 128 : (j + 1) * 128]
        gather(table, indices(placed_s, 0), sent)
        features_by = jnp.concatenate([extras[j, 0:4, :] for j in range(4)], axis=1)

        def work(t, carry):
            i = chunk_list[t]
            inputs[...] = chunk_of(sent).astype(bf16)
            gather(rows, indices(recv_s, t), got)
            latent = silu(dot(inputs[...], embed_weight[...]) + embed_bias[...]).astype(bf16)
            before = (
                dot(latent, send_weight[...])
                + chunk_of(got)
                + lax.dot_general(
                    features[first_chunk + i], features_by, (((0,), (0,)), ((), ())),
                    preferred_element_type=f32,
                )
            )
            hidden = silu(before).astype(bf16)
            node = lax.broadcasted_iota(jnp.int32, (nodes, 128), 0) * 4
            hots = [
                jnp.where(node == ids[pl.ds(i * 4 + q, 1), :], 1.0, 0.0) for q in range(4)
            ]
            hot = jnp.concatenate([value.astype(bf16) for value in hots], axis=1)
            gather(table, indices(placed_s, jnp.minimum(t + 1, count - 1)), sent)
            totals[...] += dot(hot, hidden)
            tally[...] += (hots[0] + hots[1]) + (hots[2] + hots[3])
            return carry

        lax.fori_loop(0, count, work, 0)

    if not outer:
        return
    counts = jnp.sum(tally[...], axis=1, keepdims=True)
    whole = totals[...]
    upper = whole.astype(bf16)
    lower = (whole - upper.astype(f32)).astype(bf16)
    for copy in late:
        copy.wait()
    totals[...] = (
        dot(upper, message_weight[...])
        + dot(lower, message_weight[...])
        + counts * message_bias[...]
    )
    for r in range(2):
        mine = pl.multiple_of(jnp.bitwise_xor(k, 2 * r) * 128, 128)
        theirs = pl.multiple_of(jnp.bitwise_xor(k, 2 * r + 1) * 128, 128)
        parts[r][...] = totals[:, pl.ds(mine, 128)]
        parts[2 + r][...] = totals[:, pl.ds(theirs, 128)]


def weights_kernel(feature_weight, hidden_bias, sender_weight, receiver_weight, message_weight,
                   bundle):
    share = message_weight.shape[0]
    for q in range(4):
        bundle[1040 + q * share : 1040 + (q + 1) * share, :] = message_weight[
            :, q * share : (q + 1) * share
        ]
    bundle[0:512, :] = sender_weight[...]
    bundle[512:1024, :] = receiver_weight[...]
    bias = hidden_bias[...]
    upper = bias.astype(bf16)
    middle = (bias - upper.astype(f32)).astype(bf16)
    lower = (bias - upper.astype(f32) - middle.astype(f32)).astype(bf16)
    bundle[1024:1040, :] = jnp.concatenate(
        [feature_weight[...].astype(f32)]
        + [value.astype(f32) for value in (upper, middle, lower)]
        + [jnp.zeros((9, bias.shape[1]), f32)],
        axis=0,
    ).astype(bf16)


def pack_kernel(chunks, points_own, all_points, nodes, lon_ref, place, senders, receivers, grid,
                points, ids, low_ref, high_ref, low_half, high_half, sems):
    lon = lon_ref[0]
    k = place[0]
    half = HALO * LAT // 2
    side = lax.bitwise_and(k, 1) * half
    low_at = pl.multiple_of(points_own - 2 * half + side, 128)
    copies = [
        pltpu.make_async_copy(grid.at[:, pl.ds(low_at, half)], low_half, sems.at[0]),
        pltpu.make_async_copy(
            grid.at[:, pl.ds(pl.multiple_of(side, 128), half)], high_half, sems.at[1]
        ),
    ]
    for copy in copies:
        copy.start()
    for i in range(chunks):
        rows = pl.ds(pl.multiple_of((k * chunks + i) * 4, 4), 4)
        point = senders[rows, :] - lon * points_own + HALO * LAT
        point = jnp.where(point < 0, point + all_points, point)
        point = jnp.where(point >= all_points, point - all_points, point)
        points[i * 4 : i * 4 + 4, :] = point * 4
        ids[i * 4 : i * 4 + 4, :] = (receivers[rows, :] - lon * nodes) * 4
        for ref, end in ((low_ref, jnp.min(point)), (high_ref, jnp.max(point))):
            ref[i] = lax.shift_right_logical(lax.shift_right_logical(end, 7) * 13108, 16)
    for copy in copies:
        copy.wait()


def weights_call(share, operands):
    return pl.pallas_call(
        weights_kernel,
        out_shape=jax.ShapeDtypeStruct((1552, share), bf16),
        in_specs=[VMEM] * 5,
        out_specs=VMEM,
        name="weights",
    )(*operands)


def pack_call(chunks, points_own, all_points, channels, nodes, operands):
    half = HALO * LAT // 2
    index = jax.ShapeDtypeStruct((chunks * 4, 128), jnp.int32)
    ends = jax.ShapeDtypeStruct((chunks,), jnp.int32)
    side = jax.ShapeDtypeStruct((channels, half), bf16)
    return pl.pallas_call(
        functools.partial(pack_kernel, chunks, points_own, all_points, nodes),
        out_shape=(index, index, ends, ends, side, side),
        in_specs=[SMEM] * 2 + [VMEM] * 2 + [ANY],
        out_specs=(VMEM, VMEM, SMEM, SMEM, VMEM, VMEM),
        scratch_shapes=[pltpu.SemaphoreType.DMA((2,))],
        name="pack",
    )(*operands)


VMEM = pl.BlockSpec(memory_space=pltpu.VMEM)
SMEM = pl.BlockSpec(memory_space=pltpu.SMEM)
ANY = pl.BlockSpec(memory_space=pl.ANY)


def block_call(outer, chunks, own_columns, channels, nodes, operands):
    width = 512
    part = jax.ShapeDtypeStruct((nodes, 128), f32)
    sums = (
        jax.ShapeDtypeStruct((nodes, width), f32),
        jax.ShapeDtypeStruct((nodes, 128), f32),
    )
    specs = [SMEM] * 3 + [ANY] * (5 if outer else 1) + [VMEM] * 5 + [ANY] * 8
    if outer:
        specs = specs + [VMEM] * 3
    slots = SLOTS * WINDOW
    edges = chunks * CHUNK
    square = pltpu.VMEM((width, width), bf16)
    return pl.pallas_call(
        functools.partial(block_kernel, outer, chunks, own_columns, channels, nodes),
        out_shape=(part,) * 4 if outer else sums,
        in_specs=specs,
        out_specs=(VMEM,) * (4 if outer else 2),
        scratch_shapes=[
            pltpu.VMEM((slots * LAT * 4, 128), f32),
            pltpu.VMEM((BUFFERS, channels, LAT), bf16),
            pltpu.VMEM((4 * PITCH, 128), f32),
            pltpu.VMEM((4 * PITCH, 128), f32),
            pltpu.VMEM((CHUNK, width), bf16),
            pltpu.VMEM((nodes * 4, 128), f32),
            square,
            square,
            square,
            square,
            pltpu.VMEM((nodes, width), bf16),
            pltpu.VMEM((4, 16, 128), bf16),
            pltpu.VMEM((chunks * 4, 128), jnp.int32),
            pltpu.SMEM((chunks * 4, 128), jnp.int32),
            pltpu.SMEM((chunks * 4, 128), jnp.int32),
            pltpu.SMEM((16,), jnp.int32),
            pltpu.SMEM((32,), jnp.int32),
            pltpu.SMEM((8,), jnp.int32),
            pltpu.SemaphoreType.DMA((BUFFERS,)),
            pltpu.SemaphoreType.DMA((48,)),
        ]
        + ([pltpu.VMEM(value.shape, f32) for value in sums] if outer else []),
        compiler_params=pltpu.CompilerParams(vmem_limit_bytes=60 * 2**20),
        cost_estimate=pl.CostEstimate(
            flops=2 * edges * width * (2 * width + nodes),
            bytes_accessed=2 * edges * width,
            transcendentals=2 * edges * width,
        ),
        name="block_outer" if outer else "block_inner",
    )(*operands)


def encoder(
    grid_inputs,
    embed_weight,
    embed_bias,
    mesh_latent,
    edge_features,
    senders,
    receivers,
    sender_weight,
    receiver_weight,
    feature_weight,
    hidden_bias,
    message_weight,
    message_bias,
    norm_gain,
    norm_shift,
):
    lon_count = lax.axis_size("lon")
    ch_count = lax.axis_size("ch")
    lon_place = lax.axis_index("lon")
    ch_place = lax.axis_index("ch")
    place = ch_place[None].astype(jnp.int32)
    points_own, channels = grid_inputs.shape
    own_columns = points_own // LAT
    mesh_nodes = mesh_latent.shape[0]
    full_width = message_weight.shape[1]
    edge_count = senders.shape[0]
    all_chunks = edge_count // CHUNK
    chunks = all_chunks // ch_count

    swap = [(i, i ^ 1) for i in range(ch_count)]
    across = [(i, i ^ 2) for i in range(ch_count)]
    facing = [
        (lon * ch_count + ch, (lon ^ 4) * ch_count + (ch ^ 2))
        for lon in range(lon_count)
        for ch in range(ch_count)
    ]
    forward = [(i, (i + 1) % lon_count) for i in range(lon_count)]
    backward = [(target, source) for source, target in forward]

    flat = grid_inputs.T
    lon_scalar = lon_place[None].astype(jnp.int32)
    bundle = weights_call(
        message_weight.shape[0],
        [
            feature_weight, hidden_bias[None, :], sender_weight, receiver_weight, message_weight,
        ],
    )
    bundle_far = lax.ppermute(bundle, ("lon", "ch"), facing)
    mesh_far = lax.ppermute(mesh_latent, "ch", across)
    points, ids, low_column, high_column, low_half, high_half = pack_call(
        chunks, points_own, points_own * lon_count, channels, mesh_nodes,
        [lon_scalar, place, senders.reshape(-1, 128), receivers.reshape(-1, 128), flat],
    )
    low_own = lax.ppermute(low_half, "lon", forward)
    high_own = lax.ppermute(high_half, "lon", backward)
    low_swap = lax.ppermute(low_own, "ch", swap)
    high_swap = lax.ppermute(high_own, "ch", swap)
    bundle_near = lax.ppermute(bundle, "ch", swap)
    bundle_last = lax.ppermute(bundle_far, "ch", swap)
    mesh_near = lax.ppermute(mesh_latent, "ch", swap)
    mesh_last = lax.ppermute(mesh_far, "ch", swap)
    feature_blocks = jnp.transpose(
        edge_features.reshape(edge_features.shape[0], all_chunks, CHUNK), (1, 0, 2)
    )

    call = functools.partial(
        block_call, chunks=chunks, own_columns=own_columns, channels=channels, nodes=mesh_nodes
    )
    scalars = [place, low_column, high_column, flat]
    arrays = [
        points, embed_weight, embed_bias[None, :], ids, feature_blocks,
        bundle, bundle_near, bundle_far, bundle_last,
        mesh_latent, mesh_near, mesh_far, mesh_last,
    ]
    totals, tally = call(False, operands=scalars + arrays)
    keep_here, keep_far, send_here, send_far = call(
        True,
        operands=scalars
        + [low_own, low_swap, high_own, high_swap]
        + arrays
        + [message_bias[None, :], totals, tally],
    )
    far = keep_far + lax.ppermute(send_far, "ch", swap)
    far = lax.ppermute(far.astype(bf16), "ch", across).astype(f32)
    node_share = keep_here + lax.ppermute(send_here, "ch", swap) + far
    first_sum, second = lax.psum(
        (
            jnp.sum(node_share, axis=1, keepdims=True),
            jnp.sum(jnp.square(node_share), axis=1, keepdims=True),
        ),
        "ch",
    )
    centre = first_sum / full_width
    spread = second / full_width - jnp.square(centre)
    normed = (node_share - centre) * lax.rsqrt(spread + 1.0)
    return (mesh_latent.astype(f32) + normed * norm_gain + norm_shift).astype(bf16)


def solution(mesh):
    return jax.shard_map(
        encoder,
        mesh=mesh,
        in_specs=(
            P("lon", None),
            P(),
            P(),
            P("lon", "ch"),
            P(None, "lon"),
            P("lon"),
            P("lon"),
            P(None, "ch"),
            P(None, "ch"),
            P(None, "ch"),
            P("ch"),
            P("ch", None),
            P(),
            P("ch"),
            P("ch"),
        ),
        out_specs=P("lon", "ch"),
        check_vma=False,
    )
```
